32 devices in a mesh: sub: 4 (over x, core), lat: 2 (over y), lon: 4 (over z).
Axes of the slice: x: 2, y: 2, z: 4, core: 2. Of those that a mesh axis runs over, the one named last changes fastest.
Arguments:
- segment_launch_values: float32 [4, 3, 1024, 1024], P('sub', None, 'lat', 'lon'), may hold values from -1.8 to 1.8
- initial_backdrop: float32 [3, 1024, 1024], P(None, 'lat', 'lon'), may hold values from -1.8 to 1.8
- spectral_inverse_variances: float32 [3, 513], replicated, may hold values from 0.3 to 3
Outputs:
- weighted_defects: float32 [4, 3, 1024, 1024], P('sub', None, 'lat', 'lon')
The draws below stay inside these ranges and needn't reach their ends.
All inputs are finite; a program needn't handle non-finite values.
Results may differ from the reference program's by a relative error of at most 0.00017.
Values sent between devices are 32-bit elements; how exact they have to be, the bound alone decides.
A program may use at most 64 MiB of HBM per device.

```python
import math
import jax
import jax.numpy as jnp
from jax import lax

NLON = 1024
STEPS = 3
NLAT = 1024
NSUB = 4
ZONAL_MODES = 513


def level_of(own_key, dims, shards, least, high):
    def one(axis_at, shards_of):
        draws = jax.random.uniform(jax.random.fold_in(jax.random.fold_in(own_key, 6), axis_at), (shards_of,), jnp.float32, least / len(shards), high / len(shards))
        return jnp.repeat(jnp.exp(draws), dims[axis_at] // shards_of).reshape((-1,) + (1,) * (len(dims) - axis_at - 1))

    factor_of = one(*shards[0])
    for cut in shards[1:]:
        factor_of = factor_of * one(*cut)
    return factor_of


def centred(key, extent, width, limit, shards=(), dtype=jnp.bfloat16):
    values = width * jax.random.normal(key, extent, jnp.float32)
    if shards:
        values = values * level_of(key, extent, shards, -0.22, 0.18)
    return jnp.clip(values, -limit, limit).astype(dtype)


def setup_inputs(seed: int = 0) -> dict:
    key_of = jax.random.split(jax.random.key(seed), 4)
    return {
        "segment_launch_values": centred(key_of[0], (NSUB, 3, NLAT, NLON), 0.3, 1.8, ((0, 4), (2, 2), (3, 4)), jnp.float32),
        "initial_backdrop": centred(key_of[1], (3, NLAT, NLON), 0.3, 1.8, ((1, 2), (2, 4)), jnp.float32),
        "spectral_inverse_variances": jnp.clip(jnp.exp(jax.random.uniform(key_of[2], (3, ZONAL_MODES), jnp.float32, math.log(0.3), math.log(3.0))), 0.3, 3.0),
    }


time_step = 0.5
coriolis_peak = 0.4


def latitude_tendencies(total_rows, first_row, count):
    index = (first_row + jnp.arange(count)).astype(jnp.float32)
    return (coriolis_peak * jnp.sin(2.0 * jnp.pi * (index + 0.5) / total_rows))[:, None]


def centre(field):
    return field[1:-1, 1:-1]


def along_lon(field):
    return 0.5 * (field[1:-1, 2:] - field[1:-1, :-2])


def along_lat(field):
    return 0.5 * (field[2:, 1:-1] - field[:-2, 1:-1])


def tendency(padded, coriolis):
    height = padded[0]
    zonal = padded[1]
    meridional = padded[2]
    depth = 1.0 + height
    height_rate = -(along_lon(depth * zonal) + along_lat(depth * meridional))
    zonal_mid = centre(zonal)
    merid_mid = centre(meridional)
    zonal_rate = -(zonal_mid * along_lon(zonal) + merid_mid * along_lat(zonal)) + coriolis * merid_mid - along_lon(height)
    merid_rate = -(zonal_mid * along_lon(meridional) + merid_mid * along_lat(meridional)) - coriolis * zonal_mid - along_lat(height)
    return jnp.stack([height_rate, zonal_rate, merid_rate])


def wrapped_rate(flow_variables, coriolis):
    padded = jnp.pad(flow_variables, ((0, 0), (1, 1), (1, 1)), mode="wrap")
    return tendency(padded, coriolis)


def model_step(flow_variables, coriolis):
    first = flow_variables + time_step * wrapped_rate(flow_variables, coriolis)
    second = 0.75 * flow_variables + 0.25 * (first + time_step * wrapped_rate(first, coriolis))
    return (1.0 / 3.0) * flow_variables + (2.0 / 3.0) * (second + time_step * wrapped_rate(second, coriolis))


def reference(segment_launch_values, initial_backdrop, spectral_inverse_variances):
    coriolis = latitude_tendencies(NLAT, 0, NLAT)

    def propagated_estimate(flow_variables):
        for step_number in range(STEPS):
            flow_variables = model_step(flow_variables, coriolis)
        return flow_variables

    interval_predictions = lax.map(propagated_estimate, segment_launch_values)
    preceding_interval = jnp.concatenate([initial_backdrop[None], interval_predictions[:-1]], axis=0)
    mismatch_misfits = segment_launch_values - preceding_interval
    spectral_coefficients = jnp.fft.rfft(mismatch_misfits, axis=-1) * spectral_inverse_variances[None, :, None, :]
    return jnp.fft.irfft(spectral_coefficients, n=NLON, axis=-1).astype(jnp.float32)
```

```python
import numpy as np
import jax
import jax.numpy as jnp
from jax import lax
from jax.experimental import pallas as pl
from jax.experimental.pallas import tpu as pltpu
from jax.sharding import PartitionSpec as P

STEPS = 3
PAD = 16
EDGE = 16
SUBLANES = 8
LANES = 128
CHUNK = 8
BLOCK = 4
LAG = 2
MESH = pl.DeviceIdType.MESH

time_step = 0.5
coriolis_peak = 0.4


def cosine_table(length):
    half = length // 2
    wave = np.arange(half)[:, None]
    angle = (wave * np.arange(length)[None, :]) % length * (2.0 * np.pi / length)
    return (np.where(wave == 0, 1.0, 2.0) / length * np.cos(angle)).astype(np.float32)


def doubled_coriolis(total_rows):
    index = np.arange(-PAD, total_rows + PAD)
    line = 2.0 * coriolis_peak * np.sin(2.0 * np.pi * (index + 0.5) / total_rows)
    return np.repeat(line.astype(np.float32)[:, None], LANES, axis=1)


def split_parts(value):
    high = value.astype(jnp.bfloat16)
    return high, (value - high.astype(jnp.float32)).astype(jnp.bfloat16)


def kernel(
    nsub, nlat, nlon, x_hbm, back_hbm, w_ref, table_hbm, f_hbm, out_hbm,
    table, wpad, wave_row, conv_hi, conv_lo, fnat, frows, own, top, bot, corners,
    packed, got_packed, edges, edge_rows, following, slab, y_own, state, mid1, mid2,
    table_sem, f_sem, own_sem, rows_send, rows_recv, corner_send, corner_recv,
    pack_send, pack_recv, next_send, next_recv, in_send, in_recv, out_send, out_recv,
):
    k = lax.axis_index("sub")
    a = lax.axis_index("lat")
    z = lax.axis_index("lon")
    fields, _, span, width = x_hbm.shape
    length = width * nlon
    half = length // 2
    slices = length // LANES
    groups = width // LANES
    ring = groups + 1
    chunks = span // CHUNK
    per = SUBLANES // nlon
    blocks_of_span = span // SUBLANES
    stages = 3 * STEPS
    k_up = lax.rem(k + 1, nsub)
    k_down = lax.rem(k + nsub - 1, nsub)
    a_up = lax.rem(a + 1, nlat)
    a_down = lax.rem(a + nlat - 1, nlat)
    z_up = lax.rem(z + 1, nlon)
    z_down = lax.rem(z + nlon - 1, nlon)
    last = nsub - 1

    barrier = pltpu.get_barrier_semaphore()
    for d in range(1, nlon):
        pl.semaphore_signal(
            barrier, inc=1, device_id=(k, a, lax.rem(z + d, nlon)), device_id_type=MESH
        )
    for d in range(nlon):
        for there in ((k, a_up), (k, a_down), (k_up, a), (k_down, a)):
            pl.semaphore_signal(barrier, inc=1, device_id=there + (jnp.int32(d),), device_id_type=MESH)
    pl.semaphore_wait(barrier, nlon - 1 + 4 * nlon)

    mine = pl.ds(pl.multiple_of(z * width, width), width)

    def local(src, dst, sem):
        return pltpu.make_async_copy(src, dst, sem)

    def remote(src, dst, send, recv, there):
        return pltpu.make_async_remote_copy(
            src_ref=src, dst_ref=dst, send_sem=send, recv_sem=recv,
            device_id=there, device_id_type=MESH,
        )

    def landed(block, sem):
        local(block, block, sem).wait()

    low_rows, high_rows = pl.ds(0, PAD), pl.ds(span - PAD, PAD)
    first_lanes, last_lanes = pl.ds(0, LANES), pl.ds(width - LANES, LANES)

    def row_copies():
        return [
            remote(x_hbm.at[:, SUBLANES - 1, high_rows, :], top, rows_send.at[0], rows_recv.at[0], (k, a_up, z)),
            remote(x_hbm.at[:, 0, low_rows, :], bot, rows_send.at[1], rows_recv.at[1], (k, a_down, z)),
        ]

    def corner_copies():
        copies = []
        for i, (g, rows, lat) in enumerate(((SUBLANES - 1, high_rows, a_up), (0, low_rows, a_down))):
            for j, (cols, lon) in enumerate(((first_lanes, z_down), (last_lanes, z_up))):
                copies.append(remote(
                    x_hbm.at[:, g, rows, cols], corners.at[2 * i + j],
                    corner_send.at[2 * i + j], corner_recv.at[2 * i + j], (k, lat, lon),
                ))
        return copies

    def pack_copies():
        return [
            remote(packed.at[i], got_packed.at[i], pack_send.at[i], pack_recv.at[i], (k, a, lon))
            for i, lon in enumerate((z_down, z_up))
        ]

    def rows_of(c):
        return pl.ds(pl.multiple_of(c * CHUNK, CHUNK), CHUNK)

    def next_copy(c):
        return remote(
            x_hbm.at[:, :, rows_of(c), :], following.at[:, :, rows_of(c), :],
            next_send.at[c], next_recv.at[c], (k_down, a, z),
        )

    def inward(c, d):
        zt = lax.rem(z + d, nlon)
        src = following.at[:, pl.ds(zt * per, per), rows_of(c), :]
        dst = slab.at[:, :, rows_of(c), mine]
        if d == 0:
            return local(src, dst, in_recv.at[c, z])
        return remote(src, dst, in_send.at[c, d], in_recv.at[c, z], (k, a, zt))

    def homeward(c, d):
        zt = lax.rem(z + d, nlon)
        src = y_own.at[:, :, rows_of(c), pl.ds(pl.multiple_of(zt * width, width), width)]
        dst = out_hbm.at[:, pl.ds(z * per, per), rows_of(c), :]
        return remote(src, dst, out_send.at[c, d], out_recv.at[c, z], (k_up, a, zt))

    order = list(range(1, nlon)) + [0]

    def own_copies(src):
        return [local(src.at[c], own.at[c], own_sem.at[c]) for c in range(fields)]

    @pl.when(k < last)
    def _():
        for copy in own_copies(x_hbm):
            copy.start()
        for copy in row_copies() + corner_copies():
            copy.start()

    @pl.when(k == last)
    def _():
        for copy in own_copies(back_hbm):
            copy.start()

    for c in range(chunks):
        next_copy(c).start()
    table_copy = local(table_hbm, table, table_sem)
    f_rows = fnat.shape[0]
    f_copy = local(f_hbm.at[pl.ds(pl.multiple_of(a * (SUBLANES * span), SUBLANES), f_rows), :], fnat, f_sem)
    f_copy.start()
    table_copy.start()

    lane = lax.broadcasted_iota(jnp.int32, (SUBLANES, LANES), 1)

    def strided(r, g):
        return pl.ds(SUBLANES * r + g, SUBLANES, stride=SUBLANES)

    def spread(put, low, main, high):
        for g in range(SUBLANES):
            for b in range((span + 2 * PAD) // SUBLANES):
                r = b * SUBLANES - PAD
                if r < 0:
                    value = low(r + PAD) if g == 0 else main(g - 1, span + r)
                elif r >= span:
                    value = high(r - span) if g == SUBLANES - 1 else main(g + 1, r - span)
                else:
                    value = main(g, r)
                put(strided(b * SUBLANES, g), value)

    @pl.when(k < last)
    def _():
        for copy in own_copies(x_hbm):
            copy.wait()

        @pl.loop(0, fields)
        def _(c):
            for side in range(2):
                cols = pl.ds(0 if side == 0 else width - LANES, LANES)

                @pl.loop(0, SUBLANES)
                def _(g):
                    parts = [own[c, g, pl.ds(SUBLANES * i, SUBLANES), cols] for i in range(blocks_of_span)]
                    step = EDGE
                    while len(parts) > 1:
                        merged = []
                        for i in range(0, len(parts), 2):
                            if side == 0:
                                far = pltpu.roll(parts[i + 1], step, 1)
                                merged.append(jnp.where(lane < step, parts[i], far))
                            else:
                                far = pltpu.roll(parts[i + 1], LANES - step, 1)
                                merged.append(jnp.where(lane >= LANES - step, parts[i], far))
                        parts, step = merged, 2 * step
                    packed[side, c, g] = parts[0]

        for copy in pack_copies():
            copy.start()
        f_copy.wait()
        for g in range(SUBLANES):
            for b in range((span + 2 * PAD) // SUBLANES):
                frows[strided(b * SUBLANES, g), :] = fnat[pl.ds(g * span + b * SUBLANES, SUBLANES), :]
        landed(top, rows_recv.at[0])
        landed(bot, rows_recv.at[1])

        @pl.loop(0, fields)
        def _(c):
            for j in range(groups):
                cols = pl.ds(j * LANES, LANES)

                def put(at, value):
                    state[c, j, at, :] = value

                spread(
                    put,
                    lambda r: top[c, pl.ds(r, SUBLANES), cols],
                    lambda g, r: own[c, g, pl.ds(r, SUBLANES), cols],
                    lambda r: bot[c, pl.ds(r, SUBLANES), cols],
                )

        for i in range(4):
            landed(corners.at[i], corner_recv.at[i])
        for i in range(2):
            landed(got_packed.at[i], pack_recv.at[i])

        def join(right, left):
            return jnp.where(lane < EDGE, right, jnp.where(lane >= LANES - EDGE, left, 0.0))

        @pl.loop(0, fields)
        def _(c):
            for i in range(2):
                for r in range(0, PAD, SUBLANES):
                    at = pl.ds(r, SUBLANES)
                    edge_rows[i, at, :] = join(corners[2 * i, c, at, :], corners[2 * i + 1, c, at, :])

            @pl.loop(0, SUBLANES)
            def _(g):
                right, left = got_packed[0, c, g], got_packed[1, c, g]
                for i in range(blocks_of_span):
                    shift = EDGE * i
                    near = pltpu.roll(right, LANES - shift, 1) if i else right
                    far = pltpu.roll(left, shift, 1) if i else left
                    edges[g, pl.ds(SUBLANES * i, SUBLANES), :] = join(near, far)

            def put(at, value):
                state[c, groups, at, :] = value

            spread(
                put,
                lambda r: edge_rows[0, pl.ds(r, SUBLANES), :],
                lambda g, r: edges[g, pl.ds(r, SUBLANES), :],
                lambda r: edge_rows[1, pl.ds(r, SUBLANES), :],
            )

    @pl.when(k == last)
    def _():
        f_copy.wait()
        for copy in own_copies(back_hbm):
            copy.wait()

    def build_filters():
        wpad[...] = jnp.zeros_like(wpad)
        wpad[0:fields, 0 : half + 1] = w_ref[...]
        table_copy.wait()
        sign = 1.0 - 2.0 * (lax.broadcasted_iota(jnp.int32, (8, length), 1) % 2).astype(jnp.float32)
        wave_row[...] = (
            jnp.dot(
                wpad[:, 0:half], table[...], precision=lax.Precision.HIGHEST,
                preferred_element_type=jnp.float32,
            )
            + wpad[:, half : half + 1] * (sign / length)
        )
        step = 16
        blocks = half // LANES
        for c in range(fields):
            line = 0.5 * wave_row[c : c + 1, :]

            @pl.loop(0, LANES // step)
            def _(i):
                row = i * step + lax.broadcasted_iota(jnp.int32, (step, length), 0)
                turned = jnp.broadcast_to(line, (step, length))
                for bit in range(LANES.bit_length() - 1):
                    far = pltpu.roll(turned, 1 << bit, 1)
                    turned = jnp.where((row >> bit) % 2 == 1, far, turned)
                for q in range(slices):
                    first = turned[:, q * LANES : (q + 1) * LANES]
                    p = (q + blocks) % slices
                    other = turned[:, p * LANES : (p + 1) * LANES]
                    for part, value in enumerate((first + other, first - other)):
                        high, low = split_parts(value)
                        for m in range(blocks):
                            t = (q + m) % slices
                            if t < blocks:
                                at = pl.ds(pl.multiple_of(m * LANES + i * step, step), step)
                                conv_hi[2 * c + part, at, t * LANES : (t + 1) * LANES] = high
                                conv_lo[2 * c + part, at, t * LANES : (t + 1) * LANES] = low

    at_first = lax.broadcasted_iota(jnp.int32, (BLOCK, SUBLANES, LANES), 2) == 0
    at_last = lax.broadcasted_iota(jnp.int32, (BLOCK, SUBLANES, LANES), 2) == LANES - 1

    def across(parts):
        ahead = [pltpu.roll(q, LANES - 1, 2) for q in parts]
        behind = [pltpu.roll(q, 1, 2) for q in parts]
        return [
            jnp.where(at_last, ahead[(j + 1) % ring], ahead[j])
            - jnp.where(at_first, behind[(j - 1) % ring], behind[j])
            for j in range(ring)
        ]

    def stage(arg, base, out, keep, mix, gain, start, blocks):
        @pl.loop(0, blocks)
        def _(i):
            r0 = start + i * BLOCK
            wide = pl.ds(pl.multiple_of(SUBLANES * (r0 - 1), SUBLANES), SUBLANES * (BLOCK + 2))
            at = pl.ds(pl.multiple_of(SUBLANES * r0, SUBLANES), SUBLANES * BLOCK)
            h, u, v = [
                [arg[c, j, wide, :].reshape(BLOCK + 2, SUBLANES, LANES) for j in range(ring)]
                for c in range(3)
            ]
            f2 = frows[at, :].reshape(BLOCK, SUBLANES, LANES)
            hm, um, vm = [[q[1:-1] for q in field] for field in (h, u, v)]

            def along(q):
                return q[2:] - q[:-2]

            flux = across([p + q * p for p, q in zip(um, hm)])
            hx, ux, vx = across(hm), across(um), across(vm)
            for j in range(ring):
                dv = v[j] + h[j] * v[j]
                rate_h = flux[j] + along(dv)
                rate_u = um[j] * ux[j] + vm[j] * along(u[j]) + hx[j] - f2 * vm[j]
                rate_v = um[j] * vx[j] + vm[j] * along(v[j]) + along(h[j]) + f2 * um[j]
                for c, (m, rate) in enumerate(((hm[j], rate_h), (um[j], rate_u), (vm[j], rate_v))):
                    if base is None:
                        value = m - gain * rate
                    else:
                        old = base[c, j, at, :].reshape(BLOCK, SUBLANES, LANES)
                        value = keep * old + mix * m - gain * rate
                    out[c, j, at, :] = value.reshape(SUBLANES * BLOCK, LANES)

    def forecast(c):
        def bounds(t):
            ahead = stages - t
            fill = 2 * ahead + BLOCK - 1
            first = c * CHUNK + ahead
            extra = jnp.where(c == 0, fill - lax.rem(fill, BLOCK), 0)
            return PAD + first - extra, (CHUNK + extra) // BLOCK

        half_step = 0.5 * time_step

        @pl.loop(0, STEPS)
        def _(step):
            stage(state, None, mid1, 0.0, 1.0, half_step, *bounds(3 * step + 1))
            stage(mid1, state, mid2, 0.75, 0.25, 0.25 * half_step, *bounds(3 * step + 2))
            stage(mid2, state, state, 1.0 / 3.0, 2.0 / 3.0, 2.0 / 3.0 * half_step, *bounds(3 * step + 3))

    def filtered(c):
        for s in range(nlon):
            landed(slab.at[:, :, rows_of(c), pl.ds(s * width, width)], in_recv.at[c, s])
        rows = per * CHUNK

        @pl.loop(0, fields)
        def _(field):
            value = slab[field, :, rows_of(c), :].reshape(rows, length)
            left, right = value[:, :half], value[:, half:]
            halves = []
            for part, mix in enumerate((left + right, left - right)):
                high, low = split_parts(mix)
                both = jnp.concatenate([high, low], axis=0)
                twice = jnp.dot(both, conv_hi[2 * field + part], preferred_element_type=jnp.float32)
                rest = jnp.dot(high, conv_lo[2 * field + part], preferred_element_type=jnp.float32)
                halves.append(twice[:rows] + (twice[rows:] + rest))
            y_own[field, :, rows_of(c), 0:half] = (halves[0] + halves[1]).reshape(per, CHUNK, half)
            y_own[field, :, rows_of(c), half:length] = (halves[0] - halves[1]).reshape(per, CHUNK, half)

        for d in order:
            homeward(c, d).start()

    @pl.loop(0, chunks)
    def _(c):
        @pl.when(k < last)
        def _():
            forecast(c)

        landed(following.at[:, :, rows_of(c), :], next_recv.at[c])

        @pl.when(k < last)
        def _():
            @pl.loop(0, fields)
            def _(field):
                for g in range(SUBLANES):
                    at = pl.ds(SUBLANES * (c * CHUNK + PAD) + g, CHUNK, stride=SUBLANES)
                    for j in range(groups):
                        cols = pl.ds(j * LANES, LANES)
                        following[field, g, rows_of(c), cols] = (
                            following[field, g, rows_of(c), cols] - state[field, j, at, :]
                        )

        @pl.when(k == last)
        def _():
            @pl.loop(0, fields)
            def _(field):
                following[field, :, rows_of(c), :] = (
                    following[field, :, rows_of(c), :] - own[field, :, rows_of(c), :]
                )

        for d in order:
            inward(c, d).start()

        @pl.when(c == LAG - 1)
        def _():
            build_filters()

        @pl.when(c >= LAG)
        def _():
            filtered(c - LAG)

    @pl.loop(chunks - LAG, chunks)
    def _(c):
        filtered(c)

    @pl.loop(0, chunks)
    def _(c):
        for s in range(nlon):
            landed(out_hbm.at[:, pl.ds(s * per, per), rows_of(c), :], out_recv.at[c, s])
        next_copy(c).wait_send()
        for d in range(nlon):
            if d:
                inward(c, d).wait_send()
            homeward(c, d).wait_send()

    @pl.when(k < last)
    def _():
        for copy in row_copies() + corner_copies() + pack_copies():
            copy.wait_send()


def solution(mesh):
    nsub, nlat, nlon = mesh.shape["sub"], mesh.shape["lat"], mesh.shape["lon"]

    def shards(launch, backdrop, inverse_variances):
        fields, lat_rows, width = backdrop.shape
        length = width * nlon
        half = length // 2
        span = lat_rows // SUBLANES
        chunks = span // CHUNK
        per = SUBLANES // nlon
        ring = width // LANES + 1
        natural = (fields, SUBLANES, span, width)
        f32, bf16 = jnp.float32, jnp.bfloat16
        dma = pltpu.SemaphoreType.DMA
        any_space = pl.BlockSpec(memory_space=pl.ANY)
        vmem = pl.BlockSpec(memory_space=pltpu.VMEM)
        spread_rows = SUBLANES * (span + 2 * PAD)
        rows_like = pltpu.VMEM((fields, ring, spread_rows, LANES), f32)
        slab_like = pltpu.VMEM((fields, per, span, length), f32)
        out = pl.pallas_call(
            lambda *refs: kernel(nsub, nlat, nlon, *refs),
            name="weighted_defects",
            out_shape=jax.ShapeDtypeStruct(natural, f32),
            in_specs=[any_space, any_space, vmem, any_space, any_space],
            out_specs=any_space,
            scratch_shapes=[
                pltpu.VMEM((half, length), f32),
                pltpu.VMEM((8, half + LANES), f32),
                pltpu.VMEM((8, length), f32),
                pltpu.VMEM((2 * fields, half, half), bf16),
                pltpu.VMEM((2 * fields, half, half), bf16),
                pltpu.VMEM((lat_rows + 2 * PAD, LANES), f32),
                pltpu.VMEM((spread_rows, LANES), f32),
                pltpu.VMEM(natural, f32),
                pltpu.VMEM((fields, PAD, width), f32),
                pltpu.VMEM((fields, PAD, width), f32),
                pltpu.VMEM((4, fields, PAD, LANES), f32),
                pltpu.VMEM((2, fields, SUBLANES, SUBLANES, LANES), f32),
                pltpu.VMEM((2, fields, SUBLANES, SUBLANES, LANES), f32),
                pltpu.VMEM((SUBLANES, span, LANES), f32),
                pltpu.VMEM((2, PAD, LANES), f32),
                pltpu.VMEM(natural, f32),
                slab_like, slab_like,
                rows_like, rows_like, rows_like,
                dma, dma, dma((fields,)),
                dma((2,)), dma((2,)), dma((4,)), dma((4,)), dma((2,)), dma((2,)),
                dma((chunks,)), dma((chunks,)),
                dma((chunks, nlon)), dma((chunks, nlon)), dma((chunks, nlon)), dma((chunks, nlon)),
            ],
            compiler_params=pltpu.CompilerParams(collective_id=0, has_side_effects=True),
        )(
            launch.reshape(natural), backdrop.reshape(natural), inverse_variances,
            jnp.asarray(cosine_table(length)), jnp.asarray(doubled_coriolis(lat_rows * nlat)),
        )
        return out.reshape(launch.shape)

    return jax.shard_map(
        shards,
        mesh=mesh,
        in_specs=(P("sub", None, "lat", "lon"), P(None, "lat", "lon"), P()),
        out_specs=P("sub", None, "lat", "lon"),
        check_vma=False,
    )
```

```python
import numpy as np
import jax
import jax.numpy as jnp
from jax import lax
from jax.experimental import pallas as pl
from jax.experimental.pallas import tpu as pltpu
from jax.sharding import PartitionSpec as P

STEPS = 3
PAD = 16
EDGE = 16
SUBLANES = 8
LANES = 128
CHUNK = 8
BLOCK = 4
LAG = 2
MESH = pl.DeviceIdType.MESH

time_step = 0.5
coriolis_peak = 0.4


def waves(length):
    half, quarter = length // 2, length // 4

    def basis(points, pairs):
        n = np.arange(points)
        columns = []
        for turn, numbers in pairs:
            for m in numbers:
                scale = np.sqrt((1.0 if m in (0, half) else 2.0) / length)
                columns.append(scale * turn(2.0 * np.pi / length * ((m * n) % length)))
        return np.stack(columns, axis=1)

    fours = basis(quarter, ((np.cos, range(0, half + 1, 4)), (np.sin, range(4, half, 4))))
    twos = basis(quarter, ((np.cos, range(2, half, 4)), (np.sin, range(2, half, 4))))
    odds = basis(half, ((np.cos, range(1, half, 2)), (np.sin, range(1, half, 2))))
    out = np.stack([
        np.concatenate([np.concatenate([e, t], axis=1), o], axis=0)
        for e, t, o in ((fours, twos, odds), (fours.T, twos.T, odds.T))
    ]).astype(np.float32)
    high = out.astype(jnp.bfloat16)
    return np.stack([high, (out - high.astype(np.float32)).astype(jnp.bfloat16)], axis=1)


def split_parts(value):
    high = value.astype(jnp.bfloat16)
    return high, (value - high.astype(jnp.float32)).astype(jnp.bfloat16)


def kernel(
    nsub, nlat, nlon, x_hbm, back_hbm, w_ref, waves_hbm, out_hbm,
    waves_ref, wpad, scales, frows, own, top, bot, corners,
    packed, got_packed, edges, edge_rows, following, slab, y_own, state, mid1, mid2,
    waves_sem, own_sem, rows_send, rows_recv, corner_send, corner_recv,
    pack_send, pack_recv, next_send, next_recv, in_send, in_recv, out_send, out_recv,
):
    k = lax.axis_index("sub")
    a = lax.axis_index("lat")
    z = lax.axis_index("lon")
    fields, _, span, width = x_hbm.shape
    length = width * nlon
    half = length // 2
    quarter = length // 4
    groups = width // LANES
    ring = groups + 1
    chunks = span // CHUNK
    per = SUBLANES // nlon
    blocks_of_span = span // SUBLANES
    stages = 3 * STEPS
    k_up = lax.rem(k + 1, nsub)
    k_down = lax.rem(k + nsub - 1, nsub)
    a_up = lax.rem(a + 1, nlat)
    a_down = lax.rem(a + nlat - 1, nlat)
    z_up = lax.rem(z + 1, nlon)
    z_down = lax.rem(z + nlon - 1, nlon)
    last = nsub - 1

    barrier = pltpu.get_barrier_semaphore()
    for d in range(1, nlon):
        pl.semaphore_signal(
            barrier, inc=1, device_id=(k, a, lax.rem(z + d, nlon)), device_id_type=MESH
        )
    for d in range(nlon):
        for there in ((k, a_up), (k, a_down), (k_up, a), (k_down, a)):
            pl.semaphore_signal(barrier, inc=1, device_id=there + (jnp.int32(d),), device_id_type=MESH)
    pl.semaphore_wait(barrier, nlon - 1 + 4 * nlon)

    mine = pl.ds(pl.multiple_of(z * width, width), width)

    def local(src, dst, sem):
        return pltpu.make_async_copy(src, dst, sem)

    def remote(src, dst, send, recv, there):
        return pltpu.make_async_remote_copy(
            src_ref=src, dst_ref=dst, send_sem=send, recv_sem=recv,
            device_id=there, device_id_type=MESH,
        )

    def landed(block, sem):
        local(block, block, sem).wait()

    low_rows, high_rows = pl.ds(0, PAD), pl.ds(span - PAD, PAD)
    first_lanes, last_lanes = pl.ds(0, LANES), pl.ds(width - LANES, LANES)

    def row_copies():
        return [
            remote(x_hbm.at[:, SUBLANES - 1, high_rows, :], top, rows_send.at[0], rows_recv.at[0], (k, a_up, z)),
            remote(x_hbm.at[:, 0, low_rows, :], bot, rows_send.at[1], rows_recv.at[1], (k, a_down, z)),
        ]

    def corner_copies():
        copies = []
        for i, (g, rows, lat) in enumerate(((SUBLANES - 1, high_rows, a_up), (0, low_rows, a_down))):
            for j, (cols, lon) in enumerate(((first_lanes, z_down), (last_lanes, z_up))):
                copies.append(remote(
                    x_hbm.at[:, g, rows, cols], corners.at[2 * i + j],
                    corner_send.at[2 * i + j], corner_recv.at[2 * i + j], (k, lat, lon),
                ))
        return copies

    def pack_copies():
        return [
            remote(packed.at[i], got_packed.at[i], pack_send.at[i], pack_recv.at[i], (k, a, lon))
            for i, lon in enumerate((z_down, z_up))
        ]

    def rows_of(c):
        return pl.ds(pl.multiple_of(c * CHUNK, CHUNK), CHUNK)

    def next_copy(c):
        return remote(
            x_hbm.at[:, :, rows_of(c), :], following.at[:, :, rows_of(c), :],
            next_send.at[c], next_recv.at[c], (k_down, a, z),
        )

    def inward(c, d):
        zt = lax.rem(z + d, nlon)
        src = following.at[:, pl.ds(zt * per, per), rows_of(c), :]
        dst = slab.at[:, :, rows_of(c), mine]
        if d == 0:
            return local(src, dst, in_recv.at[c, z])
        return remote(src, dst, in_send.at[c, d], in_recv.at[c, z], (k, a, zt))

    def homeward(c, d):
        zt = lax.rem(z + d, nlon)
        src = y_own.at[:, :, rows_of(c), pl.ds(pl.multiple_of(zt * width, width), width)]
        dst = out_hbm.at[:, pl.ds(z * per, per), rows_of(c), :]
        return remote(src, dst, out_send.at[c, d], out_recv.at[c, z], (k_up, a, zt))

    order = list(range(1, nlon)) + [0]

    def own_copies(src):
        return [local(src.at[c], own.at[c], own_sem.at[c]) for c in range(fields)]

    @pl.when(k < last)
    def _():
        for copy in own_copies(x_hbm):
            copy.start()
        for copy in row_copies() + corner_copies():
            copy.start()

    @pl.when(k == last)
    def _():
        for copy in own_copies(back_hbm):
            copy.start()

    for c in range(chunks):
        next_copy(c).start()
    waves_copy = local(waves_hbm, waves_ref, waves_sem)
    waves_copy.start()

    lane = lax.broadcasted_iota(jnp.int32, (SUBLANES, LANES), 1)

    def strided(r, g):
        return pl.ds(SUBLANES * r + g, SUBLANES, stride=SUBLANES)

    def spread(put, low, main, high):
        for g in range(SUBLANES):
            for b in range((span + 2 * PAD) // SUBLANES):
                r = b * SUBLANES - PAD
                if r < 0:
                    value = low(r + PAD) if g == 0 else main(g - 1, span + r)
                elif r >= span:
                    value = high(r - span) if g == SUBLANES - 1 else main(g + 1, r - span)
                else:
                    value = main(g, r)
                put(strided(b * SUBLANES, g), value)

    def coriolis_rows():
        count = SUBLANES * (span + 2 * PAD)
        total = nlat * SUBLANES * span
        at = lax.broadcasted_iota(jnp.int32, (count, LANES), 0)
        row = a * (SUBLANES * span) + lax.rem(at, SUBLANES) * span + at // SUBLANES - PAD
        row = lax.rem(row + total, total).astype(jnp.float32)
        frows[...] = (2.0 * coriolis_peak) * jnp.sin((2.0 * np.pi / total) * (row + 0.5))

    @pl.when(k < last)
    def _():
        for copy in own_copies(x_hbm):
            copy.wait()

        @pl.loop(0, fields)
        def _(c):
            for side in range(2):
                cols = pl.ds(0 if side == 0 else width - LANES, LANES)

                @pl.loop(0, SUBLANES)
                def _(g):
                    parts = [own[c, g, pl.ds(SUBLANES * i, SUBLANES), cols] for i in range(blocks_of_span)]
                    step = EDGE
                    while len(parts) > 1:
                        merged = []
                        for i in range(0, len(parts), 2):
                            if side == 0:
                                far = pltpu.roll(parts[i + 1], step, 1)
                                merged.append(jnp.where(lane < step, parts[i], far))
                            else:
                                far = pltpu.roll(parts[i + 1], LANES - step, 1)
                                merged.append(jnp.where(lane >= LANES - step, parts[i], far))
                        parts, step = merged, 2 * step
                    packed[side, c, g] = parts[0]

        for copy in pack_copies():
            copy.start()
        coriolis_rows()
        landed(top, rows_recv.at[0])
        landed(bot, rows_recv.at[1])

        @pl.loop(0, fields)
        def _(c):
            for j in range(groups):
                cols = pl.ds(j * LANES, LANES)

                def put(at, value):
                    state[c, j, at, :] = value

                spread(
                    put,
                    lambda r: top[c, pl.ds(r, SUBLANES), cols],
                    lambda g, r: own[c, g, pl.ds(r, SUBLANES), cols],
                    lambda r: bot[c, pl.ds(r, SUBLANES), cols],
                )

        for i in range(4):
            landed(corners.at[i], corner_recv.at[i])
        for i in range(2):
            landed(got_packed.at[i], pack_recv.at[i])

        def join(right, left):
            return jnp.where(lane < EDGE, right, jnp.where(lane >= LANES - EDGE, left, 0.0))

        @pl.loop(0, fields)
        def _(c):
            for i in range(2):
                for r in range(0, PAD, SUBLANES):
                    at = pl.ds(r, SUBLANES)
                    edge_rows[i, at, :] = join(corners[2 * i, c, at, :], corners[2 * i + 1, c, at, :])

            @pl.loop(0, SUBLANES)
            def _(g):
                right, left = got_packed[0, c, g], got_packed[1, c, g]
                for i in range(blocks_of_span):
                    shift = EDGE * i
                    near = pltpu.roll(right, LANES - shift, 1) if i else right
                    far = pltpu.roll(left, shift, 1) if i else left
                    edges[g, pl.ds(SUBLANES * i, SUBLANES), :] = join(near, far)

            def put(at, value):
                state[c, groups, at, :] = value

            spread(
                put,
                lambda r: edge_rows[0, pl.ds(r, SUBLANES), :],
                lambda g, r: edges[g, pl.ds(r, SUBLANES), :],
                lambda r: edge_rows[1, pl.ds(r, SUBLANES), :],
            )

    @pl.when(k == last)
    def _():
        for copy in own_copies(back_hbm):
            copy.wait()

    def spread_scales():
        wpad[...] = jnp.zeros_like(wpad)
        wpad[0:fields, 0 : half + 1] = w_ref[...]
        depth = wpad.shape[1]
        parts, rest = [], wpad[...]
        for _ in range(3):
            part = rest.astype(jnp.bfloat16).astype(jnp.float32)
            parts.append(part)
            rest = rest - part
        parts = jnp.concatenate(parts + [jnp.zeros_like(rest)], axis=0).astype(jnp.bfloat16)
        at = lax.broadcasted_iota(jnp.int32, (LANES, length), 1)
        row = lax.broadcasted_iota(jnp.int32, (LANES, length), 0)
        eighth = quarter // 2
        fours = 4 * jnp.where(at <= eighth, at, at - eighth)
        twos = 4 * lax.rem(at, eighth) + 2
        odds = 2 * lax.rem(at, quarter) + 1
        number = jnp.where(at < quarter, fours, jnp.where(at < half, twos, odds))
        total = jnp.zeros((parts.shape[0], length), jnp.float32)
        for b in range(depth // LANES):
            chosen = jnp.where(number == row + b * LANES, 1.0, 0.0).astype(jnp.bfloat16)
            total += jnp.dot(
                parts[:, b * LANES : (b + 1) * LANES], chosen, preferred_element_type=jnp.float32
            )
        line = total[0:8] + (total[8:16] + total[16:24])
        rows = per * CHUNK
        for c in range(fields):
            scales[c * rows : (c + 1) * rows, :] = jnp.broadcast_to(line[c : c + 1, :], (rows, length))

    at_first = lax.broadcasted_iota(jnp.int32, (BLOCK, SUBLANES, LANES), 2) == 0
    at_last = lax.broadcasted_iota(jnp.int32, (BLOCK, SUBLANES, LANES), 2) == LANES - 1

    def beside(parts):
        ahead = [pltpu.roll(q, LANES - 1, 2) for q in parts]
        behind = [pltpu.roll(q, 1, 2) for q in parts]
        return [
            (
                jnp.where(at_last, ahead[(j + 1) % ring], ahead[j]),
                jnp.where(at_first, behind[(j - 1) % ring], behind[j]),
            )
            for j in range(ring)
        ]

    def stage(arg, base, out, keep, mix, gain, start, blocks):
        @pl.loop(0, blocks)
        def _(i):
            r0 = start + i * BLOCK
            wide = pl.ds(pl.multiple_of(SUBLANES * (r0 - 1), SUBLANES), SUBLANES * (BLOCK + 2))
            at = pl.ds(pl.multiple_of(SUBLANES * r0, SUBLANES), SUBLANES * BLOCK)
            h, u, v = [
                [arg[c, j, wide, :].reshape(BLOCK + 2, SUBLANES, LANES) for j in range(ring)]
                for c in range(3)
            ]
            f2 = frows[at, :].reshape(BLOCK, SUBLANES, LANES)
            hm, um, vm = [[q[1:-1] for q in field] for field in (h, u, v)]

            def along(q):
                return q[2:] - q[:-2]

            h_by, u_by, v_by = beside(hm), beside(um), beside(vm)
            for j in range(ring):
                (h1, h0), (u1, u0), (v1, v0) = h_by[j], u_by[j], v_by[j]
                dv = v[j] + h[j] * v[j]
                rate_h = (u1 + h1 * u1) - (u0 + h0 * u0) + along(dv)
                rate_u = um[j] * (u1 - u0) + vm[j] * along(u[j]) + (h1 - h0) - f2 * vm[j]
                rate_v = um[j] * (v1 - v0) + vm[j] * along(v[j]) + along(h[j]) + f2 * um[j]
                for c, (m, rate) in enumerate(((hm[j], rate_h), (um[j], rate_u), (vm[j], rate_v))):
                    if base is None:
                        value = m - gain * rate
                    else:
                        old = base[c, j, at, :].reshape(BLOCK, SUBLANES, LANES)
                        value = keep * old + mix * m - gain * rate
                    out[c, j, at, :] = value.reshape(SUBLANES * BLOCK, LANES)

    def forecast(c):
        def bounds(t):
            ahead = stages - t
            fill = 2 * ahead + BLOCK - 1
            first = c * CHUNK + ahead
            extra = jnp.where(c == 0, fill - lax.rem(fill, BLOCK), 0)
            return PAD + first - extra, (CHUNK + extra) // BLOCK

        half_step = 0.5 * time_step

        @pl.loop(0, STEPS)
        def _(step):
            stage(state, None, mid1, 0.0, 1.0, half_step, *bounds(3 * step + 1))
            stage(mid1, state, mid2, 0.75, 0.25, 0.25 * half_step, *bounds(3 * step + 2))
            stage(mid2, state, state, 1.0 / 3.0, 2.0 / 3.0, 2.0 / 3.0 * half_step, *bounds(3 * step + 3))

    def filtered(c):
        for s in range(nlon):
            landed(slab.at[:, :, rows_of(c), pl.ds(s * width, width)], in_recv.at[c, s])
        rows = fields * per * CHUNK

        def product(value, way, place):
            high, low = split_parts(value)
            both = jnp.concatenate([high, low], axis=0)
            twice = jnp.dot(both, waves_ref[(way, 0) + place], preferred_element_type=jnp.float32)
            rest = jnp.dot(high, waves_ref[(way, 1) + place], preferred_element_type=jnp.float32)
            return twice[:rows] + (twice[rows:] + rest)

        value = slab[:, :, rows_of(c), :].reshape(rows, length)
        left, right = value[:, :half], value[:, half:]
        even, odd = left + right, left - right
        places = (
            (slice(0, quarter), slice(0, quarter)),
            (slice(0, quarter), slice(quarter, half)),
            (slice(quarter, quarter + half), slice(0, half)),
        )
        inputs = (even[:, :quarter] + even[:, quarter:], even[:, :quarter] - even[:, quarter:], odd)
        at, outputs = 0, []
        for place, mix in zip(places, inputs):
            count = mix.shape[1]
            coefficients = product(mix, 0, place) * scales[:, at : at + count]
            outputs.append(product(coefficients, 1, place))
            at += count
        fours, twos, odds = outputs
        for first, even in ((0, fours + twos), (quarter, fours - twos)):
            part = odds[:, first : first + quarter]
            for start, result in ((first, even + part), (first + half, even - part)):
                y_own[:, :, rows_of(c), start : start + quarter] = result.reshape(
                    fields, per, CHUNK, quarter
                )

        for d in order:
            homeward(c, d).start()

    def send_defects(c):
        for d in order:
            inward(c, d).start()

    @pl.when(k == last)
    def _():
        @pl.loop(0, chunks)
        def _(c):
            landed(following.at[:, :, rows_of(c), :], next_recv.at[c])

            @pl.loop(0, fields)
            def _(field):
                following[field, :, rows_of(c), :] = (
                    following[field, :, rows_of(c), :] - own[field, :, rows_of(c), :]
                )

            send_defects(c)

        spread_scales()
        waves_copy.wait()

    @pl.when(k < last)
    def _():
        @pl.loop(0, chunks)
        def _(c):
            forecast(c)
            landed(following.at[:, :, rows_of(c), :], next_recv.at[c])

            @pl.loop(0, fields)
            def _(field):
                for g in range(SUBLANES):
                    at = pl.ds(SUBLANES * (c * CHUNK + PAD) + g, CHUNK, stride=SUBLANES)
                    for j in range(groups):
                        cols = pl.ds(j * LANES, LANES)
                        following[field, g, rows_of(c), cols] = (
                            following[field, g, rows_of(c), cols] - state[field, j, at, :]
                        )

            send_defects(c)

            @pl.when(c == 0)
            def _():
                spread_scales()
                waves_copy.wait()

            @pl.when(c >= LAG)
            def _():
                filtered(c - LAG)

    @pl.loop(jnp.where(k == last, 0, chunks - LAG), chunks)
    def _(c):
        filtered(c)

    @pl.loop(0, chunks)
    def _(c):
        for s in range(nlon):
            landed(out_hbm.at[:, pl.ds(s * per, per), rows_of(c), :], out_recv.at[c, s])
        next_copy(c).wait_send()
        for d in range(nlon):
            if d:
                inward(c, d).wait_send()
            homeward(c, d).wait_send()

    @pl.when(k < last)
    def _():
        for copy in row_copies() + corner_copies() + pack_copies():
            copy.wait_send()


def solution(mesh):
    nsub, nlat, nlon = mesh.shape["sub"], mesh.shape["lat"], mesh.shape["lon"]

    def shards(launch, backdrop, inverse_variances):
        fields, lat_rows, width = backdrop.shape
        length = width * nlon
        half = length // 2
        span = lat_rows // SUBLANES
        chunks = span // CHUNK
        per = SUBLANES // nlon
        ring = width // LANES + 1
        natural = (fields, SUBLANES, span, width)
        f32, bf16 = jnp.float32, jnp.bfloat16
        dma = pltpu.SemaphoreType.DMA
        any_space = pl.BlockSpec(memory_space=pl.ANY)
        vmem = pl.BlockSpec(memory_space=pltpu.VMEM)
        spread_rows = SUBLANES * (span + 2 * PAD)
        rows_like = pltpu.VMEM((fields, ring, spread_rows, LANES), f32)
        slab_like = pltpu.VMEM((fields, per, span, length), f32)
        out = pl.pallas_call(
            lambda *refs: kernel(nsub, nlat, nlon, *refs),
            name="weighted_defects",
            out_shape=jax.ShapeDtypeStruct(natural, f32),
            in_specs=[any_space, any_space, vmem, any_space],
            out_specs=any_space,
            scratch_shapes=[
                pltpu.VMEM((2, 2, half + half // 2, half), bf16),
                pltpu.VMEM((8, half + LANES), f32),
                pltpu.VMEM((fields * per * CHUNK, length), f32),
                pltpu.VMEM((spread_rows, LANES), f32),
                pltpu.VMEM(natural, f32),
                pltpu.VMEM((fields, PAD, width), f32),
                pltpu.VMEM((fields, PAD, width), f32),
                pltpu.VMEM((4, fields, PAD, LANES), f32),
                pltpu.VMEM((2, fields, SUBLANES, SUBLANES, LANES), f32),
                pltpu.VMEM((2, fields, SUBLANES, SUBLANES, LANES), f32),
                pltpu.VMEM((SUBLANES, span, LANES), f32),
                pltpu.VMEM((2, PAD, LANES), f32),
                pltpu.VMEM(natural, f32),
                slab_like, slab_like,
                rows_like, rows_like, rows_like,
                dma, dma((fields,)),
                dma((2,)), dma((2,)), dma((4,)), dma((4,)), dma((2,)), dma((2,)),
                dma((chunks,)), dma((chunks,)),
                dma((chunks, nlon)), dma((chunks, nlon)), dma((chunks, nlon)), dma((chunks, nlon)),
            ],
            compiler_params=pltpu.CompilerParams(collective_id=0, has_side_effects=True),
        )(
            launch.reshape(natural), backdrop.reshape(natural), inverse_variances,
            jnp.asarray(waves(length)),
        )
        return out.reshape(launch.shape)

    return jax.shard_map(
        shards,
        mesh=mesh,
        in_specs=(P("sub", None, "lat", "lon"), P(None, "lat", "lon"), P()),
        out_specs=P("sub", None, "lat", "lon"),
        check_vma=False,
    )
```

```python
import numpy as np
import jax
import jax.numpy as jnp
from jax import lax
from jax.experimental import pallas as pl
from jax.experimental.pallas import tpu as pltpu
from jax.sharding import PartitionSpec as P

STEPS = 3
PAD = 16
EDGE = 16
SUBLANES = 8
LANES = 128
CHUNK = 8
BLOCK = 4
LAG = 3
MESH = pl.DeviceIdType.MESH

time_step = 0.5
coriolis_peak = 0.4


def waves(length):
    half, quarter = length // 2, length // 4

    def basis(points, pairs):
        n = np.arange(points)
        columns = []
        for turn, numbers in pairs:
            for m in numbers:
                scale = np.sqrt((1.0 if m in (0, half) else 2.0) / length)
                columns.append(scale * turn(2.0 * np.pi / length * ((m * n) % length)))
        return np.stack(columns, axis=1)

    fours = basis(quarter, ((np.cos, range(0, half + 1, 4)), (np.sin, range(4, half, 4))))
    twos = basis(quarter, ((np.cos, range(2, half, 4)), (np.sin, range(2, half, 4))))
    odds = basis(half, ((np.cos, range(1, half, 2)), (np.sin, range(1, half, 2))))
    out = np.stack([
        np.concatenate([np.concatenate([e, t], axis=1), o], axis=0)
        for e, t, o in ((fours, twos, odds), (fours.T, twos.T, odds.T))
    ]).astype(np.float32)
    high = out.astype(jnp.bfloat16)
    return np.stack([high, (out - high.astype(np.float32)).astype(jnp.bfloat16)], axis=1)


def split_parts(value):
    high = value.astype(jnp.bfloat16)
    return high, (value - high.astype(jnp.float32)).astype(jnp.bfloat16)


def kernel(
    nsub, nlat, nlon, x_hbm, back_hbm, w_ref, waves_hbm, out_hbm,
    waves_ref, wpad, scales, frows, own, top, bot, corners,
    corner_packs, packed, got_packed, following, slab, y_own, state, mid1, mid2,
    waves_sem, own_sem, rows_send, rows_recv, corner_send, corner_recv,
    pack_send, pack_recv, next_send, next_recv, in_send, in_recv, out_send, out_recv,
):
    k = lax.axis_index("sub")
    a = lax.axis_index("lat")
    z = lax.axis_index("lon")
    fields, _, span, width = x_hbm.shape
    length = width * nlon
    half = length // 2
    quarter = length // 4
    groups = width // LANES
    ring = groups + 1
    chunks = span // CHUNK
    per = SUBLANES // nlon
    stages = 3 * STEPS
    k_up = lax.rem(k + 1, nsub)
    k_down = lax.rem(k + nsub - 1, nsub)
    a_up = lax.rem(a + 1, nlat)
    a_down = lax.rem(a + nlat - 1, nlat)
    z_up = lax.rem(z + 1, nlon)
    z_down = lax.rem(z + nlon - 1, nlon)
    last = nsub - 1

    barrier = pltpu.get_barrier_semaphore()
    for d in range(1, nlon):
        pl.semaphore_signal(
            barrier, inc=1, device_id=(k, a, lax.rem(z + d, nlon)), device_id_type=MESH
        )
    for d in range(nlon):
        for there in ((k, a_up), (k, a_down), (k_up, a), (k_down, a)):
            pl.semaphore_signal(barrier, inc=1, device_id=there + (jnp.int32(d),), device_id_type=MESH)

    mine = pl.ds(pl.multiple_of(z * width, width), width)

    def local(src, dst, sem):
        return pltpu.make_async_copy(src, dst, sem)

    def remote(src, dst, send, recv, there):
        return pltpu.make_async_remote_copy(
            src_ref=src, dst_ref=dst, send_sem=send, recv_sem=recv,
            device_id=there, device_id_type=MESH,
        )

    def landed(block, sem):
        local(block, block, sem).wait()

    low_rows, high_rows = pl.ds(0, PAD), pl.ds(span - PAD, PAD)
    first_lanes, last_lanes = pl.ds(0, LANES), pl.ds(width - LANES, LANES)

    def row_copies():
        return [
            remote(x_hbm.at[:, SUBLANES - 1, high_rows, :], top, rows_send.at[0], rows_recv.at[0], (k, a_up, z)),
            remote(x_hbm.at[:, 0, low_rows, :], bot, rows_send.at[1], rows_recv.at[1], (k, a_down, z)),
        ]

    def corner_copies():
        return [
            remote(
                corner_packs.at[2 * i + j], corners.at[2 * i + j],
                corner_send.at[2 * i + j], corner_recv.at[2 * i + j], (k, lat, lon),
            )
            for i, lat in enumerate((a_up, a_down)) for j, lon in enumerate((z_down, z_up))
        ]

    blocks_of_span = span // SUBLANES
    early = blocks_of_span // 2 + 1
    turn = PAD // SUBLANES

    def place_of(i):
        return (i + turn) % blocks_of_span

    def pack_copies(part):
        at = pl.ds(0, early) if part == 0 else pl.ds(early, blocks_of_span - early)
        return [
            remote(
                packed.at[i, :, at], got_packed.at[i, :, at],
                pack_send.at[part, i], pack_recv.at[part, i], (k, a, lon),
            )
            for i, lon in enumerate((z_down, z_up))
        ]

    def rows_of(c):
        return pl.ds(pl.multiple_of(c * CHUNK, CHUNK), CHUNK)

    def next_copy(c):
        return remote(
            x_hbm.at[:, :, rows_of(c), :], following.at[:, :, rows_of(c), :],
            next_send.at[c], next_recv.at[c], (k_down, a, z),
        )

    def inward(c, d):
        zt = lax.rem(z + d, nlon)
        src = following.at[:, pl.ds(zt * per, per), rows_of(c), :]
        dst = slab.at[:, :, rows_of(c), mine]
        if d == 0:
            return local(src, dst, in_recv.at[c, z])
        return remote(src, dst, in_send.at[c, d], in_recv.at[c, z], (k, a, zt))

    def homeward(c, d):
        zt = lax.rem(z + d, nlon)
        src = y_own.at[:, :, rows_of(c), pl.ds(pl.multiple_of(zt * width, width), width)]
        dst = out_hbm.at[:, pl.ds(z * per, per), rows_of(c), :]
        return remote(src, dst, out_send.at[c, d], out_recv.at[c, z], (k_up, a, zt))

    order = list(range(1, nlon)) + [0]

    def own_copies(src):
        return [local(src.at[c], own.at[c], own_sem.at[c]) for c in range(fields)]

    @pl.when(k < last)
    def _():
        for copy in own_copies(x_hbm):
            copy.start()

    @pl.when(k == last)
    def _():
        for copy in own_copies(back_hbm):
            copy.start()

    waves_copy = local(waves_hbm, waves_ref, waves_sem)
    waves_copy.start()

    lane = lax.broadcasted_iota(jnp.int32, (SUBLANES, LANES), 1)

    def strided(r, g):
        return pl.ds(SUBLANES * r + g, SUBLANES, stride=SUBLANES)

    def spread(put, low, main, high):
        for g in range(SUBLANES):
            for b in range((span + 2 * PAD) // SUBLANES):
                r = b * SUBLANES - PAD
                if r < 0:
                    value = low(r + PAD) if g == 0 else main(g - 1, span + r)
                elif r >= span:
                    value = high(r - span) if g == SUBLANES - 1 else main(g + 1, r - span)
                else:
                    value = main(g, r)
                put(strided(b * SUBLANES, g), value)

    def coriolis_rows():
        count = SUBLANES * (span + 2 * PAD)
        total = nlat * SUBLANES * span
        at = lax.broadcasted_iota(jnp.int32, (count, LANES), 0)
        row = a * (SUBLANES * span) + lax.rem(at, SUBLANES) * span + at // SUBLANES - PAD
        row = lax.rem(row + total, total).astype(jnp.float32)
        frows[...] = (2.0 * coriolis_peak) * jnp.sin((2.0 * np.pi / total) * (row + 0.5))

    def merge(parts, side):
        step = EDGE
        while len(parts) > 1:
            merged = []
            for i in range(0, len(parts) - 1, 2):
                if side == 0:
                    far = pltpu.roll(parts[i + 1], step, 1)
                    merged.append(jnp.where(lanes_of(far) < step, parts[i], far))
                else:
                    far = pltpu.roll(parts[i + 1], LANES - step, 1)
                    merged.append(jnp.where(lanes_of(far) >= LANES - step, parts[i], far))
            if len(parts) % 2:
                merged.append(parts[-1])
            parts, step = merged, 2 * step
        return parts[0]

    def lanes_of(value):
        return lax.broadcasted_iota(jnp.int32, value.shape, len(value.shape) - 1)

    def join(right, left, slot):
        shift = EDGE * slot
        near = pltpu.roll(right, LANES - shift, 1) if slot else right
        far = pltpu.roll(left, shift, 1) if slot else left
        return jnp.where(lane < EDGE, near, jnp.where(lane >= LANES - EDGE, far, 0.0))

    ends = ((SUBLANES - 1, span - PAD), (0, 0))

    @pl.when(k < last)
    def _():
        for copy in own_copies(x_hbm):
            copy.wait()

        @pl.loop(0, fields)
        def _(c):
            for side in range(2):
                cols = pl.ds(0 if side == 0 else width - LANES, LANES)
                whole = merge([own[c, g, :, cols] for g in range(SUBLANES)], side)
                for i in range(blocks_of_span):
                    packed[side, c, place_of(i)] = whole[SUBLANES * i : SUBLANES * (i + 1)]

        for i, (g, first) in enumerate(ends):
            for side in range(2):
                cols = pl.ds(0 if side == 0 else width - LANES, LANES)
                corner_packs[2 * i + side] = merge(
                    [
                        own[c, g, pl.ds(first + SUBLANES * b, SUBLANES), cols]
                        for c in range(fields) for b in range(turn)
                    ],
                    side,
                )
        coriolis_rows()

    pl.semaphore_wait(barrier, nlon - 1 + 4 * nlon)

    @pl.when(k < last)
    def _():
        for copy in pack_copies(0) + row_copies() + corner_copies() + pack_copies(1):
            copy.start()

    for c in range(chunks):
        next_copy(c).start()

    def edge_blocks(numbers, corner):
        @pl.loop(0, fields)
        def _(c):
            def put(r, g, value):
                state[c, groups, strided(r + PAD, g), :] = value

            for i in numbers:
                right, left = got_packed[0, c, place_of(i)], got_packed[1, c, place_of(i)]
                for g in range(SUBLANES):
                    value = join(right, left, g)
                    r = SUBLANES * i
                    put(r, g, value)
                    if r >= span - PAD and g < SUBLANES - 1:
                        put(r - span, g + 1, value)
                    if r < PAD and g > 0:
                        put(r + span, g - 1, value)

        for c in range(fields):
            for b in range(turn):
                value = join(corners[2 * corner], corners[2 * corner + 1], c * turn + b)
                g, r = ((0, -PAD), (SUBLANES - 1, span))[corner]
                state[c, groups, strided(r + SUBLANES * b + PAD, g), :] = value

    early_blocks = [i for i in range(blocks_of_span) if place_of(i) < early]
    late_blocks = [i for i in range(blocks_of_span) if place_of(i) >= early]

    def late_edges():
        for i in range(2):
            landed(got_packed.at[i, :, pl.ds(early, blocks_of_span - early)], pack_recv.at[1, i])
            landed(corners.at[2 + i], corner_recv.at[2 + i])
        edge_blocks(late_blocks, 1)

    @pl.when(k < last)
    def _():
        landed(top, rows_recv.at[0])
        landed(bot, rows_recv.at[1])

        @pl.loop(0, fields)
        def _(c):
            for j in range(groups):
                cols = pl.ds(j * LANES, LANES)

                def put(at, value):
                    state[c, j, at, :] = value

                spread(
                    put,
                    lambda r: top[c, pl.ds(r, SUBLANES), cols],
                    lambda g, r: own[c, g, pl.ds(r, SUBLANES), cols],
                    lambda r: bot[c, pl.ds(r, SUBLANES), cols],
                )

        for i in range(2):
            landed(got_packed.at[i, :, pl.ds(0, early)], pack_recv.at[0, i])
            landed(corners.at[i], corner_recv.at[i])
        edge_blocks(early_blocks, 0)

    @pl.when(k == last)
    def _():
        for copy in own_copies(back_hbm):
            copy.wait()

    def spread_scales():
        wpad[...] = jnp.zeros_like(wpad)
        wpad[0:fields, 0 : half + 1] = w_ref[...]
        depth = wpad.shape[1]
        parts, rest = [], wpad[...]
        for _ in range(3):
            part = rest.astype(jnp.bfloat16).astype(jnp.float32)
            parts.append(part)
            rest = rest - part
        parts = jnp.concatenate(parts + [jnp.zeros_like(rest)], axis=0).astype(jnp.bfloat16)
        at = lax.broadcasted_iota(jnp.int32, (LANES, length), 1)
        row = lax.broadcasted_iota(jnp.int32, (LANES, length), 0)
        eighth = quarter // 2
        fours = 4 * jnp.where(at <= eighth, at, at - eighth)
        twos = 4 * lax.rem(at, eighth) + 2
        odds = 2 * lax.rem(at, quarter) + 1
        number = jnp.where(at < quarter, fours, jnp.where(at < half, twos, odds))
        total = jnp.zeros((parts.shape[0], length), jnp.float32)
        for b in range(depth // LANES):
            chosen = jnp.where(number == row + b * LANES, 1.0, 0.0).astype(jnp.bfloat16)
            total += jnp.dot(
                parts[:, b * LANES : (b + 1) * LANES], chosen, preferred_element_type=jnp.float32
            )
        line = total[0:8] + (total[8:16] + total[16:24])
        rows = per * CHUNK
        for c in range(fields):
            scales[c * rows : (c + 1) * rows, :] = jnp.broadcast_to(line[c : c + 1, :], (rows, length))

    at_first = lax.broadcasted_iota(jnp.int32, (BLOCK, SUBLANES, LANES), 2) == 0
    at_last = lax.broadcasted_iota(jnp.int32, (BLOCK, SUBLANES, LANES), 2) == LANES - 1

    def beside(parts):
        ahead = [pltpu.roll(q, LANES - 1, 2) for q in parts]
        behind = [pltpu.roll(q, 1, 2) for q in parts]
        return [
            (
                jnp.where(at_last, ahead[(j + 1) % ring], ahead[j]),
                jnp.where(at_first, behind[(j - 1) % ring], behind[j]),
            )
            for j in range(ring)
        ]

    def stage(arg, base, out, keep, mix, gain, start, blocks):
        @pl.loop(0, blocks)
        def _(i):
            r0 = start + i * BLOCK
            wide = pl.ds(pl.multiple_of(SUBLANES * (r0 - 1), SUBLANES), SUBLANES * (BLOCK + 2))
            at = pl.ds(pl.multiple_of(SUBLANES * r0, SUBLANES), SUBLANES * BLOCK)
            h, u, v = [
                [arg[c, j, wide, :].reshape(BLOCK + 2, SUBLANES, LANES) for j in range(ring)]
                for c in range(3)
            ]
            f2 = frows[at, :].reshape(BLOCK, SUBLANES, LANES)
            hm, um, vm = [[q[1:-1] for q in field] for field in (h, u, v)]

            def along(q):
                return q[2:] - q[:-2]

            h_by, u_by, v_by = beside(hm), beside(um), beside(vm)
            for j in range(ring):
                (h1, h0), (u1, u0), (v1, v0) = h_by[j], u_by[j], v_by[j]
                dv = v[j] + h[j] * v[j]
                rate_h = (u1 + h1 * u1) - (u0 + h0 * u0) + along(dv)
                rate_u = um[j] * (u1 - u0) + vm[j] * along(u[j]) + (h1 - h0) - f2 * vm[j]
                rate_v = um[j] * (v1 - v0) + vm[j] * along(v[j]) + along(h[j]) + f2 * um[j]
                for c, (m, rate) in enumerate(((hm[j], rate_h), (um[j], rate_u), (vm[j], rate_v))):
                    if base is None:
                        value = m - gain * rate
                    else:
                        old = base[c, j, at, :].reshape(BLOCK, SUBLANES, LANES)
                        value = keep * old + mix * m - gain * rate
                    out[c, j, at, :] = value.reshape(SUBLANES * BLOCK, LANES)

    def forecast(c):
        def bounds(t):
            ahead = stages - t
            fill = 2 * ahead + BLOCK - 1
            first = c * CHUNK + ahead
            extra = jnp.where(c == 0, fill - lax.rem(fill, BLOCK), 0)
            return PAD + first - extra, (CHUNK + extra) // BLOCK

        half_step = 0.5 * time_step

        @pl.loop(0, STEPS)
        def _(step):
            stage(state, None, mid1, 0.0, 1.0, half_step, *bounds(3 * step + 1))
            stage(mid1, state, mid2, 0.75, 0.25, 0.25 * half_step, *bounds(3 * step + 2))
            stage(mid2, state, state, 1.0 / 3.0, 2.0 / 3.0, 2.0 / 3.0 * half_step, *bounds(3 * step + 3))

    def filtered(c):
        for s in range(nlon):
            landed(slab.at[:, :, rows_of(c), pl.ds(s * width, width)], in_recv.at[c, s])
        rows = fields * per * CHUNK

        def product(value, way, place):
            high, low = split_parts(value)
            both = jnp.concatenate([high, low], axis=0)
            twice = jnp.dot(both, waves_ref[(way, 0) + place], preferred_element_type=jnp.float32)
            rest = jnp.dot(high, waves_ref[(way, 1) + place], preferred_element_type=jnp.float32)
            return twice[:rows] + (twice[rows:] + rest)

        value = slab[:, :, rows_of(c), :].reshape(rows, length)
        left, right = value[:, :half], value[:, half:]
        even, odd = left + right, left - right
        places = (
            (slice(0, quarter), slice(0, quarter)),
            (slice(0, quarter), slice(quarter, half)),
            (slice(quarter, quarter + half), slice(0, half)),
        )
        inputs = (even[:, :quarter] + even[:, quarter:], even[:, :quarter] - even[:, quarter:], odd)
        at, outputs = 0, []
        for place, mix in zip(places, inputs):
            count = mix.shape[1]
            coefficients = product(mix, 0, place) * scales[:, at : at + count]
            outputs.append(product(coefficients, 1, place))
            at += count
        fours, twos, odds = outputs
        for first, even in ((0, fours + twos), (quarter, fours - twos)):
            part = odds[:, first : first + quarter]
            for start, result in ((first, even + part), (first + half, even - part)):
                y_own[:, :, rows_of(c), start : start + quarter] = result.reshape(
                    fields, per, CHUNK, quarter
                )

        for d in order:
            homeward(c, d).start()

    def send_defects(c):
        for d in order:
            inward(c, d).start()

    @pl.when(k == last)
    def _():
        @pl.loop(0, chunks)
        def _(c):
            landed(following.at[:, :, rows_of(c), :], next_recv.at[c])

            @pl.loop(0, fields)
            def _(field):
                following[field, :, rows_of(c), :] = (
                    following[field, :, rows_of(c), :] - own[field, :, rows_of(c), :]
                )

            send_defects(c)

        spread_scales()
        waves_copy.wait()

    @pl.when(k < last)
    def _():
        @pl.loop(0, chunks)
        def _(c):
            forecast(c)
            landed(following.at[:, :, rows_of(c), :], next_recv.at[c])

            @pl.loop(0, fields)
            def _(field):
                for g in range(SUBLANES):
                    at = pl.ds(SUBLANES * (c * CHUNK + PAD) + g, CHUNK, stride=SUBLANES)
                    for j in range(groups):
                        cols = pl.ds(j * LANES, LANES)
                        following[field, g, rows_of(c), cols] = (
                            following[field, g, rows_of(c), cols] - state[field, j, at, :]
                        )

            send_defects(c)

            @pl.when(c == 0)
            def _():
                late_edges()
                spread_scales()
                waves_copy.wait()

            @pl.when(c >= LAG)
            def _():
                filtered(c - LAG)

    @pl.loop(jnp.where(k == last, 0, chunks - LAG), chunks)
    def _(c):
        filtered(c)

    @pl.loop(0, chunks)
    def _(c):
        for s in range(nlon):
            landed(out_hbm.at[:, pl.ds(s * per, per), rows_of(c), :], out_recv.at[c, s])
        next_copy(c).wait_send()
        for d in range(nlon):
            if d:
                inward(c, d).wait_send()
            homeward(c, d).wait_send()

    @pl.when(k < last)
    def _():
        for copy in row_copies() + corner_copies() + pack_copies(0) + pack_copies(1):
            copy.wait_send()


def solution(mesh):
    nsub, nlat, nlon = mesh.shape["sub"], mesh.shape["lat"], mesh.shape["lon"]

    def shards(launch, backdrop, inverse_variances):
        fields, lat_rows, width = backdrop.shape
        length = width * nlon
        half = length // 2
        span = lat_rows // SUBLANES
        chunks = span // CHUNK
        per = SUBLANES // nlon
        ring = width // LANES + 1
        natural = (fields, SUBLANES, span, width)
        f32, bf16 = jnp.float32, jnp.bfloat16
        dma = pltpu.SemaphoreType.DMA
        any_space = pl.BlockSpec(memory_space=pl.ANY)
        vmem = pl.BlockSpec(memory_space=pltpu.VMEM)
        spread_rows = SUBLANES * (span + 2 * PAD)
        corner_like = pltpu.VMEM((4, SUBLANES, LANES), f32)
        pack_like = pltpu.VMEM((2, fields, span // SUBLANES, SUBLANES, LANES), f32)
        rows_like = pltpu.VMEM((fields, ring, spread_rows, LANES), f32)
        slab_like = pltpu.VMEM((fields, per, span, length), f32)
        out = pl.pallas_call(
            lambda *refs: kernel(nsub, nlat, nlon, *refs),
            name="weighted_defects",
            out_shape=jax.ShapeDtypeStruct(natural, f32),
            in_specs=[any_space, any_space, vmem, any_space],
            out_specs=any_space,
            scratch_shapes=[
                pltpu.VMEM((2, 2, half + half // 2, half), bf16),
                pltpu.VMEM((8, half + LANES), f32),
                pltpu.VMEM((fields * per * CHUNK, length), f32),
                pltpu.VMEM((spread_rows, LANES), f32),
                pltpu.VMEM(natural, f32),
                pltpu.VMEM((fields, PAD, width), f32),
                pltpu.VMEM((fields, PAD, width), f32),
                corner_like, corner_like, pack_like, pack_like,
                pltpu.VMEM(natural, f32),
                slab_like, slab_like,
                rows_like, rows_like, rows_like,
                dma, dma((fields,)),
                dma((2,)), dma((2,)), dma((4,)), dma((4,)), dma((2, 2)), dma((2, 2)),
                dma((chunks,)), dma((chunks,)),
                dma((chunks, nlon)), dma((chunks, nlon)), dma((chunks, nlon)), dma((chunks, nlon)),
            ],
            compiler_params=pltpu.CompilerParams(collective_id=0, has_side_effects=True),
        )(
            launch.reshape(natural), backdrop.reshape(natural), inverse_variances,
            jnp.asarray(waves(length)),
        )
        return out.reshape(launch.shape)

    return jax.shard_map(
        shards,
        mesh=mesh,
        in_specs=(P("sub", None, "lat", "lon"), P(None, "lat", "lon"), P()),
        out_specs=P("sub", None, "lat", "lon"),
        check_vma=False,
    )
```

```python
import numpy as np
import jax
import jax.numpy as jnp
from jax import lax
from jax.experimental import pallas as pl
from jax.experimental.pallas import tpu as pltpu
from jax.sharding import PartitionSpec as P

STEPS = 3
PAD = 16
EDGE = 16
SUBLANES = 8
LANES = 128
CHUNK = 8
BLOCK = 4
LAG = 3
VMEM_LIMIT = 52 * 2**20
MESH = pl.DeviceIdType.MESH

time_step = 0.5
coriolis_peak = 0.4


def waves(length):
    half, quarter = length // 2, length // 4

    def basis(points, pairs):
        n = np.arange(points)
        columns = []
        for turn, numbers in pairs:
            for m in numbers:
                scale = np.sqrt((1.0 if m in (0, half) else 2.0) / length)
                columns.append(scale * turn(2.0 * np.pi / length * ((m * n) % length)))
        return np.stack(columns, axis=1)

    fours = basis(quarter, ((np.cos, range(0, half + 1, 4)), (np.sin, range(4, half, 4))))
    twos = basis(quarter, ((np.cos, range(2, half, 4)), (np.sin, range(2, half, 4))))
    odds = basis(half, ((np.cos, range(1, half, 2)), (np.sin, range(1, half, 2))))
    out = np.stack([
        np.concatenate([np.concatenate([e, t], axis=1), o], axis=0)
        for e, t, o in ((fours, twos, odds), (fours.T, twos.T, odds.T))
    ]).astype(np.float32)
    high = out.astype(jnp.bfloat16)
    return np.stack([high, (out - high.astype(np.float32)).astype(jnp.bfloat16)], axis=1)


def split_parts(value):
    high = value.astype(jnp.bfloat16)
    return high, (value - high.astype(jnp.float32)).astype(jnp.bfloat16)


def kernel(
    nsub, nlat, nlon, x_hbm, back_hbm, w_ref, waves_hbm, out_hbm,
    waves_ref, wpad, scales, frows, own, top, bot, corners,
    corner_packs, packed, got_packed, following, relayed, slab, y_own, state, mid1, mid2,
    waves_sem, own_sem, rows_send, rows_recv, corner_send, corner_recv,
    pack_send, pack_recv, next_send, next_recv, relay_send, relay_recv, in_send, in_recv, out_send, out_recv,
):
    k = lax.axis_index("sub")
    a = lax.axis_index("lat")
    z = lax.axis_index("lon")
    fields, _, span, width = x_hbm.shape
    length = width * nlon
    half = length // 2
    quarter = length // 4
    groups = width // LANES
    ring = groups + 1
    chunks = span // CHUNK
    per = SUBLANES // nlon
    stages = 3 * STEPS
    k_up = lax.rem(k + 1, nsub)
    k_down = lax.rem(k + nsub - 1, nsub)
    a_up = lax.rem(a + 1, nlat)
    a_down = lax.rem(a + nlat - 1, nlat)
    z_up = lax.rem(z + 1, nlon)
    z_down = lax.rem(z + nlon - 1, nlon)
    last = nsub - 1
    giver, taker = (last - 2, last - 1) if nsub > 2 else (-1, -1)

    barrier = pltpu.get_barrier_semaphore()
    for d in range(1, nlon):
        pl.semaphore_signal(
            barrier, inc=1, device_id=(k, a, lax.rem(z + d, nlon)), device_id_type=MESH
        )
    for d in range(nlon):
        for there in ((k, a_up), (k, a_down), (k_up, a), (k_down, a)):
            pl.semaphore_signal(barrier, inc=1, device_id=there + (jnp.int32(d),), device_id_type=MESH)

    mine = pl.ds(pl.multiple_of(z * width, width), width)

    def local(src, dst, sem):
        return pltpu.make_async_copy(src, dst, sem)

    def remote(src, dst, send, recv, there):
        return pltpu.make_async_remote_copy(
            src_ref=src, dst_ref=dst, send_sem=send, recv_sem=recv,
            device_id=there, device_id_type=MESH,
        )

    def landed(block, sem):
        local(block, block, sem).wait()

    low_rows, high_rows = pl.ds(0, PAD), pl.ds(span - PAD, PAD)
    first_lanes, last_lanes = pl.ds(0, LANES), pl.ds(width - LANES, LANES)

    def row_copies():
        return [
            remote(x_hbm.at[:, SUBLANES - 1, high_rows, :], top, rows_send.at[0], rows_recv.at[0], (k, a_up, z)),
            remote(x_hbm.at[:, 0, low_rows, :], bot, rows_send.at[1], rows_recv.at[1], (k, a_down, z)),
        ]

    def corner_copies():
        return [
            remote(
                corner_packs.at[2 * i + j], corners.at[2 * i + j],
                corner_send.at[2 * i + j], corner_recv.at[2 * i + j], (k, lat, lon),
            )
            for i, lat in enumerate((a_up, a_down)) for j, lon in enumerate((z_down, z_up))
        ]

    blocks_of_span = span // SUBLANES
    early = blocks_of_span // 2 + 1
    turn = PAD // SUBLANES

    def place_of(i):
        return (i + turn) % blocks_of_span

    def pack_copies(part):
        at = pl.ds(0, early) if part == 0 else pl.ds(early, blocks_of_span - early)
        return [
            remote(
                packed.at[i, :, at], got_packed.at[i, :, at],
                pack_send.at[part, i], pack_recv.at[part, i], (k, a, lon),
            )
            for i, lon in enumerate((z_down, z_up))
        ]

    def rows_of(c):
        return pl.ds(pl.multiple_of(c * CHUNK, CHUNK), CHUNK)

    def next_copy(c):
        return remote(
            x_hbm.at[:, :, rows_of(c), :], following.at[:, :, rows_of(c), :],
            next_send.at[c], next_recv.at[c], (k_down, a, z),
        )

    def inward(c, d, block=None):
        zt = lax.rem(z + d, nlon)
        if block is None:
            block = following.at[:, :, rows_of(c), :]
        src = block.at[:, pl.ds(zt * per, per)]
        dst = slab.at[:, :, rows_of(c), mine]
        if d == 0:
            return local(src, dst, in_recv.at[c, z])
        return remote(src, dst, in_send.at[c, d], in_recv.at[c, z], (k, a, zt))

    def relay():
        return remote(following.at[:, :, rows_of(chunks - 1), :], relayed, relay_send, relay_recv, (k_up, a, z))

    def homeward(c, d, target=None):
        zt = lax.rem(z + d, nlon)
        home = c if target is None else target
        src = y_own.at[:, :, rows_of(c), pl.ds(pl.multiple_of(zt * width, width), width)]
        dst = out_hbm.at[:, pl.ds(z * per, per), rows_of(home), :]
        if target is not None and d == 0:
            return local(src, dst, out_recv.at[home, z])
        return remote(
            src, dst, out_send.at[c, d], out_recv.at[home, z], (k_up if target is None else k, a, zt)
        )

    order = list(range(1, nlon)) + [0]

    def own_copies(src):
        return [local(src.at[c], own.at[c], own_sem.at[c]) for c in range(fields)]

    @pl.when(k < last)
    def _():
        for copy in own_copies(x_hbm):
            copy.start()

    @pl.when(k == last)
    def _():
        for copy in own_copies(back_hbm):
            copy.start()

    waves_copy = local(waves_hbm, waves_ref, waves_sem)
    waves_copy.start()

    lane = lax.broadcasted_iota(jnp.int32, (SUBLANES, LANES), 1)

    def strided(r, g):
        return pl.ds(SUBLANES * r + g, SUBLANES, stride=SUBLANES)

    def spread(put, low, main, high):
        for g in range(SUBLANES):
            for b in range((span + 2 * PAD) // SUBLANES):
                r = b * SUBLANES - PAD
                if r < 0:
                    value = low(r + PAD) if g == 0 else main(g - 1, span + r)
                elif r >= span:
                    value = high(r - span) if g == SUBLANES - 1 else main(g + 1, r - span)
                else:
                    value = main(g, r)
                put(strided(b * SUBLANES, g), value)

    def coriolis_rows():
        total = nlat * SUBLANES * span
        group = lax.broadcasted_iota(jnp.int32, (SUBLANES, LANES), 0)
        for first in range(0, span + 2 * PAD, LANES):
            row = a * (SUBLANES * span) + group * span + lane + (first - PAD)
            row = lax.rem(row + total, total).astype(jnp.float32)
            line = (2.0 * coriolis_peak) * jnp.sin((2.0 * np.pi / total) * (row + 0.5))
            for r in range(first, min(first + LANES, span + 2 * PAD)):
                frows[SUBLANES * r : SUBLANES * (r + 1), :] = jnp.broadcast_to(
                    line[:, r - first : r - first + 1], (SUBLANES, LANES)
                )

    def merge(parts, side):
        step = EDGE
        while len(parts) > 1:
            merged = []
            for i in range(0, len(parts) - 1, 2):
                if side == 0:
                    far = pltpu.roll(parts[i + 1], step, 1)
                    merged.append(jnp.where(lanes_of(far) < step, parts[i], far))
                else:
                    far = pltpu.roll(parts[i + 1], LANES - step, 1)
                    merged.append(jnp.where(lanes_of(far) >= LANES - step, parts[i], far))
            if len(parts) % 2:
                merged.append(parts[-1])
            parts, step = merged, 2 * step
        return parts[0]

    def lanes_of(value):
        return lax.broadcasted_iota(jnp.int32, value.shape, len(value.shape) - 1)

    def join(right, left, slot):
        shift = EDGE * slot
        near = pltpu.roll(right, LANES - shift, 1) if slot else right
        far = pltpu.roll(left, shift, 1) if slot else left
        return jnp.where(lane < EDGE, near, jnp.where(lane >= LANES - EDGE, far, 0.0))

    ends = ((SUBLANES - 1, span - PAD), (0, 0))

    @pl.when(k < last)
    def _():
        for copy in own_copies(x_hbm):
            copy.wait()

        @pl.loop(0, fields)
        def _(c):
            for side in range(2):
                cols = pl.ds(0 if side == 0 else width - LANES, LANES)
                whole = merge([own[c, g, :, cols] for g in range(SUBLANES)], side)
                for i in range(blocks_of_span):
                    packed[side, c, place_of(i)] = whole[SUBLANES * i : SUBLANES * (i + 1)]

        for i, (g, first) in enumerate(ends):
            for side in range(2):
                cols = pl.ds(0 if side == 0 else width - LANES, LANES)
                corner_packs[2 * i + side] = merge(
                    [
                        own[c, g, pl.ds(first + SUBLANES * b, SUBLANES), cols]
                        for c in range(fields) for b in range(turn)
                    ],
                    side,
                )

    pl.semaphore_wait(barrier, nlon - 1 + 4 * nlon)

    @pl.when(k < last)
    def _():
        for copy in pack_copies(0) + row_copies() + corner_copies() + pack_copies(1):
            copy.start()

    for c in range(chunks):
        next_copy(c).start()

    def edge_blocks(numbers, corner):
        @pl.loop(0, fields)
        def _(c):
            def put(r, g, value):
                state[c, groups, strided(r + PAD, g), :] = value

            for i in numbers:
                right, left = got_packed[0, c, place_of(i)], got_packed[1, c, place_of(i)]
                for g in range(SUBLANES):
                    value = join(right, left, g)
                    r = SUBLANES * i
                    put(r, g, value)
                    if r >= span - PAD and g < SUBLANES - 1:
                        put(r - span, g + 1, value)
                    if r < PAD and g > 0:
                        put(r + span, g - 1, value)

        for c in range(fields):
            for b in range(turn):
                value = join(corners[2 * corner], corners[2 * corner + 1], c * turn + b)
                g, r = ((0, -PAD), (SUBLANES - 1, span))[corner]
                state[c, groups, strided(r + SUBLANES * b + PAD, g), :] = value

    early_blocks = [i for i in range(blocks_of_span) if place_of(i) < early]
    late_blocks = [i for i in range(blocks_of_span) if place_of(i) >= early]

    def late_edges():
        for i in range(2):
            landed(got_packed.at[i, :, pl.ds(early, blocks_of_span - early)], pack_recv.at[1, i])
            landed(corners.at[2 + i], corner_recv.at[2 + i])
        edge_blocks(late_blocks, 1)

    @pl.when(k < last)
    def _():
        coriolis_rows()
        landed(top, rows_recv.at[0])
        landed(bot, rows_recv.at[1])

        @pl.loop(0, fields)
        def _(c):
            for j in range(groups):
                cols = pl.ds(j * LANES, LANES)

                def put(at, value):
                    state[c, j, at, :] = value

                spread(
                    put,
                    lambda r: top[c, pl.ds(r, SUBLANES), cols],
                    lambda g, r: own[c, g, pl.ds(r, SUBLANES), cols],
                    lambda r: bot[c, pl.ds(r, SUBLANES), cols],
                )

        for i in range(2):
            landed(got_packed.at[i, :, pl.ds(0, early)], pack_recv.at[0, i])
            landed(corners.at[i], corner_recv.at[i])
        edge_blocks(early_blocks, 0)

    @pl.when(k == last)
    def _():
        for copy in own_copies(back_hbm):
            copy.wait()

    def spread_scales():
        wpad[...] = jnp.zeros_like(wpad)
        wpad[0:fields, 0 : half + 1] = w_ref[...]
        depth = wpad.shape[1]
        parts, rest = [], wpad[...]
        for _ in range(3):
            part = rest.astype(jnp.bfloat16).astype(jnp.float32)
            parts.append(part)
            rest = rest - part
        parts = jnp.concatenate(parts + [jnp.zeros_like(rest)], axis=0).astype(jnp.bfloat16)
        at = lax.broadcasted_iota(jnp.int32, (LANES, length), 1)
        row = lax.broadcasted_iota(jnp.int32, (LANES, length), 0)
        eighth = quarter // 2
        fours = 4 * jnp.where(at <= eighth, at, at - eighth)
        twos = 4 * lax.rem(at, eighth) + 2
        odds = 2 * lax.rem(at, quarter) + 1
        number = jnp.where(at < quarter, fours, jnp.where(at < half, twos, odds))
        total = jnp.zeros((parts.shape[0], length), jnp.float32)
        for b in range(depth // LANES):
            chosen = jnp.where(number == row + b * LANES, 1.0, 0.0).astype(jnp.bfloat16)
            total += jnp.dot(
                parts[:, b * LANES : (b + 1) * LANES], chosen, preferred_element_type=jnp.float32
            )
        line = total[0:8] + (total[8:16] + total[16:24])
        rows = per * CHUNK
        for c in range(fields):
            scales[c * rows : (c + 1) * rows, :] = jnp.broadcast_to(line[c : c + 1, :], (rows, length))

    at_first = lax.broadcasted_iota(jnp.int32, (BLOCK, SUBLANES, LANES), 2) == 0
    at_last = lax.broadcasted_iota(jnp.int32, (BLOCK, SUBLANES, LANES), 2) == LANES - 1

    def beside(parts):
        ahead = [pltpu.roll(q, LANES - 1, 2) for q in parts]
        behind = [pltpu.roll(q, 1, 2) for q in parts]
        return [
            (
                jnp.where(at_last, ahead[(j + 1) % ring], ahead[j]),
                jnp.where(at_first, behind[(j - 1) % ring], behind[j]),
            )
            for j in range(ring)
        ]

    def stage(arg, base, out, keep, mix, gain, start, blocks):
        @pl.loop(0, blocks)
        def _(i):
            r0 = start + i * BLOCK
            wide = pl.ds(pl.multiple_of(SUBLANES * (r0 - 1), SUBLANES), SUBLANES * (BLOCK + 2))
            at = pl.ds(pl.multiple_of(SUBLANES * r0, SUBLANES), SUBLANES * BLOCK)
            h, u, v = [
                [arg[c, j, wide, :].reshape(BLOCK + 2, SUBLANES, LANES) for j in range(ring)]
                for c in range(3)
            ]
            f2 = frows[at, :].reshape(BLOCK, SUBLANES, LANES)
            hm, um, vm = [[q[1:-1] for q in field] for field in (h, u, v)]

            def along(q):
                return q[2:] - q[:-2]

            h_by, u_by, v_by = beside(hm), beside(um), beside(vm)
            for j in range(ring):
                (h1, h0), (u1, u0), (v1, v0) = h_by[j], u_by[j], v_by[j]
                dv = v[j] + h[j] * v[j]
                rate_h = (u1 + h1 * u1) - (u0 + h0 * u0) + along(dv)
                rate_u = um[j] * (u1 - u0) + vm[j] * along(u[j]) + (h1 - h0) - f2 * vm[j]
                rate_v = um[j] * (v1 - v0) + vm[j] * along(v[j]) + along(h[j]) + f2 * um[j]
                for c, (m, rate) in enumerate(((hm[j], rate_h), (um[j], rate_u), (vm[j], rate_v))):
                    if base is None:
                        value = m - gain * rate
                    else:
                        old = base[c, j, at, :].reshape(BLOCK, SUBLANES, LANES)
                        value = keep * old + mix * m - gain * rate
                    out[c, j, at, :] = value.reshape(SUBLANES * BLOCK, LANES)

    def forecast(c):
        def bounds(t):
            ahead = stages - t
            fill = 2 * ahead + BLOCK - 1
            first = c * CHUNK + ahead
            extra = jnp.where(c == 0, fill - lax.rem(fill, BLOCK), 0)
            return PAD + first - extra, (CHUNK + extra) // BLOCK

        half_step = 0.5 * time_step

        @pl.loop(0, STEPS)
        def _(step):
            stage(state, None, mid1, 0.0, 1.0, half_step, *bounds(3 * step + 1))
            stage(mid1, state, mid2, 0.75, 0.25, 0.25 * half_step, *bounds(3 * step + 2))
            stage(mid2, state, state, 1.0 / 3.0, 2.0 / 3.0, 2.0 / 3.0 * half_step, *bounds(3 * step + 3))

    def filtered(c):
        for s in range(nlon):
            landed(slab.at[:, :, rows_of(c), pl.ds(s * width, width)], in_recv.at[c, s])
        rows = fields * per * CHUNK

        def product(value, way, place):
            high, low = split_parts(value)
            both = jnp.concatenate([high, low], axis=0)
            twice = jnp.dot(both, waves_ref[(way, 0) + place], preferred_element_type=jnp.float32)
            rest = jnp.dot(high, waves_ref[(way, 1) + place], preferred_element_type=jnp.float32)
            return twice[:rows] + (twice[rows:] + rest)

        value = slab[:, :, rows_of(c), :].reshape(rows, length)
        left, right = value[:, :half], value[:, half:]
        even, odd = left + right, left - right
        places = (
            (slice(0, quarter), slice(0, quarter)),
            (slice(0, quarter), slice(quarter, half)),
            (slice(quarter, quarter + half), slice(0, half)),
        )
        inputs = (even[:, :quarter] + even[:, quarter:], even[:, :quarter] - even[:, quarter:], odd)
        at, outputs = 0, []
        for place, mix in zip(places, inputs):
            count = mix.shape[1]
            coefficients = product(mix, 0, place) * scales[:, at : at + count]
            outputs.append(product(coefficients, 1, place))
            at += count
        fours, twos, odds = outputs
        for first, even in ((0, fours + twos), (quarter, fours - twos)):
            part = odds[:, first : first + quarter]
            for start, result in ((first, even + part), (first + half, even - part)):
                y_own[:, :, rows_of(c), start : start + quarter] = result.reshape(
                    fields, per, CHUNK, quarter
                )

        @pl.when(c < chunks)
        def _():
            for d in order:
                homeward(c, d).start()

        @pl.when(c == chunks)
        def _():
            for d in order:
                homeward(chunks, d, chunks - 1).start()

    def send_defects(c):
        for d in order:
            inward(c, d).start()

    @pl.when(k == last)
    def _():
        @pl.loop(0, chunks)
        def _(c):
            landed(following.at[:, :, rows_of(c), :], next_recv.at[c])

            @pl.loop(0, fields)
            def _(field):
                following[field, :, rows_of(c), :] = (
                    following[field, :, rows_of(c), :] - own[field, :, rows_of(c), :]
                )

            send_defects(c)

        spread_scales()
        waves_copy.wait()

    @pl.when(k < last)
    def _():
        @pl.loop(0, chunks)
        def _(c):
            forecast(c)
            landed(following.at[:, :, rows_of(c), :], next_recv.at[c])

            @pl.loop(0, fields)
            def _(field):
                for g in range(SUBLANES):
                    at = pl.ds(SUBLANES * (c * CHUNK + PAD) + g, CHUNK, stride=SUBLANES)
                    for j in range(groups):
                        cols = pl.ds(j * LANES, LANES)
                        following[field, g, rows_of(c), cols] = (
                            following[field, g, rows_of(c), cols] - state[field, j, at, :]
                        )

            passes = (k == giver) & (c == chunks - 1)

            @pl.when(passes)
            def _():
                relay().start()

            @pl.when(jnp.logical_not(passes))
            def _():
                send_defects(c)

            @pl.when(c == 0)
            def _():
                late_edges()
                spread_scales()
                waves_copy.wait()

            @pl.when(c >= LAG)
            def _():
                filtered(c - LAG)

    handled = chunks + (k == taker).astype(jnp.int32) - (k == giver).astype(jnp.int32)

    @pl.loop(jnp.where(k == last, 0, chunks - LAG), handled)
    def _(c):
        filtered(c)

        @pl.when((k == taker) & (c == chunks - LAG))
        def _():
            landed(relayed, relay_recv)
            for d in order:
                inward(chunks, d, relayed).start()

    @pl.loop(0, chunks)
    def _(c):
        for s in range(nlon):
            landed(out_hbm.at[:, pl.ds(s * per, per), rows_of(c), :], out_recv.at[c, s])
        next_copy(c).wait_send()

    @pl.loop(0, handled)
    def _(c):
        for d in range(1, nlon):
            inward(c, d, relayed).wait_send()
            homeward(c, d, 0).wait_send()

        @pl.when(c < chunks)
        def _():
            homeward(c, 0).wait_send()

    @pl.when(k == giver)
    def _():
        relay().wait_send()

    @pl.when(k < last)
    def _():
        for copy in row_copies() + corner_copies() + pack_copies(0) + pack_copies(1):
            copy.wait_send()


def solution(mesh):
    nsub, nlat, nlon = mesh.shape["sub"], mesh.shape["lat"], mesh.shape["lon"]

    def shards(launch, backdrop, inverse_variances):
        fields, lat_rows, width = backdrop.shape
        length = width * nlon
        half = length // 2
        span = lat_rows // SUBLANES
        chunks = span // CHUNK
        per = SUBLANES // nlon
        ring = width // LANES + 1
        natural = (fields, SUBLANES, span, width)
        f32, bf16 = jnp.float32, jnp.bfloat16
        dma = pltpu.SemaphoreType.DMA
        any_space = pl.BlockSpec(memory_space=pl.ANY)
        vmem = pl.BlockSpec(memory_space=pltpu.VMEM)
        spread_rows = SUBLANES * (span + 2 * PAD)
        corner_like = pltpu.VMEM((4, SUBLANES, LANES), f32)
        pack_like = pltpu.VMEM((2, fields, span // SUBLANES, SUBLANES, LANES), f32)
        rows_like = pltpu.VMEM((fields, ring, spread_rows, LANES), f32)
        slab_like = pltpu.VMEM((fields, per, span + CHUNK, length), f32)
        out = pl.pallas_call(
            lambda *refs: kernel(nsub, nlat, nlon, *refs),
            name="weighted_defects",
            out_shape=jax.ShapeDtypeStruct(natural, f32),
            in_specs=[any_space, any_space, vmem, any_space],
            out_specs=any_space,
            scratch_shapes=[
                pltpu.VMEM((2, 2, half + half // 2, half), bf16),
                pltpu.VMEM((8, half + LANES), f32),
                pltpu.VMEM((fields * per * CHUNK, length), f32),
                pltpu.VMEM((spread_rows, LANES), f32),
                pltpu.VMEM(natural, f32),
                pltpu.VMEM((fields, PAD, width), f32),
                pltpu.VMEM((fields, PAD, width), f32),
                corner_like, corner_like, pack_like, pack_like,
                pltpu.VMEM(natural, f32),
                pltpu.VMEM((fields, SUBLANES, CHUNK, width), f32),
                slab_like, slab_like,
                rows_like, rows_like, rows_like,
                dma, dma((fields,)),
                dma((2,)), dma((2,)), dma((4,)), dma((4,)), dma((2, 2)), dma((2, 2)),
                dma((chunks,)), dma((chunks,)), dma, dma,
                dma((chunks + 1, nlon)), dma((chunks + 1, nlon)),
                dma((chunks + 1, nlon)), dma((chunks, nlon)),
            ],
            compiler_params=pltpu.CompilerParams(collective_id=0, has_side_effects=True, vmem_limit_bytes=VMEM_LIMIT),
        )(
            launch.reshape(natural), backdrop.reshape(natural), inverse_variances,
            jnp.asarray(waves(length)),
        )
        return out.reshape(launch.shape)

    return jax.shard_map(
        shards,
        mesh=mesh,
        in_specs=(P("sub", None, "lat", "lon"), P(None, "lat", "lon"), P()),
        out_specs=P("sub", None, "lat", "lon"),
        check_vma=False,
    )
```

```python
import numpy as np
import jax
import jax.numpy as jnp
from jax import lax
from jax.experimental import pallas as pl
from jax.experimental.pallas import tpu as pltpu
from jax.sharding import PartitionSpec as P

STEPS = 3
PAD = 16
EDGE = 16
SUBLANES = 8
LANES = 128
CHUNK = 8
BLOCK = 4
LAG = 3
EXTRA = 5
VMEM_LIMIT = 52 * 2**20
MESH = pl.DeviceIdType.MESH

time_step = 0.5
coriolis_peak = 0.4


def waves(length):
    half, quarter = length // 2, length // 4

    def basis(points, pairs):
        n = np.arange(points)
        columns = []
        for turn, numbers in pairs:
            for m in numbers:
                scale = np.sqrt((1.0 if m in (0, half) else 2.0) / length)
                columns.append(scale * turn(2.0 * np.pi / length * ((m * n) % length)))
        return np.stack(columns, axis=1)

    fours = basis(quarter, ((np.cos, range(0, half + 1, 4)), (np.sin, range(4, half, 4))))
    twos = basis(quarter, ((np.cos, range(2, half, 4)), (np.sin, range(2, half, 4))))
    odds = basis(half, ((np.cos, range(1, half, 2)), (np.sin, range(1, half, 2))))
    out = np.stack([
        np.concatenate([np.concatenate([e, t], axis=1), o], axis=0)
        for e, t, o in ((fours, twos, odds), (fours.T, twos.T, odds.T))
    ]).astype(np.float32)
    high = out.astype(jnp.bfloat16)
    return np.stack([high, (out - high.astype(np.float32)).astype(jnp.bfloat16)], axis=1)


def split_parts(value):
    high = value.astype(jnp.bfloat16)
    return high, (value - high.astype(jnp.float32)).astype(jnp.bfloat16)


def kernel(
    nsub, nlat, nlon, x_hbm, back_hbm, w_ref, waves_hbm, out_hbm,
    waves_ref, wpad, scales, frows, own, top, bot, corners,
    corner_packs, packed, got_packed, following, extra, slab, y_own, state, mid1, mid2,
    waves_sem, own_sem, extra_sem, rows_send, rows_recv, corner_send, corner_recv,
    pack_send, pack_recv, next_send, next_recv, relay_send, relay_recv, in_send, in_recv, out_send, out_recv,
):
    k = lax.axis_index("sub")
    a = lax.axis_index("lat")
    z = lax.axis_index("lon")
    fields, _, span, width = x_hbm.shape
    length = width * nlon
    half = length // 2
    quarter = length // 4
    groups = width // LANES
    ring = groups + 1
    chunks = span // CHUNK
    per = SUBLANES // nlon
    stages = 3 * STEPS
    k_up = lax.rem(k + 1, nsub)
    k_down = lax.rem(k + nsub - 1, nsub)
    a_up = lax.rem(a + 1, nlat)
    a_down = lax.rem(a + nlat - 1, nlat)
    z_up = lax.rem(z + 1, nlon)
    z_down = lax.rem(z + nlon - 1, nlon)
    last = nsub - 1
    giver, taker = (last - 2, last - 1) if nsub > 2 else (-1, -1)
    kept = chunks - EXTRA
    is_giver, is_taker = (k == giver).astype(jnp.int32), (k == taker).astype(jnp.int32)
    is_first, is_last = (k == 0).astype(jnp.int32), (k == last).astype(jnp.int32)
    n_own = chunks - EXTRA * (is_giver + is_last)
    n_extra = EXTRA * (is_taker + is_first)

    barrier = pltpu.get_barrier_semaphore()
    for d in range(1, nlon):
        pl.semaphore_signal(
            barrier, inc=1, device_id=(k, a, lax.rem(z + d, nlon)), device_id_type=MESH
        )
    for d in range(nlon):
        for there in ((k, a_up), (k, a_down), (k_up, a), (k_down, a)):
            pl.semaphore_signal(barrier, inc=1, device_id=there + (jnp.int32(d),), device_id_type=MESH)

    mine = pl.ds(pl.multiple_of(z * width, width), width)

    def local(src, dst, sem):
        return pltpu.make_async_copy(src, dst, sem)

    def remote(src, dst, send, recv, there):
        return pltpu.make_async_remote_copy(
            src_ref=src, dst_ref=dst, send_sem=send, recv_sem=recv,
            device_id=there, device_id_type=MESH,
        )

    def landed(block, sem):
        local(block, block, sem).wait()

    low_rows, high_rows = pl.ds(0, PAD), pl.ds(span - PAD, PAD)
    first_lanes, last_lanes = pl.ds(0, LANES), pl.ds(width - LANES, LANES)

    def row_copies():
        return [
            remote(x_hbm.at[:, SUBLANES - 1, high_rows, :], top, rows_send.at[0], rows_recv.at[0], (k, a_up, z)),
            remote(x_hbm.at[:, 0, low_rows, :], bot, rows_send.at[1], rows_recv.at[1], (k, a_down, z)),
        ]

    def corner_copies():
        return [
            remote(
                corner_packs.at[2 * i + j], corners.at[2 * i + j],
                corner_send.at[2 * i + j], corner_recv.at[2 * i + j], (k, lat, lon),
            )
            for i, lat in enumerate((a_up, a_down)) for j, lon in enumerate((z_down, z_up))
        ]

    blocks_of_span = span // SUBLANES
    early = blocks_of_span // 2 + 1
    turn = PAD // SUBLANES

    def place_of(i):
        return (i + turn) % blocks_of_span

    def pack_copies(part):
        at = pl.ds(0, early) if part == 0 else pl.ds(early, blocks_of_span - early)
        return [
            remote(
                packed.at[i, :, at], got_packed.at[i, :, at],
                pack_send.at[part, i], pack_recv.at[part, i], (k, a, lon),
            )
            for i, lon in enumerate((z_down, z_up))
        ]

    def rows_of(c):
        return pl.ds(pl.multiple_of(c * CHUNK, CHUNK), CHUNK)

    def next_copy(c):
        return remote(
            x_hbm.at[:, :, rows_of(c), :], following.at[:, :, rows_of(c), :],
            next_send.at[c], next_recv.at[c], (k_down, a, z),
        )

    def inward(c, d, extras=False):
        zt = lax.rem(z + d, nlon)
        block = extra.at[:, :, rows_of(c - chunks), :] if extras else following.at[:, :, rows_of(c), :]
        src = block.at[:, pl.ds(zt * per, per)]
        dst = slab.at[:, :, rows_of(c), mine]
        if d == 0:
            return local(src, dst, in_recv.at[c, z])
        return remote(src, dst, in_send.at[c, d], in_recv.at[c, z], (k, a, zt))

    def relay(e):
        return remote(
            following.at[:, :, rows_of(kept + e), :], extra.at[:, :, rows_of(e), :],
            relay_send.at[e], relay_recv.at[e], (k_up, a, z),
        )

    def homeward(c, d, extras=False):
        zt = lax.rem(z + d, nlon)
        home = c - EXTRA if extras else c
        src = y_own.at[:, :, rows_of(c), pl.ds(pl.multiple_of(zt * width, width), width)]
        dst = out_hbm.at[:, pl.ds(z * per, per), rows_of(home), :]
        if extras and d == 0:
            return local(src, dst, out_recv.at[home, z])
        return remote(
            src, dst, out_send.at[c, d], out_recv.at[home, z], (k if extras else k_up, a, zt)
        )

    order = list(range(1, nlon)) + [0]

    def own_copies(src):
        return [local(src.at[c], own.at[c], own_sem.at[c]) for c in range(fields)]

    @pl.when(k < last)
    def _():
        for copy in own_copies(x_hbm):
            copy.start()

    @pl.when(k == last)
    def _():
        for copy in own_copies(back_hbm):
            copy.start()

    extra_copy = local(back_hbm.at[:, :, pl.ds(kept * CHUNK, EXTRA * CHUNK), :], extra, extra_sem)

    @pl.when(k == 0)
    def _():
        extra_copy.start()

    waves_copy = local(waves_hbm, waves_ref, waves_sem)
    waves_copy.start()

    lane = lax.broadcasted_iota(jnp.int32, (SUBLANES, LANES), 1)

    def strided(r, g):
        return pl.ds(SUBLANES * r + g, SUBLANES, stride=SUBLANES)

    def spread(put, low, main, high):
        for g in range(SUBLANES):
            for b in range((span + 2 * PAD) // SUBLANES):
                r = b * SUBLANES - PAD
                if r < 0:
                    value = low(r + PAD) if g == 0 else main(g - 1, span + r)
                elif r >= span:
                    value = high(r - span) if g == SUBLANES - 1 else main(g + 1, r - span)
                else:
                    value = main(g, r)
                put(strided(b * SUBLANES, g), value)

    def coriolis_rows():
        total = nlat * SUBLANES * span
        group = lax.broadcasted_iota(jnp.int32, (SUBLANES, LANES), 0)
        for first in range(0, span + 2 * PAD, LANES):
            row = a * (SUBLANES * span) + group * span + lane + (first - PAD)
            row = lax.rem(row + total, total).astype(jnp.float32)
            line = (2.0 * coriolis_peak) * jnp.sin((2.0 * np.pi / total) * (row + 0.5))
            for r in range(first, min(first + LANES, span + 2 * PAD)):
                frows[SUBLANES * r : SUBLANES * (r + 1), :] = jnp.broadcast_to(
                    line[:, r - first : r - first + 1], (SUBLANES, LANES)
                )

    def merge(parts, side):
        step = EDGE
        while len(parts) > 1:
            merged = []
            for i in range(0, len(parts) - 1, 2):
                if side == 0:
                    far = pltpu.roll(parts[i + 1], step, 1)
                    merged.append(jnp.where(lanes_of(far) < step, parts[i], far))
                else:
                    far = pltpu.roll(parts[i + 1], LANES - step, 1)
                    merged.append(jnp.where(lanes_of(far) >= LANES - step, parts[i], far))
            if len(parts) % 2:
                merged.append(parts[-1])
            parts, step = merged, 2 * step
        return parts[0]

    def lanes_of(value):
        return lax.broadcasted_iota(jnp.int32, value.shape, len(value.shape) - 1)

    def join(right, left, slot):
        shift = EDGE * slot
        near = pltpu.roll(right, LANES - shift, 1) if slot else right
        far = pltpu.roll(left, shift, 1) if slot else left
        return jnp.where(lane < EDGE, near, jnp.where(lane >= LANES - EDGE, far, 0.0))

    ends = ((SUBLANES - 1, span - PAD), (0, 0))

    @pl.when(k < last)
    def _():
        for copy in own_copies(x_hbm):
            copy.wait()

        @pl.loop(0, fields)
        def _(c):
            for side in range(2):
                cols = pl.ds(0 if side == 0 else width - LANES, LANES)
                whole = merge([own[c, g, :, cols] for g in range(SUBLANES)], side)
                for i in range(blocks_of_span):
                    packed[side, c, place_of(i)] = whole[SUBLANES * i : SUBLANES * (i + 1)]

        for i, (g, first) in enumerate(ends):
            for side in range(2):
                cols = pl.ds(0 if side == 0 else width - LANES, LANES)
                corner_packs[2 * i + side] = merge(
                    [
                        own[c, g, pl.ds(first + SUBLANES * b, SUBLANES), cols]
                        for c in range(fields) for b in range(turn)
                    ],
                    side,
                )

    @pl.when(k == 0)
    def _():
        extra_copy.wait()

        @pl.loop(0, fields)
        def _(c):
            extra[c] = own[c, :, pl.ds(kept * CHUNK, EXTRA * CHUNK), :] - extra[c]

    pl.semaphore_wait(barrier, nlon - 1 + 4 * nlon)

    @pl.when(k < last)
    def _():
        for copy in pack_copies(0) + row_copies() + corner_copies() + pack_copies(1):
            copy.start()

    for c in range(kept):
        next_copy(c).start()

    @pl.when(k > 0)
    def _():
        for c in range(kept, chunks):
            next_copy(c).start()

    @pl.when(k == 0)
    def _():
        @pl.loop(0, EXTRA)
        def _(e):
            for d in order:
                inward(chunks + e, d, True).start()

    def edge_blocks(numbers, corner):
        @pl.loop(0, fields)
        def _(c):
            def put(r, g, value):
                state[c, groups, strided(r + PAD, g), :] = value

            for i in numbers:
                right, left = got_packed[0, c, place_of(i)], got_packed[1, c, place_of(i)]
                for g in range(SUBLANES):
                    value = join(right, left, g)
                    r = SUBLANES * i
                    put(r, g, value)
                    if r >= span - PAD and g < SUBLANES - 1:
                        put(r - span, g + 1, value)
                    if r < PAD and g > 0:
                        put(r + span, g - 1, value)

        for c in range(fields):
            for b in range(turn):
                value = join(corners[2 * corner], corners[2 * corner + 1], c * turn + b)
                g, r = ((0, -PAD), (SUBLANES - 1, span))[corner]
                state[c, groups, strided(r + SUBLANES * b + PAD, g), :] = value

    early_blocks = [i for i in range(blocks_of_span) if place_of(i) < early]
    late_blocks = [i for i in range(blocks_of_span) if place_of(i) >= early]

    def late_edges():
        for i in range(2):
            landed(got_packed.at[i, :, pl.ds(early, blocks_of_span - early)], pack_recv.at[1, i])
            landed(corners.at[2 + i], corner_recv.at[2 + i])
        edge_blocks(late_blocks, 1)

    @pl.when(k < last)
    def _():
        coriolis_rows()
        landed(top, rows_recv.at[0])
        landed(bot, rows_recv.at[1])

        @pl.loop(0, fields)
        def _(c):
            for j in range(groups):
                cols = pl.ds(j * LANES, LANES)

                def put(at, value):
                    state[c, j, at, :] = value

                spread(
                    put,
                    lambda r: top[c, pl.ds(r, SUBLANES), cols],
                    lambda g, r: own[c, g, pl.ds(r, SUBLANES), cols],
                    lambda r: bot[c, pl.ds(r, SUBLANES), cols],
                )

        for i in range(2):
            landed(got_packed.at[i, :, pl.ds(0, early)], pack_recv.at[0, i])
            landed(corners.at[i], corner_recv.at[i])
        edge_blocks(early_blocks, 0)

    @pl.when(k == last)
    def _():
        for copy in own_copies(back_hbm):
            copy.wait()

    def spread_scales():
        wpad[...] = jnp.zeros_like(wpad)
        wpad[0:fields, 0 : half + 1] = w_ref[...]
        depth = wpad.shape[1]
        parts, rest = [], wpad[...]
        for _ in range(3):
            part = rest.astype(jnp.bfloat16).astype(jnp.float32)
            parts.append(part)
            rest = rest - part
        parts = jnp.concatenate(parts + [jnp.zeros_like(rest)], axis=0).astype(jnp.bfloat16)
        at = lax.broadcasted_iota(jnp.int32, (LANES, length), 1)
        row = lax.broadcasted_iota(jnp.int32, (LANES, length), 0)
        eighth = quarter // 2
        fours = 4 * jnp.where(at <= eighth, at, at - eighth)
        twos = 4 * lax.rem(at, eighth) + 2
        odds = 2 * lax.rem(at, quarter) + 1
        number = jnp.where(at < quarter, fours, jnp.where(at < half, twos, odds))
        total = jnp.zeros((parts.shape[0], length), jnp.float32)
        for b in range(depth // LANES):
            chosen = jnp.where(number == row + b * LANES, 1.0, 0.0).astype(jnp.bfloat16)
            total += jnp.dot(
                parts[:, b * LANES : (b + 1) * LANES], chosen, preferred_element_type=jnp.float32
            )
        line = total[0:8] + (total[8:16] + total[16:24])
        rows = per * CHUNK
        for c in range(fields):
            scales[c * rows : (c + 1) * rows, :] = jnp.broadcast_to(line[c : c + 1, :], (rows, length))

    at_first = lax.broadcasted_iota(jnp.int32, (BLOCK, SUBLANES, LANES), 2) == 0
    at_last = lax.broadcasted_iota(jnp.int32, (BLOCK, SUBLANES, LANES), 2) == LANES - 1

    def beside(parts):
        ahead = [pltpu.roll(q, LANES - 1, 2) for q in parts]
        behind = [pltpu.roll(q, 1, 2) for q in parts]
        return [
            (
                jnp.where(at_last, ahead[(j + 1) % ring], ahead[j]),
                jnp.where(at_first, behind[(j - 1) % ring], behind[j]),
            )
            for j in range(ring)
        ]

    def stage(arg, base, out, keep, mix, gain, start, blocks):
        @pl.loop(0, blocks)
        def _(i):
            r0 = start + i * BLOCK
            wide = pl.ds(pl.multiple_of(SUBLANES * (r0 - 1), SUBLANES), SUBLANES * (BLOCK + 2))
            at = pl.ds(pl.multiple_of(SUBLANES * r0, SUBLANES), SUBLANES * BLOCK)
            h, u, v = [
                [arg[c, j, wide, :].reshape(BLOCK + 2, SUBLANES, LANES) for j in range(ring)]
                for c in range(3)
            ]
            f2 = frows[at, :].reshape(BLOCK, SUBLANES, LANES)
            hm, um, vm = [[q[1:-1] for q in field] for field in (h, u, v)]

            def along(q):
                return q[2:] - q[:-2]

            h_by, u_by, v_by = beside(hm), beside(um), beside(vm)
            for j in range(ring):
                (h1, h0), (u1, u0), (v1, v0) = h_by[j], u_by[j], v_by[j]
                dv = v[j] + h[j] * v[j]
                rate_h = (u1 + h1 * u1) - (u0 + h0 * u0) + along(dv)
                rate_u = um[j] * (u1 - u0) + vm[j] * along(u[j]) + (h1 - h0) - f2 * vm[j]
                rate_v = um[j] * (v1 - v0) + vm[j] * along(v[j]) + along(h[j]) + f2 * um[j]
                for c, (m, rate) in enumerate(((hm[j], rate_h), (um[j], rate_u), (vm[j], rate_v))):
                    if base is None:
                        value = m - gain * rate
                    else:
                        old = base[c, j, at, :].reshape(BLOCK, SUBLANES, LANES)
                        value = keep * old + mix * m - gain * rate
                    out[c, j, at, :] = value.reshape(SUBLANES * BLOCK, LANES)

    def forecast(c):
        def bounds(t):
            ahead = stages - t
            fill = 2 * ahead + BLOCK - 1
            first = c * CHUNK + ahead
            extra = jnp.where(c == 0, fill - lax.rem(fill, BLOCK), 0)
            return PAD + first - extra, (CHUNK + extra) // BLOCK

        half_step = 0.5 * time_step

        @pl.loop(0, STEPS)
        def _(step):
            stage(state, None, mid1, 0.0, 1.0, half_step, *bounds(3 * step + 1))
            stage(mid1, state, mid2, 0.75, 0.25, 0.25 * half_step, *bounds(3 * step + 2))
            stage(mid2, state, state, 1.0 / 3.0, 2.0 / 3.0, 2.0 / 3.0 * half_step, *bounds(3 * step + 3))

    def filtered(c):
        for s in range(nlon):
            landed(slab.at[:, :, rows_of(c), pl.ds(s * width, width)], in_recv.at[c, s])
        rows = fields * per * CHUNK

        def product(value, way, place):
            high, low = split_parts(value)
            both = jnp.concatenate([high, low], axis=0)
            twice = jnp.dot(both, waves_ref[(way, 0) + place], preferred_element_type=jnp.float32)
            rest = jnp.dot(high, waves_ref[(way, 1) + place], preferred_element_type=jnp.float32)
            return twice[:rows] + (twice[rows:] + rest)

        value = slab[:, :, rows_of(c), :].reshape(rows, length)
        left, right = value[:, :half], value[:, half:]
        even, odd = left + right, left - right
        places = (
            (slice(0, quarter), slice(0, quarter)),
            (slice(0, quarter), slice(quarter, half)),
            (slice(quarter, quarter + half), slice(0, half)),
        )
        inputs = (even[:, :quarter] + even[:, quarter:], even[:, :quarter] - even[:, quarter:], odd)
        at, outputs = 0, []
        for place, mix in zip(places, inputs):
            count = mix.shape[1]
            coefficients = product(mix, 0, place) * scales[:, at : at + count]
            outputs.append(product(coefficients, 1, place))
            at += count
        fours, twos, odds = outputs
        for first, even in ((0, fours + twos), (quarter, fours - twos)):
            part = odds[:, first : first + quarter]
            for start, result in ((first, even + part), (first + half, even - part)):
                y_own[:, :, rows_of(c), start : start + quarter] = result.reshape(
                    fields, per, CHUNK, quarter
                )

        @pl.when(c < chunks)
        def _():
            for d in order:
                homeward(c, d).start()

        @pl.when(c >= chunks)
        def _():
            for d in order:
                homeward(c, d, True).start()

    def send_defects(c):
        for d in order:
            inward(c, d).start()

    def pass_on(e):
        landed(extra.at[:, :, rows_of(e), :], relay_recv.at[e])
        for d in order:
            inward(chunks + e, d, True).start()

    @pl.when(k == last)
    def _():
        @pl.loop(0, kept)
        def _(c):
            landed(following.at[:, :, rows_of(c), :], next_recv.at[c])

            @pl.loop(0, fields)
            def _(field):
                following[field, :, rows_of(c), :] = (
                    following[field, :, rows_of(c), :] - own[field, :, rows_of(c), :]
                )

            send_defects(c)

        spread_scales()
        waves_copy.wait()

    @pl.when(k < last)
    def _():
        @pl.loop(0, chunks)
        def _(c):
            forecast(c)
            landed(following.at[:, :, rows_of(c), :], next_recv.at[c])

            @pl.loop(0, fields)
            def _(field):
                for g in range(SUBLANES):
                    at = pl.ds(SUBLANES * (c * CHUNK + PAD) + g, CHUNK, stride=SUBLANES)
                    for j in range(groups):
                        cols = pl.ds(j * LANES, LANES)
                        following[field, g, rows_of(c), cols] = (
                            following[field, g, rows_of(c), cols] - state[field, j, at, :]
                        )

            passes = (k == giver) & (c >= kept)

            @pl.when(passes)
            def _():
                relay(c - kept).start()

            @pl.when(jnp.logical_not(passes))
            def _():
                send_defects(c)

            @pl.when((k == taker) & (c > kept))
            def _():
                pass_on(c - kept - 1)

            @pl.when(c == 0)
            def _():
                late_edges()
                spread_scales()
                waves_copy.wait()

            @pl.loop(0, 2)
            def _(turn):
                slot = jnp.where(turn == 0, chunks + c, c - LAG)
                begun = ((k == 0) & (c < EXTRA)).astype(jnp.int32)
                ready = ((c >= LAG) & (c - LAG < n_own)).astype(jnp.int32)

                @pl.when(jnp.where(turn == 0, begun, ready) == 1)
                def _():
                    filtered(slot)

        @pl.when(k == taker)
        def _():
            pass_on(EXTRA - 1)

    first_slot = jnp.where(k == last, 0, jnp.minimum(n_own, chunks - LAG))

    @pl.loop(first_slot, n_own + EXTRA * is_taker)
    def _(c):
        filtered(c)

    @pl.loop(0, chunks)
    def _(c):
        for s in range(nlon):
            landed(out_hbm.at[:, pl.ds(s * per, per), rows_of(c), :], out_recv.at[c, s])

    for c in range(kept):
        next_copy(c).wait_send()

    @pl.when(k > 0)
    def _():
        for c in range(kept, chunks):
            next_copy(c).wait_send()

    @pl.loop(0, n_own)
    def _(c):
        for d in range(nlon):
            if d:
                inward(c, d).wait_send()
            homeward(c, d).wait_send()

    @pl.loop(chunks, chunks + n_extra)
    def _(c):
        for d in range(1, nlon):
            inward(c, d, True).wait_send()
            homeward(c, d, True).wait_send()

    @pl.when(k == giver)
    def _():
        for e in range(EXTRA):
            relay(e).wait_send()

    @pl.when(k < last)
    def _():
        for copy in row_copies() + corner_copies() + pack_copies(0) + pack_copies(1):
            copy.wait_send()


def solution(mesh):
    nsub, nlat, nlon = mesh.shape["sub"], mesh.shape["lat"], mesh.shape["lon"]

    def shards(launch, backdrop, inverse_variances):
        fields, lat_rows, width = backdrop.shape
        length = width * nlon
        half = length // 2
        span = lat_rows // SUBLANES
        chunks = span // CHUNK
        per = SUBLANES // nlon
        ring = width // LANES + 1
        natural = (fields, SUBLANES, span, width)
        f32, bf16 = jnp.float32, jnp.bfloat16
        dma = pltpu.SemaphoreType.DMA
        any_space = pl.BlockSpec(memory_space=pl.ANY)
        vmem = pl.BlockSpec(memory_space=pltpu.VMEM)
        spread_rows = SUBLANES * (span + 2 * PAD)
        corner_like = pltpu.VMEM((4, SUBLANES, LANES), f32)
        pack_like = pltpu.VMEM((2, fields, span // SUBLANES, SUBLANES, LANES), f32)
        rows_like = pltpu.VMEM((fields, ring, spread_rows, LANES), f32)
        slab_like = pltpu.VMEM((fields, per, span + EXTRA * CHUNK, length), f32)
        out = pl.pallas_call(
            lambda *refs: kernel(nsub, nlat, nlon, *refs),
            name="weighted_defects",
            out_shape=jax.ShapeDtypeStruct(natural, f32),
            in_specs=[any_space, any_space, vmem, any_space],
            out_specs=any_space,
            scratch_shapes=[
                pltpu.VMEM((2, 2, half + half // 2, half), bf16),
                pltpu.VMEM((8, half + LANES), f32),
                pltpu.VMEM((fields * per * CHUNK, length), f32),
                pltpu.VMEM((spread_rows, LANES), f32),
                pltpu.VMEM(natural, f32),
                pltpu.VMEM((fields, PAD, width), f32),
                pltpu.VMEM((fields, PAD, width), f32),
                corner_like, corner_like, pack_like, pack_like,
                pltpu.VMEM(natural, f32),
                pltpu.VMEM((fields, SUBLANES, EXTRA * CHUNK, width), f32),
                slab_like, slab_like,
                rows_like, rows_like, rows_like,
                dma, dma((fields,)), dma,
                dma((2,)), dma((2,)), dma((4,)), dma((4,)), dma((2, 2)), dma((2, 2)),
                dma((chunks,)), dma((chunks,)), dma((EXTRA,)), dma((EXTRA,)),
                dma((chunks + EXTRA, nlon)), dma((chunks + EXTRA, nlon)),
                dma((chunks + EXTRA, nlon)), dma((chunks, nlon)),
            ],
            compiler_params=pltpu.CompilerParams(collective_id=0, has_side_effects=True, vmem_limit_bytes=VMEM_LIMIT),
        )(
            launch.reshape(natural), backdrop.reshape(natural), inverse_variances,
            jnp.asarray(waves(length)),
        )
        return out.reshape(launch.shape)

    return jax.shard_map(
        shards,
        mesh=mesh,
        in_specs=(P("sub", None, "lat", "lon"), P(None, "lat", "lon"), P()),
        out_specs=P("sub", None, "lat", "lon"),
        check_vma=False,
    )
```

```python
import numpy as np
import jax
import jax.numpy as jnp
from jax import lax
from jax.experimental import pallas as pl
from jax.experimental.pallas import tpu as pltpu
from jax.sharding import PartitionSpec as P

STEPS = 3
PAD = 16
EDGE = 3 * STEPS
SUBLANES = 8
LANES = 128
CHUNK = 8
BLOCK = 4
LAG = 3
EXTRA = 5
VMEM_LIMIT = 52 * 2**20
MESH = pl.DeviceIdType.MESH

time_step = 0.5
coriolis_peak = 0.4


def waves(length):
    half, quarter = length // 2, length // 4

    def basis(points, pairs):
        n = np.arange(points)
        columns = []
        for turn, numbers in pairs:
            for m in numbers:
                scale = np.sqrt((1.0 if m in (0, half) else 2.0) / length)
                columns.append(scale * turn(2.0 * np.pi / length * ((m * n) % length)))
        return np.stack(columns, axis=1)

    fours = basis(quarter, ((np.cos, range(0, half + 1, 4)), (np.sin, range(4, half, 4))))
    twos = basis(quarter, ((np.cos, range(2, half, 4)), (np.sin, range(2, half, 4))))
    odds = basis(half, ((np.cos, range(1, half, 2)), (np.sin, range(1, half, 2))))
    out = np.stack([
        np.concatenate([np.concatenate([e, t], axis=1), o], axis=0)
        for e, t, o in ((fours, twos, odds), (fours.T, twos.T, odds.T))
    ]).astype(np.float32)
    high = out.astype(jnp.bfloat16)
    return np.stack([high, (out - high.astype(np.float32)).astype(jnp.bfloat16)], axis=1)


def split_parts(value):
    high = value.astype(jnp.bfloat16)
    return high, (value - high.astype(jnp.float32)).astype(jnp.bfloat16)


def kernel(
    nsub, nlat, nlon, x_hbm, back_hbm, w_hbm, waves_hbm, out_hbm,
    waves_ref, w_ref, wpad, scales, frows, own, top, bot, corners,
    corner_packs, packed, got_packed, following, extra, slab, y_own, state, mid1, mid2,
    waves_sem, w_sem, own_sem, extra_sem, rows_send, rows_recv, corner_send, corner_recv,
    pack_send, pack_recv, next_send, next_recv, part_send, part_recv, relay_send, relay_recv, in_send, in_recv, out_send, out_recv,
):
    k = lax.axis_index("sub")
    a = lax.axis_index("lat")
    z = lax.axis_index("lon")
    fields, _, span, width = x_hbm.shape
    length = width * nlon
    half = length // 2
    quarter = length // 4
    groups = width // LANES
    ring = groups + 1
    chunks = span // CHUNK
    per = SUBLANES // nlon
    stages = 3 * STEPS
    k_up = lax.rem(k + 1, nsub)
    k_down = lax.rem(k + nsub - 1, nsub)
    a_up = lax.rem(a + 1, nlat)
    a_down = lax.rem(a + nlat - 1, nlat)
    z_up = lax.rem(z + 1, nlon)
    z_down = lax.rem(z + nlon - 1, nlon)
    last = nsub - 1
    giver, taker = (last - 2, last - 1) if nsub > 2 else (-1, -1)
    kept = chunks - EXTRA
    is_giver, is_taker = (k == giver).astype(jnp.int32), (k == taker).astype(jnp.int32)
    is_first, is_last = (k == 0).astype(jnp.int32), (k == last).astype(jnp.int32)
    n_own = chunks - EXTRA * (is_giver + is_last)
    n_extra = EXTRA * (is_taker + is_first)

    barrier = pltpu.get_barrier_semaphore()
    for d in range(1, nlon):
        pl.semaphore_signal(
            barrier, inc=1, device_id=(k, a, lax.rem(z + d, nlon)), device_id_type=MESH
        )
    for there in ((k_up, a, z), (k_down, a, z)) + tuple(
        (k, lat, lon) for lat in (a_up, a_down) for lon in (z_down, z, z_up)
    ):
        pl.semaphore_signal(barrier, inc=1, device_id=there, device_id_type=MESH)

    mine = pl.ds(pl.multiple_of(z * width, width), width)

    def local(src, dst, sem):
        return pltpu.make_async_copy(src, dst, sem)

    def remote(src, dst, send, recv, there):
        return pltpu.make_async_remote_copy(
            src_ref=src, dst_ref=dst, send_sem=send, recv_sem=recv,
            device_id=there, device_id_type=MESH,
        )

    def landed(block, sem):
        local(block, block, sem).wait()

    low_rows, high_rows = pl.ds(0, PAD), pl.ds(span - PAD, PAD)
    first_lanes, last_lanes = pl.ds(0, LANES), pl.ds(width - LANES, LANES)

    def row_copies():
        return [
            remote(x_hbm.at[:, SUBLANES - 1, high_rows, :], top, rows_send.at[0], rows_recv.at[0], (k, a_up, z)),
            remote(x_hbm.at[:, 0, low_rows, :], bot, rows_send.at[1], rows_recv.at[1], (k, a_down, z)),
        ]

    def corner_copies():
        return [
            remote(
                corner_packs.at[2 * i + j], corners.at[2 * i + j],
                corner_send.at[2 * i + j], corner_recv.at[2 * i + j], (k, lat, lon),
            )
            for i, lat in enumerate((a_up, a_down)) for j, lon in enumerate((z_down, z_up))
        ]

    blocks_of_span = span // SUBLANES
    turn = PAD // SUBLANES
    slots = LANES // EDGE
    first_blocks = list(range(turn + 1)) + list(range(blocks_of_span - turn, blocks_of_span))
    other_blocks = [i for i in range(blocks_of_span) if i not in first_blocks]
    early, late = [[(i, g) for i in numbers for g in range(SUBLANES)] for numbers in (first_blocks, other_blocks)]
    n_early, n_late = pl.cdiv(len(early), slots), pl.cdiv(len(late), slots)
    packs = ((early, 0), (late, n_early))

    def pack_copies(part):
        at = pl.ds(0, n_early) if part == 0 else pl.ds(n_early, n_late)
        return [
            remote(
                packed.at[i, :, at], got_packed.at[i, :, at],
                pack_send.at[part, i], pack_recv.at[part, i], (k, a, lon),
            )
            for i, lon in enumerate((z_down, z_up))
        ]

    def rows_of(c):
        return pl.ds(pl.multiple_of(c * CHUNK, CHUNK), CHUNK)

    def next_copy(c):
        return remote(
            x_hbm.at[:, :, rows_of(c), :], following.at[:, :, rows_of(c), :],
            next_send.at[c], next_recv.at[c], (k_down, a, z),
        )

    def part_copy(c, d):
        block = (slice(None), pl.ds(lax.rem(z + d, nlon) * per, per), rows_of(c), slice(None))
        return remote(
            x_hbm.at[block], following.at[block], part_send.at[c, d], part_recv.at[c, d], (k_down, a, z)
        )

    def inward(c, d, extras=False):
        zt = lax.rem(z + d, nlon)
        block = extra.at[:, :, rows_of(c - chunks), :] if extras else following.at[:, :, rows_of(c), :]
        src = block.at[:, pl.ds(zt * per, per)]
        dst = slab.at[:, :, rows_of(c), mine]
        if d == 0:
            return local(src, dst, in_recv.at[c, z])
        return remote(src, dst, in_send.at[c, d], in_recv.at[c, z], (k, a, zt))

    def relay(e):
        return remote(
            following.at[:, :, rows_of(kept + e), :], extra.at[:, :, rows_of(e), :],
            relay_send.at[e], relay_recv.at[e], (k_up, a, z),
        )

    def homeward(c, d, extras=False):
        zt = lax.rem(z + d, nlon)
        home = c - EXTRA if extras else c
        src = y_own.at[:, :, rows_of(c), pl.ds(pl.multiple_of(zt * width, width), width)]
        dst = out_hbm.at[:, pl.ds(z * per, per), rows_of(home), :]
        if extras and d == 0:
            return local(src, dst, out_recv.at[home, z])
        return remote(
            src, dst, out_send.at[c, d], out_recv.at[home, z], (k if extras else k_up, a, zt)
        )

    order = list(range(1, nlon)) + [0]

    def own_copies(src):
        return [local(src.at[c], own.at[c], own_sem.at[c]) for c in range(fields)]

    @pl.when(k < last)
    def _():
        for copy in own_copies(x_hbm):
            copy.start()

    @pl.when(k == last)
    def _():
        for copy in own_copies(back_hbm):
            copy.start()

    extra_copy = local(back_hbm.at[:, :, pl.ds(kept * CHUNK, EXTRA * CHUNK), :], extra, extra_sem)

    @pl.when(k == 0)
    def _():
        extra_copy.start()

    waves_copy = local(waves_hbm, waves_ref, waves_sem)

    lane = lax.broadcasted_iota(jnp.int32, (SUBLANES, LANES), 1)

    def strided(r, g):
        return pl.ds(SUBLANES * r + g, SUBLANES, stride=SUBLANES)

    def spread(put, low, main, high):
        for g in range(SUBLANES):
            for b in range((span + 2 * PAD) // SUBLANES):
                r = b * SUBLANES - PAD
                if r < 0:
                    value = low(r + PAD) if g == 0 else main(g - 1, span + r)
                elif r >= span:
                    value = high(r - span) if g == SUBLANES - 1 else main(g + 1, r - span)
                else:
                    value = main(g, r)
                put(strided(b * SUBLANES, g), value)

    def coriolis_rows():
        total = nlat * SUBLANES * span
        group = lax.broadcasted_iota(jnp.int32, (SUBLANES, LANES), 0)
        for first in range(0, span + 2 * PAD, LANES):
            row = a * (SUBLANES * span) + group * span + lane + (first - PAD)
            row = lax.rem(row + total, total).astype(jnp.float32)
            line = (2.0 * coriolis_peak) * jnp.sin((2.0 * np.pi / total) * (row + 0.5))
            for r in range(first, min(first + LANES, span + 2 * PAD)):
                frows[SUBLANES * r : SUBLANES * (r + 1), :] = jnp.broadcast_to(
                    line[:, r - first : r - first + 1], (SUBLANES, LANES)
                )

    def merge(parts, side):
        step = EDGE
        while len(parts) > 1:
            merged = []
            for i in range(0, len(parts) - 1, 2):
                if side == 0:
                    far = pltpu.roll(parts[i + 1], step, 1)
                    merged.append(jnp.where(lanes_of(far) < step, parts[i], far))
                else:
                    far = pltpu.roll(parts[i + 1], LANES - step, 1)
                    merged.append(jnp.where(lanes_of(far) >= LANES - step, parts[i], far))
            if len(parts) % 2:
                merged.append(parts[-1])
            parts, step = merged, 2 * step
        return parts[0]

    def lanes_of(value):
        return lax.broadcasted_iota(jnp.int32, value.shape, len(value.shape) - 1)

    def join(right, left, slot):
        shift = EDGE * slot
        near = pltpu.roll(right, LANES - shift, 1) if slot else right
        far = pltpu.roll(left, shift, 1) if slot else left
        return jnp.where(lane < EDGE, near, jnp.where(lane >= LANES - EDGE, far, 0.0))

    ends = ((SUBLANES - 1, span - PAD), (0, 0))

    @pl.when(k < last)
    def _():
        for copy in own_copies(x_hbm):
            copy.wait()

        @pl.loop(0, fields)
        def _(c):
            for side in range(2):
                cols = pl.ds(0 if side == 0 else width - LANES, LANES)
                for blocks, base in packs:
                    for v in range(0, len(blocks), slots):
                        packed[side, c, base + v // slots] = merge(
                            [own[c, g, pl.ds(SUBLANES * i, SUBLANES), cols] for i, g in blocks[v : v + slots]],
                            side,
                        )

        for i, (g, first) in enumerate(ends):
            for side in range(2):
                cols = pl.ds(0 if side == 0 else width - LANES, LANES)
                corner_packs[2 * i + side] = merge(
                    [
                        own[c, g, pl.ds(first + SUBLANES * b, SUBLANES), cols]
                        for c in range(fields) for b in range(turn)
                    ],
                    side,
                )

    @pl.when(k == 0)
    def _():
        extra_copy.wait()

        @pl.loop(0, fields)
        def _(c):
            extra[c] = own[c, :, pl.ds(kept * CHUNK, EXTRA * CHUNK), :] - extra[c]

    pl.semaphore_wait(barrier, nlon - 1 + 8)

    @pl.when(k < last)
    def _():
        for copy in pack_copies(0) + row_copies() + corner_copies() + pack_copies(1):
            copy.start()

    @pl.when(k == 0)
    def _():
        for c in range(kept):
            for d in order:
                part_copy(c, d).start()

    @pl.when(k > 0)
    def _():
        for c in range(chunks):
            next_copy(c).start()

    @pl.when(k == 0)
    def _():
        @pl.loop(0, EXTRA)
        def _(e):
            for d in order:
                inward(chunks + e, d, True).start()

    waves_copy.start()
    w_copy = local(w_hbm, w_ref, w_sem)
    w_copy.start()

    def edge_blocks(blocks, base, corner):
        @pl.loop(0, fields)
        def _(c):
            def put(r, g, value):
                state[c, groups, strided(r + PAD, g), :] = value

            for n, (i, g) in enumerate(blocks):
                v = base + n // slots
                value = join(got_packed[0, c, v], got_packed[1, c, v], n % slots)
                r = SUBLANES * i
                put(r, g, value)
                if r >= span - PAD and g < SUBLANES - 1:
                    put(r - span, g + 1, value)
                if r < PAD and g > 0:
                    put(r + span, g - 1, value)

        for c in range(fields):
            for b in range(turn):
                value = join(corners[2 * corner], corners[2 * corner + 1], c * turn + b)
                g, r = ((0, -PAD), (SUBLANES - 1, span))[corner]
                state[c, groups, strided(r + SUBLANES * b + PAD, g), :] = value

    def late_edges():
        for i in range(2):
            landed(got_packed.at[i, :, pl.ds(n_early, n_late)], pack_recv.at[1, i])
            landed(corners.at[2 + i], corner_recv.at[2 + i])
        edge_blocks(late, n_early, 1)

    @pl.when(k < last)
    def _():
        landed(top, rows_recv.at[0])
        landed(bot, rows_recv.at[1])
        coriolis_rows()

        @pl.loop(0, fields)
        def _(c):
            for j in range(groups):
                cols = pl.ds(j * LANES, LANES)

                def put(at, value):
                    state[c, j, at, :] = value

                spread(
                    put,
                    lambda r: top[c, pl.ds(r, SUBLANES), cols],
                    lambda g, r: own[c, g, pl.ds(r, SUBLANES), cols],
                    lambda r: bot[c, pl.ds(r, SUBLANES), cols],
                )

        for i in range(2):
            landed(got_packed.at[i, :, pl.ds(0, n_early)], pack_recv.at[0, i])
            landed(corners.at[i], corner_recv.at[i])
        edge_blocks(early, 0, 0)

    @pl.when(k == last)
    def _():
        for copy in own_copies(back_hbm):
            copy.wait()

    def spread_scales():
        wpad[...] = jnp.zeros_like(wpad)
        w_copy.wait()
        wpad[0:fields, 0 : half + 1] = w_ref[...]
        depth = wpad.shape[1]
        parts, rest = [], wpad[...]
        for _ in range(3):
            part = rest.astype(jnp.bfloat16).astype(jnp.float32)
            parts.append(part)
            rest = rest - part
        parts = jnp.concatenate(parts + [jnp.zeros_like(rest)], axis=0).astype(jnp.bfloat16)
        at = lax.broadcasted_iota(jnp.int32, (LANES, length), 1)
        row = lax.broadcasted_iota(jnp.int32, (LANES, length), 0)
        eighth = quarter // 2
        fours = 4 * jnp.where(at <= eighth, at, at - eighth)
        twos = 4 * lax.rem(at, eighth) + 2
        odds = 2 * lax.rem(at, quarter) + 1
        number = jnp.where(at < quarter, fours, jnp.where(at < half, twos, odds))
        total = jnp.zeros((parts.shape[0], length), jnp.float32)
        for b in range(depth // LANES):
            chosen = jnp.where(number == row + b * LANES, 1.0, 0.0).astype(jnp.bfloat16)
            total += jnp.dot(
                parts[:, b * LANES : (b + 1) * LANES], chosen, preferred_element_type=jnp.float32
            )
        line = total[0:8] + (total[8:16] + total[16:24])
        rows = per * CHUNK
        for c in range(fields):
            scales[c * rows : (c + 1) * rows, :] = jnp.broadcast_to(line[c : c + 1, :], (rows, length))

    at_first = lax.broadcasted_iota(jnp.int32, (BLOCK, SUBLANES, LANES), 2) == 0
    at_last = lax.broadcasted_iota(jnp.int32, (BLOCK, SUBLANES, LANES), 2) == LANES - 1

    def beside(parts):
        ahead = [pltpu.roll(q, LANES - 1, 2) for q in parts]
        behind = [pltpu.roll(q, 1, 2) for q in parts]
        return [
            (
                jnp.where(at_last, ahead[(j + 1) % ring], ahead[j]),
                jnp.where(at_first, behind[(j - 1) % ring], behind[j]),
            )
            for j in range(ring)
        ]

    def stage(arg, base, out, keep, mix, gain, start, blocks):
        @pl.loop(0, blocks)
        def _(i):
            r0 = start + i * BLOCK
            wide = pl.ds(pl.multiple_of(SUBLANES * (r0 - 1), SUBLANES), SUBLANES * (BLOCK + 2))
            at = pl.ds(pl.multiple_of(SUBLANES * r0, SUBLANES), SUBLANES * BLOCK)
            h, u, v = [
                [arg[c, j, wide, :].reshape(BLOCK + 2, SUBLANES, LANES) for j in range(ring)]
                for c in range(3)
            ]
            f2 = frows[at, :].reshape(BLOCK, SUBLANES, LANES)
            hm, um, vm = [[q[1:-1] for q in field] for field in (h, u, v)]

            def along(q):
                return q[2:] - q[:-2]

            h_by, u_by, v_by = beside(hm), beside(um), beside(vm)
            for j in range(ring):
                (h1, h0), (u1, u0), (v1, v0) = h_by[j], u_by[j], v_by[j]
                dv = v[j] + h[j] * v[j]
                rate_h = (u1 + h1 * u1) - (u0 + h0 * u0) + along(dv)
                rate_u = um[j] * (u1 - u0) + vm[j] * along(u[j]) + (h1 - h0) - f2 * vm[j]
                rate_v = um[j] * (v1 - v0) + vm[j] * along(v[j]) + along(h[j]) + f2 * um[j]
                for c, (m, rate) in enumerate(((hm[j], rate_h), (um[j], rate_u), (vm[j], rate_v))):
                    if base is None:
                        value = m - gain * rate
                    else:
                        old = base[c, j, at, :].reshape(BLOCK, SUBLANES, LANES)
                        value = keep * old + mix * m - gain * rate
                    out[c, j, at, :] = value.reshape(SUBLANES * BLOCK, LANES)

    def forecast(c):
        def bounds(t):
            ahead = stages - t
            fill = 2 * ahead + BLOCK - 1
            first = c * CHUNK + ahead
            extra = jnp.where(c == 0, fill - lax.rem(fill, BLOCK), 0)
            return PAD + first - extra, (CHUNK + extra) // BLOCK

        half_step = 0.5 * time_step

        @pl.loop(0, STEPS)
        def _(step):
            stage(state, None, mid1, 0.0, 1.0, half_step, *bounds(3 * step + 1))
            stage(mid1, state, mid2, 0.75, 0.25, 0.25 * half_step, *bounds(3 * step + 2))
            stage(mid2, state, state, 1.0 / 3.0, 2.0 / 3.0, 2.0 / 3.0 * half_step, *bounds(3 * step + 3))

    def filtered(c):
        for s in range(nlon):
            landed(slab.at[:, :, rows_of(c), pl.ds(s * width, width)], in_recv.at[c, s])
        rows = fields * per * CHUNK

        def product(value, way, place):
            high, low = split_parts(value)
            both = jnp.concatenate([high, low], axis=0)
            twice = jnp.dot(both, waves_ref[(way, 0) + place], preferred_element_type=jnp.float32)
            rest = jnp.dot(high, waves_ref[(way, 1) + place], preferred_element_type=jnp.float32)
            return twice[:rows] + (twice[rows:] + rest)

        value = slab[:, :, rows_of(c), :].reshape(rows, length)
        left, right = value[:, :half], value[:, half:]
        even, odd = left + right, left - right
        places = (
            (slice(0, quarter), slice(0, quarter)),
            (slice(0, quarter), slice(quarter, half)),
            (slice(quarter, quarter + half), slice(0, half)),
        )
        inputs = (even[:, :quarter] + even[:, quarter:], even[:, :quarter] - even[:, quarter:], odd)
        at, outputs = 0, []
        for place, mix in zip(places, inputs):
            count = mix.shape[1]
            coefficients = product(mix, 0, place) * scales[:, at : at + count]
            outputs.append(product(coefficients, 1, place))
            at += count
        fours, twos, odds = outputs
        for first, even in ((0, fours + twos), (quarter, fours - twos)):
            part = odds[:, first : first + quarter]
            for start, result in ((first, even + part), (first + half, even - part)):
                y_own[:, :, rows_of(c), start : start + quarter] = result.reshape(
                    fields, per, CHUNK, quarter
                )

        @pl.when(c < chunks)
        def _():
            for d in order:
                homeward(c, d).start()

        @pl.when(c >= chunks)
        def _():
            for d in order:
                homeward(c, d, True).start()

    def send_defects(c):
        for d in order:
            inward(c, d).start()

    def pass_on(e):
        landed(extra.at[:, :, rows_of(e), :], relay_recv.at[e])
        for d in order:
            inward(chunks + e, d, True).start()

    @pl.when(k == last)
    def _():
        @pl.loop(0, kept)
        def _(c):
            for d in order:
                at = pl.ds(lax.rem(z + d, nlon) * per, per)
                landed(following.at[:, at, rows_of(c), :], part_recv.at[c, d])
                following[:, at, rows_of(c), :] = (
                    following[:, at, rows_of(c), :] - own[:, at, rows_of(c), :]
                )
                inward(c, d).start()

        spread_scales()
        waves_copy.wait()

    @pl.when(k < last)
    def _():
        @pl.loop(0, chunks)
        def _(c):
            forecast(c)
            landed(following.at[:, :, rows_of(c), :], next_recv.at[c])

            @pl.loop(0, fields)
            def _(field):
                for g in range(SUBLANES):
                    at = pl.ds(SUBLANES * (c * CHUNK + PAD) + g, CHUNK, stride=SUBLANES)
                    for j in range(groups):
                        cols = pl.ds(j * LANES, LANES)
                        following[field, g, rows_of(c), cols] = (
                            following[field, g, rows_of(c), cols] - state[field, j, at, :]
                        )

            passes = (k == giver) & (c >= kept)

            @pl.when(passes)
            def _():
                relay(c - kept).start()

            @pl.when(jnp.logical_not(passes))
            def _():
                send_defects(c)

            @pl.when((k == taker) & (c > kept))
            def _():
                pass_on(c - kept - 1)

            @pl.when(c == 0)
            def _():
                late_edges()
                spread_scales()
                waves_copy.wait()

            @pl.loop(0, 2)
            def _(turn):
                slot = jnp.where(turn == 0, chunks + c, c - LAG)
                begun = ((k == 0) & (c < EXTRA)).astype(jnp.int32)
                ready = ((c >= LAG) & (c - LAG < n_own)).astype(jnp.int32)

                @pl.when(jnp.where(turn == 0, begun, ready) == 1)
                def _():
                    filtered(slot)

        @pl.when(k == taker)
        def _():
            pass_on(EXTRA - 1)

    first_slot = jnp.where(k == last, 0, jnp.minimum(n_own, chunks - LAG))

    @pl.loop(first_slot, n_own + EXTRA * is_taker)
    def _(c):
        filtered(c)

    @pl.loop(0, chunks)
    def _(c):
        for s in range(nlon):
            landed(out_hbm.at[:, pl.ds(s * per, per), rows_of(c), :], out_recv.at[c, s])

    @pl.when(k == 0)
    def _():
        for c in range(kept):
            for d in range(nlon):
                part_copy(c, d).wait_send()

    @pl.when(k > 0)
    def _():
        for c in range(chunks):
            next_copy(c).wait_send()

    @pl.loop(0, n_own)
    def _(c):
        for d in range(nlon):
            if d:
                inward(c, d).wait_send()
            homeward(c, d).wait_send()

    @pl.loop(chunks, chunks + n_extra)
    def _(c):
        for d in range(1, nlon):
            inward(c, d, True).wait_send()
            homeward(c, d, True).wait_send()

    @pl.when(k == giver)
    def _():
        for e in range(EXTRA):
            relay(e).wait_send()

    @pl.when(k < last)
    def _():
        for copy in row_copies() + corner_copies() + pack_copies(0) + pack_copies(1):
            copy.wait_send()


def solution(mesh):
    nsub, nlat, nlon = mesh.shape["sub"], mesh.shape["lat"], mesh.shape["lon"]

    def shards(launch, backdrop, inverse_variances):
        fields, lat_rows, width = backdrop.shape
        length = width * nlon
        half = length // 2
        span = lat_rows // SUBLANES
        chunks = span // CHUNK
        per = SUBLANES // nlon
        ring = width // LANES + 1
        natural = (fields, SUBLANES, span, width)
        f32, bf16 = jnp.float32, jnp.bfloat16
        dma = pltpu.SemaphoreType.DMA
        any_space = pl.BlockSpec(memory_space=pl.ANY)
        spread_rows = SUBLANES * (span + 2 * PAD)
        corner_like = pltpu.VMEM((4, SUBLANES, LANES), f32)
        slots = LANES // EDGE
        near = SUBLANES * (2 * (PAD // SUBLANES) + 1)
        n_packs = pl.cdiv(near, slots) + pl.cdiv(span - near, slots)
        pack_like = pltpu.VMEM((2, fields, n_packs, SUBLANES, LANES), f32)
        rows_like = pltpu.VMEM((fields, ring, spread_rows, LANES), f32)
        slab_like = pltpu.VMEM((fields, per, span + EXTRA * CHUNK, length), f32)
        out = pl.pallas_call(
            lambda *refs: kernel(nsub, nlat, nlon, *refs),
            name="weighted_defects",
            out_shape=jax.ShapeDtypeStruct(natural, f32),
            in_specs=[any_space, any_space, any_space, any_space],
            out_specs=any_space,
            scratch_shapes=[
                pltpu.VMEM((2, 2, half + half // 2, half), bf16),
                pltpu.VMEM((fields, half + 1), f32),
                pltpu.VMEM((8, half + LANES), f32),
                pltpu.VMEM((fields * per * CHUNK, length), f32),
                pltpu.VMEM((spread_rows, LANES), f32),
                pltpu.VMEM(natural, f32),
                pltpu.VMEM((fields, PAD, width), f32),
                pltpu.VMEM((fields, PAD, width), f32),
                corner_like, corner_like, pack_like, pack_like,
                pltpu.VMEM(natural, f32),
                pltpu.VMEM((fields, SUBLANES, EXTRA * CHUNK, width), f32),
                slab_like, slab_like,
                rows_like, rows_like, rows_like,
                dma, dma, dma((fields,)), dma,
                dma((2,)), dma((2,)), dma((4,)), dma((4,)), dma((2, 2)), dma((2, 2)),
                dma((chunks,)), dma((chunks,)),
                dma((chunks - EXTRA, nlon)), dma((chunks - EXTRA, nlon)), dma((EXTRA,)), dma((EXTRA,)),
                dma((chunks + EXTRA, nlon)), dma((chunks + EXTRA, nlon)),
                dma((chunks + EXTRA, nlon)), dma((chunks, nlon)),
            ],
            compiler_params=pltpu.CompilerParams(collective_id=0, has_side_effects=True, vmem_limit_bytes=VMEM_LIMIT),
        )(
            launch.reshape(natural), backdrop.reshape(natural), pltpu.with_memory_space_constraint(inverse_variances, pltpu.HBM),
            jnp.asarray(waves(length)),
        )
        return out.reshape(launch.shape)

    return jax.shard_map(
        shards,
        mesh=mesh,
        in_specs=(P("sub", None, "lat", "lon"), P(None, "lat", "lon"), P()),
        out_specs=P("sub", None, "lat", "lon"),
        check_vma=False,
    )
```

```python
import numpy as np
import jax
import jax.numpy as jnp
from jax import lax
from jax.experimental import pallas as pl
from jax.experimental.pallas import tpu as pltpu
from jax.sharding import PartitionSpec as P

STEPS = 3
PAD = 16
EDGE = 3 * STEPS
SUBLANES = 8
LANES = 128
CHUNK = 8
BLOCK = 4
LAG = 3
EXTRA = 4
VMEM_LIMIT = 52 * 2**20
MESH = pl.DeviceIdType.MESH

time_step = 0.5
coriolis_peak = 0.4


def waves(length):
    half, quarter = length // 2, length // 4

    def basis(points, pairs):
        n = np.arange(points)
        columns = []
        for turn, numbers in pairs:
            for m in numbers:
                scale = np.sqrt((1.0 if m in (0, half) else 2.0) / length)
                columns.append(scale * turn(2.0 * np.pi / length * ((m * n) % length)))
        return np.stack(columns, axis=1)

    fours = basis(quarter, ((np.cos, range(0, half + 1, 4)), (np.sin, range(4, half, 4))))
    twos = basis(quarter, ((np.cos, range(2, half, 4)), (np.sin, range(2, half, 4))))
    odds = basis(half, ((np.cos, range(1, half, 2)), (np.sin, range(1, half, 2))))
    out = np.stack([
        np.concatenate([np.concatenate([e, t], axis=1), o], axis=0)
        for e, t, o in ((fours, twos, odds), (fours.T, twos.T, odds.T))
    ]).astype(np.float32)
    high = out.astype(jnp.bfloat16)
    return np.stack([high, (out - high.astype(np.float32)).astype(jnp.bfloat16)], axis=1)


def split_parts(value):
    high = value.astype(jnp.bfloat16)
    return high, (value - high.astype(jnp.float32)).astype(jnp.bfloat16)


def kernel(
    nsub, nlat, nlon, x_hbm, back_hbm, w_hbm, waves_hbm, out_hbm,
    waves_ref, w_ref, wpad, scales, frows, own, top, bot, corners,
    corner_packs, packed, got_packed, following, extra, slab, y_own, state, mid1, mid2,
    waves_sem, w_sem, own_sem, extra_sem, rows_send, rows_recv, corner_send, corner_recv,
    pack_send, pack_recv, next_send, next_recv, part_send, part_recv, relay_send, relay_recv, in_send, in_recv, out_send, out_recv,
):
    k = lax.axis_index("sub")
    a = lax.axis_index("lat")
    z = lax.axis_index("lon")
    fields, _, span, width = x_hbm.shape
    length = width * nlon
    half = length // 2
    quarter = length // 4
    groups = width // LANES
    ring = groups + 1
    chunks = span // CHUNK
    per = SUBLANES // nlon
    stages = 3 * STEPS
    k_up = lax.rem(k + 1, nsub)
    k_down = lax.rem(k + nsub - 1, nsub)
    a_up = lax.rem(a + 1, nlat)
    a_down = lax.rem(a + nlat - 1, nlat)
    z_up = lax.rem(z + 1, nlon)
    z_down = lax.rem(z + nlon - 1, nlon)
    last = nsub - 1
    giver, taker = (last - 2, last - 1) if nsub > 2 else (-1, -1)
    kept = chunks - EXTRA
    is_giver, is_taker = (k == giver).astype(jnp.int32), (k == taker).astype(jnp.int32)
    is_first, is_last = (k == 0).astype(jnp.int32), (k == last).astype(jnp.int32)
    n_own = chunks - EXTRA * (is_giver + is_last)
    n_extra = EXTRA * (is_taker + is_first)

    barrier = pltpu.get_barrier_semaphore()
    for d in range(1, nlon):
        pl.semaphore_signal(
            barrier, inc=1, device_id=(k, a, lax.rem(z + d, nlon)), device_id_type=MESH
        )
    for there in ((k_up, a, z), (k_down, a, z)) + tuple(
        (k, lat, lon) for lat in (a_up, a_down) for lon in (z_down, z, z_up)
    ):
        pl.semaphore_signal(barrier, inc=1, device_id=there, device_id_type=MESH)

    mine = pl.ds(pl.multiple_of(z * width, width), width)

    def local(src, dst, sem):
        return pltpu.make_async_copy(src, dst, sem)

    def remote(src, dst, send, recv, there):
        return pltpu.make_async_remote_copy(
            src_ref=src, dst_ref=dst, send_sem=send, recv_sem=recv,
            device_id=there, device_id_type=MESH,
        )

    def landed(block, sem):
        local(block, block, sem).wait()

    low_rows, high_rows = pl.ds(0, PAD), pl.ds(span - PAD, PAD)
    first_lanes, last_lanes = pl.ds(0, LANES), pl.ds(width - LANES, LANES)

    def row_copies():
        return [
            remote(x_hbm.at[:, SUBLANES - 1, high_rows, :], top, rows_send.at[0], rows_recv.at[0], (k, a_up, z)),
            remote(x_hbm.at[:, 0, low_rows, :], bot, rows_send.at[1], rows_recv.at[1], (k, a_down, z)),
        ]

    def corner_copies():
        return [
            remote(
                corner_packs.at[2 * i + j], corners.at[2 * i + j],
                corner_send.at[2 * i + j], corner_recv.at[2 * i + j], (k, lat, lon),
            )
            for i, lat in enumerate((a_up, a_down)) for j, lon in enumerate((z_down, z_up))
        ]

    blocks_of_span = span // SUBLANES
    turn = PAD // SUBLANES
    slots = LANES // EDGE
    first_blocks = list(range(turn + 1)) + list(range(blocks_of_span - turn, blocks_of_span))
    other_blocks = [i for i in range(blocks_of_span) if i not in first_blocks]
    early, late = [[(i, g) for i in numbers for g in range(SUBLANES)] for numbers in (first_blocks, other_blocks)]
    n_early, n_late = pl.cdiv(len(early), slots), pl.cdiv(len(late), slots)
    packs = ((early, 0), (late, n_early))

    def pack_copies(part):
        at = pl.ds(0, n_early) if part == 0 else pl.ds(n_early, n_late)
        return [
            remote(
                packed.at[i, :, at], got_packed.at[i, :, at],
                pack_send.at[part, i], pack_recv.at[part, i], (k, a, lon),
            )
            for i, lon in enumerate((z_down, z_up))
        ]

    def rows_of(c):
        return pl.ds(pl.multiple_of(c * CHUNK, CHUNK), CHUNK)

    def next_copy(c):
        return remote(
            x_hbm.at[:, :, rows_of(c), :], following.at[:, :, rows_of(c), :],
            next_send.at[c], next_recv.at[c], (k_down, a, z),
        )

    def part_copy(c, d):
        block = (slice(None), pl.ds(lax.rem(z + d, nlon) * per, per), rows_of(c), slice(None))
        return remote(
            x_hbm.at[block], following.at[block], part_send.at[c, d], part_recv.at[c, d], (k_down, a, z)
        )

    def inward(c, d, extras=False):
        zt = lax.rem(z + d, nlon)
        block = extra.at[:, :, rows_of(c - chunks), :] if extras else following.at[:, :, rows_of(c), :]
        src = block.at[:, pl.ds(zt * per, per)]
        dst = slab.at[:, :, rows_of(c), mine]
        if d == 0:
            return local(src, dst, in_recv.at[c, z])
        return remote(src, dst, in_send.at[c, d], in_recv.at[c, z], (k, a, zt))

    def relay(e):
        return remote(
            following.at[:, :, rows_of(kept + e), :], extra.at[:, :, rows_of(e), :],
            relay_send.at[e], relay_recv.at[e], (k_up, a, z),
        )

    def homeward(c, d, extras=False):
        zt = lax.rem(z + d, nlon)
        home = c - EXTRA if extras else c
        src = y_own.at[:, :, rows_of(c), pl.ds(pl.multiple_of(zt * width, width), width)]
        dst = out_hbm.at[:, pl.ds(z * per, per), rows_of(home), :]
        if extras and d == 0:
            return local(src, dst, out_recv.at[home, z])
        return remote(
            src, dst, out_send.at[c, d], out_recv.at[home, z], (k if extras else k_up, a, zt)
        )

    order = list(range(1, nlon)) + [0]

    def own_copies(src):
        return [local(src.at[c], own.at[c], own_sem.at[c]) for c in range(fields)]

    @pl.when(k < last)
    def _():
        for copy in own_copies(x_hbm):
            copy.start()

    @pl.when(k == last)
    def _():
        for copy in own_copies(back_hbm):
            copy.start()

    extra_copy = local(back_hbm.at[:, :, pl.ds(kept * CHUNK, EXTRA * CHUNK), :], extra, extra_sem)

    @pl.when(k == 0)
    def _():
        extra_copy.start()

    waves_copy = local(waves_hbm, waves_ref, waves_sem)

    lane = lax.broadcasted_iota(jnp.int32, (SUBLANES, LANES), 1)

    def strided(r, g):
        return pl.ds(SUBLANES * r + g, SUBLANES, stride=SUBLANES)

    def spread(put, low, main, high):
        for g in range(SUBLANES):
            for b in range((span + 2 * PAD) // SUBLANES):
                r = b * SUBLANES - PAD
                if r < 0:
                    value = low(r + PAD) if g == 0 else main(g - 1, span + r)
                elif r >= span:
                    value = high(r - span) if g == SUBLANES - 1 else main(g + 1, r - span)
                else:
                    value = main(g, r)
                put(strided(b * SUBLANES, g), value)

    def coriolis_rows():
        total = nlat * SUBLANES * span
        group = lax.broadcasted_iota(jnp.int32, (SUBLANES, LANES), 0)
        for first in range(0, span + 2 * PAD, LANES):
            row = a * (SUBLANES * span) + group * span + lane + (first - PAD)
            row = lax.rem(row + total, total).astype(jnp.float32)
            line = (2.0 * coriolis_peak) * jnp.sin((2.0 * np.pi / total) * (row + 0.5))
            for r in range(first, min(first + LANES, span + 2 * PAD)):
                frows[SUBLANES * r : SUBLANES * (r + 1), :] = jnp.broadcast_to(
                    line[:, r - first : r - first + 1], (SUBLANES, LANES)
                )

    def merge(parts, side):
        step = EDGE
        while len(parts) > 1:
            merged = []
            for i in range(0, len(parts) - 1, 2):
                if side == 0:
                    far = pltpu.roll(parts[i + 1], step, 1)
                    merged.append(jnp.where(lanes_of(far) < step, parts[i], far))
                else:
                    far = pltpu.roll(parts[i + 1], LANES - step, 1)
                    merged.append(jnp.where(lanes_of(far) >= LANES - step, parts[i], far))
            if len(parts) % 2:
                merged.append(parts[-1])
            parts, step = merged, 2 * step
        return parts[0]

    def lanes_of(value):
        return lax.broadcasted_iota(jnp.int32, value.shape, len(value.shape) - 1)

    def join(right, left, slot):
        shift = EDGE * slot
        near = pltpu.roll(right, LANES - shift, 1) if slot else right
        far = pltpu.roll(left, shift, 1) if slot else left
        return jnp.where(lane < EDGE, near, jnp.where(lane >= LANES - EDGE, far, 0.0))

    ends = ((SUBLANES - 1, span - PAD), (0, 0))

    @pl.when(k < last)
    def _():
        for copy in own_copies(x_hbm):
            copy.wait()

        @pl.loop(0, fields)
        def _(c):
            for side in range(2):
                cols = pl.ds(0 if side == 0 else width - LANES, LANES)
                for blocks, base in packs:
                    for v in range(0, len(blocks), slots):
                        packed[side, c, base + v // slots] = merge(
                            [own[c, g, pl.ds(SUBLANES * i, SUBLANES), cols] for i, g in blocks[v : v + slots]],
                            side,
                        )

        for i, (g, first) in enumerate(ends):
            for side in range(2):
                cols = pl.ds(0 if side == 0 else width - LANES, LANES)
                corner_packs[2 * i + side] = merge(
                    [
                        own[c, g, pl.ds(first + SUBLANES * b, SUBLANES), cols]
                        for c in range(fields) for b in range(turn)
                    ],
                    side,
                )

    @pl.when(k == 0)
    def _():
        extra_copy.wait()

        @pl.loop(0, fields)
        def _(c):
            extra[c] = own[c, :, pl.ds(kept * CHUNK, EXTRA * CHUNK), :] - extra[c]

    pl.semaphore_wait(barrier, nlon - 1 + 8)

    @pl.when(k < last)
    def _():
        for copy in pack_copies(0) + row_copies() + corner_copies():
            copy.start()

    @pl.when(k == 0)
    def _():
        for c in range(kept):
            for d in order:
                part_copy(c, d).start()

    @pl.when(k > 0)
    def _():
        for c in range(chunks):
            next_copy(c).start()

    @pl.when(k == 0)
    def _():
        @pl.loop(0, EXTRA)
        def _(e):
            for d in order:
                inward(chunks + e, d, True).start()

    @pl.when(k < last)
    def _():
        for copy in pack_copies(1):
            copy.start()

    waves_copy.start()
    w_copy = local(w_hbm, w_ref, w_sem)
    w_copy.start()

    def edge_blocks(blocks, base, corner):
        @pl.loop(0, fields)
        def _(c):
            def put(r, g, value):
                state[c, groups, strided(r + PAD, g), :] = value

            for n, (i, g) in enumerate(blocks):
                v = base + n // slots
                value = join(got_packed[0, c, v], got_packed[1, c, v], n % slots)
                r = SUBLANES * i
                put(r, g, value)
                if r >= span - PAD and g < SUBLANES - 1:
                    put(r - span, g + 1, value)
                if r < PAD and g > 0:
                    put(r + span, g - 1, value)

        for c in range(fields):
            for b in range(turn):
                value = join(corners[2 * corner], corners[2 * corner + 1], c * turn + b)
                g, r = ((0, -PAD), (SUBLANES - 1, span))[corner]
                state[c, groups, strided(r + SUBLANES * b + PAD, g), :] = value

    def late_edges():
        for i in range(2):
            landed(got_packed.at[i, :, pl.ds(n_early, n_late)], pack_recv.at[1, i])
            landed(corners.at[2 + i], corner_recv.at[2 + i])
        edge_blocks(late, n_early, 1)

    @pl.when(k < last)
    def _():
        landed(top, rows_recv.at[0])
        landed(bot, rows_recv.at[1])
        coriolis_rows()

        @pl.loop(0, fields)
        def _(c):
            for j in range(groups):
                cols = pl.ds(j * LANES, LANES)

                def put(at, value):
                    state[c, j, at, :] = value

                spread(
                    put,
                    lambda r: top[c, pl.ds(r, SUBLANES), cols],
                    lambda g, r: own[c, g, pl.ds(r, SUBLANES), cols],
                    lambda r: bot[c, pl.ds(r, SUBLANES), cols],
                )

        for i in range(2):
            landed(got_packed.at[i, :, pl.ds(0, n_early)], pack_recv.at[0, i])
            landed(corners.at[i], corner_recv.at[i])
        edge_blocks(early, 0, 0)

    @pl.when(k == last)
    def _():
        for copy in own_copies(back_hbm):
            copy.wait()

    def spread_scales():
        wpad[...] = jnp.zeros_like(wpad)
        w_copy.wait()
        wpad[0:fields, 0 : half + 1] = w_ref[...]
        depth = wpad.shape[1]
        parts, rest = [], wpad[...]
        for _ in range(3):
            part = rest.astype(jnp.bfloat16).astype(jnp.float32)
            parts.append(part)
            rest = rest - part
        parts = jnp.concatenate(parts + [jnp.zeros_like(rest)], axis=0).astype(jnp.bfloat16)
        at = lax.broadcasted_iota(jnp.int32, (LANES, length), 1)
        row = lax.broadcasted_iota(jnp.int32, (LANES, length), 0)
        eighth = quarter // 2
        fours = 4 * jnp.where(at <= eighth, at, at - eighth)
        twos = 4 * lax.rem(at, eighth) + 2
        odds = 2 * lax.rem(at, quarter) + 1
        number = jnp.where(at < quarter, fours, jnp.where(at < half, twos, odds))
        total = jnp.zeros((parts.shape[0], length), jnp.float32)
        for b in range(depth // LANES):
            chosen = jnp.where(number == row + b * LANES, 1.0, 0.0).astype(jnp.bfloat16)
            total += jnp.dot(
                parts[:, b * LANES : (b + 1) * LANES], chosen, preferred_element_type=jnp.float32
            )
        line = total[0:8] + (total[8:16] + total[16:24])
        rows = per * CHUNK
        for c in range(fields):
            scales[c * rows : (c + 1) * rows, :] = jnp.broadcast_to(line[c : c + 1, :], (rows, length))

    at_first = lax.broadcasted_iota(jnp.int32, (BLOCK, SUBLANES, LANES), 2) == 0
    at_last = lax.broadcasted_iota(jnp.int32, (BLOCK, SUBLANES, LANES), 2) == LANES - 1

    def beside(parts):
        ahead = [pltpu.roll(q, LANES - 1, 2) for q in parts]
        behind = [pltpu.roll(q, 1, 2) for q in parts]
        return [
            (
                jnp.where(at_last, ahead[(j + 1) % ring], ahead[j]),
                jnp.where(at_first, behind[(j - 1) % ring], behind[j]),
            )
            for j in range(ring)
        ]

    def stage(arg, base, out, keep, mix, gain, start, blocks):
        @pl.loop(0, blocks)
        def _(i):
            r0 = start + i * BLOCK
            wide = pl.ds(pl.multiple_of(SUBLANES * (r0 - 1), SUBLANES), SUBLANES * (BLOCK + 2))
            at = pl.ds(pl.multiple_of(SUBLANES * r0, SUBLANES), SUBLANES * BLOCK)
            h, u, v = [
                [arg[c, j, wide, :].reshape(BLOCK + 2, SUBLANES, LANES) for j in range(ring)]
                for c in range(3)
            ]
            f2 = frows[at, :].reshape(BLOCK, SUBLANES, LANES)
            hm, um, vm = [[q[1:-1] for q in field] for field in (h, u, v)]

            def along(q):
                return q[2:] - q[:-2]

            h_by, u_by, v_by = beside(hm), beside(um), beside(vm)
            for j in range(ring):
                (h1, h0), (u1, u0), (v1, v0) = h_by[j], u_by[j], v_by[j]
                dv = v[j] + h[j] * v[j]
                rate_h = (u1 + h1 * u1) - (u0 + h0 * u0) + along(dv)
                rate_u = um[j] * (u1 - u0) + vm[j] * along(u[j]) + (h1 - h0) - f2 * vm[j]
                rate_v = um[j] * (v1 - v0) + vm[j] * along(v[j]) + along(h[j]) + f2 * um[j]
                for c, (m, rate) in enumerate(((hm[j], rate_h), (um[j], rate_u), (vm[j], rate_v))):
                    if base is None:
                        value = m - gain * rate
                    else:
                        old = base[c, j, at, :].reshape(BLOCK, SUBLANES, LANES)
                        value = keep * old + mix * m - gain * rate
                    out[c, j, at, :] = value.reshape(SUBLANES * BLOCK, LANES)

    def forecast(c):
        def bounds(t):
            ahead = stages - t
            fill = 2 * ahead + BLOCK - 1
            first = c * CHUNK + ahead
            extra = jnp.where(c == 0, fill - lax.rem(fill, BLOCK), 0)
            return PAD + first - extra, (CHUNK + extra) // BLOCK

        half_step = 0.5 * time_step

        @pl.loop(0, STEPS)
        def _(step):
            stage(state, None, mid1, 0.0, 1.0, half_step, *bounds(3 * step + 1))
            stage(mid1, state, mid2, 0.75, 0.25, 0.25 * half_step, *bounds(3 * step + 2))
            stage(mid2, state, state, 1.0 / 3.0, 2.0 / 3.0, 2.0 / 3.0 * half_step, *bounds(3 * step + 3))

    def filtered(c):
        for s in range(nlon):
            landed(slab.at[:, :, rows_of(c), pl.ds(s * width, width)], in_recv.at[c, s])
        rows = fields * per * CHUNK

        def product(value, way, place):
            high, low = split_parts(value)
            both = jnp.concatenate([high, low], axis=0)
            twice = jnp.dot(both, waves_ref[(way, 0) + place], preferred_element_type=jnp.float32)
            rest = jnp.dot(high, waves_ref[(way, 1) + place], preferred_element_type=jnp.float32)
            return twice[:rows] + (twice[rows:] + rest)

        value = slab[:, :, rows_of(c), :].reshape(rows, length)
        left, right = value[:, :half], value[:, half:]
        even, odd = left + right, left - right
        places = (
            (slice(0, quarter), slice(0, quarter)),
            (slice(0, quarter), slice(quarter, half)),
            (slice(quarter, quarter + half), slice(0, half)),
        )
        inputs = (even[:, :quarter] + even[:, quarter:], even[:, :quarter] - even[:, quarter:], odd)
        at, outputs = 0, []
        for place, mix in zip(places, inputs):
            count = mix.shape[1]
            coefficients = product(mix, 0, place) * scales[:, at : at + count]
            outputs.append(product(coefficients, 1, place))
            at += count
        fours, twos, odds = outputs
        for first, even in ((0, fours + twos), (quarter, fours - twos)):
            part = odds[:, first : first + quarter]
            for start, result in ((first, even + part), (first + half, even - part)):
                y_own[:, :, rows_of(c), start : start + quarter] = result.reshape(
                    fields, per, CHUNK, quarter
                )

        @pl.when(c < chunks)
        def _():
            for d in order:
                homeward(c, d).start()

        @pl.when(c >= chunks)
        def _():
            for d in order:
                homeward(c, d, True).start()

    def send_defects(c):
        for d in order:
            inward(c, d).start()

    def pass_on(e):
        landed(extra.at[:, :, rows_of(e), :], relay_recv.at[e])
        for d in order:
            inward(chunks + e, d, True).start()

    @pl.when(k == last)
    def _():
        @pl.loop(0, kept)
        def _(c):
            for d in order:
                at = pl.ds(lax.rem(z + d, nlon) * per, per)
                landed(following.at[:, at, rows_of(c), :], part_recv.at[c, d])
                following[:, at, rows_of(c), :] = (
                    following[:, at, rows_of(c), :] - own[:, at, rows_of(c), :]
                )
                inward(c, d).start()

        spread_scales()
        waves_copy.wait()

    @pl.when(k < last)
    def _():
        @pl.loop(0, chunks)
        def _(c):
            forecast(c)
            landed(following.at[:, :, rows_of(c), :], next_recv.at[c])

            @pl.loop(0, fields)
            def _(field):
                for g in range(SUBLANES):
                    at = pl.ds(SUBLANES * (c * CHUNK + PAD) + g, CHUNK, stride=SUBLANES)
                    for j in range(groups):
                        cols = pl.ds(j * LANES, LANES)
                        following[field, g, rows_of(c), cols] = (
                            following[field, g, rows_of(c), cols] - state[field, j, at, :]
                        )

            passes = (k == giver) & (c >= kept)

            @pl.when(passes)
            def _():
                relay(c - kept).start()

            @pl.when(jnp.logical_not(passes))
            def _():
                send_defects(c)

            @pl.when((k == taker) & (c > kept))
            def _():
                pass_on(c - kept - 1)

            @pl.when(c == 0)
            def _():
                late_edges()
                spread_scales()
                waves_copy.wait()

            @pl.loop(0, 2)
            def _(turn):
                slot = jnp.where(turn == 0, chunks + c, c - LAG)
                begun = ((k == 0) & (c < EXTRA)).astype(jnp.int32)
                ready = ((c >= LAG) & (c - LAG < n_own)).astype(jnp.int32)

                @pl.when(jnp.where(turn == 0, begun, ready) == 1)
                def _():
                    filtered(slot)

        @pl.when(k == taker)
        def _():
            pass_on(EXTRA - 1)

    first_slot = jnp.where(k == last, 0, jnp.minimum(n_own, chunks - LAG))

    @pl.loop(first_slot, n_own + EXTRA * is_taker)
    def _(c):
        filtered(c)

    @pl.loop(0, chunks)
    def _(c):
        for s in range(nlon):
            landed(out_hbm.at[:, pl.ds(s * per, per), rows_of(c), :], out_recv.at[c, s])

    @pl.when(k == 0)
    def _():
        for c in range(kept):
            for d in range(nlon):
                part_copy(c, d).wait_send()

    @pl.when(k > 0)
    def _():
        for c in range(chunks):
            next_copy(c).wait_send()

    @pl.loop(0, n_own)
    def _(c):
        for d in range(nlon):
            if d:
                inward(c, d).wait_send()
            homeward(c, d).wait_send()

    @pl.loop(chunks, chunks + n_extra)
    def _(c):
        for d in range(1, nlon):
            inward(c, d, True).wait_send()
            homeward(c, d, True).wait_send()

    @pl.when(k == giver)
    def _():
        for e in range(EXTRA):
            relay(e).wait_send()

    @pl.when(k < last)
    def _():
        for copy in row_copies() + corner_copies() + pack_copies(0) + pack_copies(1):
            copy.wait_send()


def solution(mesh):
    nsub, nlat, nlon = mesh.shape["sub"], mesh.shape["lat"], mesh.shape["lon"]

    def shards(launch, backdrop, inverse_variances):
        fields, lat_rows, width = backdrop.shape
        length = width * nlon
        half = length // 2
        span = lat_rows // SUBLANES
        chunks = span // CHUNK
        per = SUBLANES // nlon
        ring = width // LANES + 1
        natural = (fields, SUBLANES, span, width)
        f32, bf16 = jnp.float32, jnp.bfloat16
        dma = pltpu.SemaphoreType.DMA
        any_space = pl.BlockSpec(memory_space=pl.ANY)
        spread_rows = SUBLANES * (span + 2 * PAD)
        corner_like = pltpu.VMEM((4, SUBLANES, LANES), f32)
        slots = LANES // EDGE
        near = SUBLANES * (2 * (PAD // SUBLANES) + 1)
        n_packs = pl.cdiv(near, slots) + pl.cdiv(span - near, slots)
        pack_like = pltpu.VMEM((2, fields, n_packs, SUBLANES, LANES), f32)
        rows_like = pltpu.VMEM((fields, ring, spread_rows, LANES), f32)
        slab_like = pltpu.VMEM((fields, per, span + EXTRA * CHUNK, length), f32)
        out = pl.pallas_call(
            lambda *refs: kernel(nsub, nlat, nlon, *refs),
            name="weighted_defects",
            out_shape=jax.ShapeDtypeStruct(natural, f32),
            in_specs=[any_space, any_space, any_space, any_space],
            out_specs=any_space,
            scratch_shapes=[
                pltpu.VMEM((2, 2, half + half // 2, half), bf16),
                pltpu.VMEM((fields, half + 1), f32),
                pltpu.VMEM((8, half + LANES), f32),
                pltpu.VMEM((fields * per * CHUNK, length), f32),
                pltpu.VMEM((spread_rows, LANES), f32),
                pltpu.VMEM(natural, f32),
                pltpu.VMEM((fields, PAD, width), f32),
                pltpu.VMEM((fields, PAD, width), f32),
                corner_like, corner_like, pack_like, pack_like,
                pltpu.VMEM(natural, f32),
                pltpu.VMEM((fields, SUBLANES, EXTRA * CHUNK, width), f32),
                slab_like, slab_like,
                rows_like, rows_like, rows_like,
                dma, dma, dma((fields,)), dma,
                dma((2,)), dma((2,)), dma((4,)), dma((4,)), dma((2, 2)), dma((2, 2)),
                dma((chunks,)), dma((chunks,)),
                dma((chunks - EXTRA, nlon)), dma((chunks - EXTRA, nlon)), dma((EXTRA,)), dma((EXTRA,)),
                dma((chunks + EXTRA, nlon)), dma((chunks + EXTRA, nlon)),
                dma((chunks + EXTRA, nlon)), dma((chunks, nlon)),
            ],
            compiler_params=pltpu.CompilerParams(collective_id=0, has_side_effects=True, vmem_limit_bytes=VMEM_LIMIT),
        )(
            launch.reshape(natural), backdrop.reshape(natural), pltpu.with_memory_space_constraint(inverse_variances, pltpu.HBM),
            jnp.asarray(waves(length)),
        )
        return out.reshape(launch.shape)

    return jax.shard_map(
        shards,
        mesh=mesh,
        in_specs=(P("sub", None, "lat", "lon"), P(None, "lat", "lon"), P()),
        out_specs=P("sub", None, "lat", "lon"),
        check_vma=False,
    )
```

```python
import numpy as np
import jax
import jax.numpy as jnp
from jax import lax
from jax.experimental import pallas as pl
from jax.experimental.pallas import tpu as pltpu
from jax.sharding import PartitionSpec as P

STEPS = 3
PAD = 16
EDGE = 3 * STEPS
SUBLANES = 8
LANES = 128
CHUNK = 8
BLOCK = 4
LAG = 3
EXTRA = 4
VMEM_LIMIT = 52 * 2**20
MESH = pl.DeviceIdType.MESH

time_step = 0.5
coriolis_peak = 0.4


def waves(length):
    half, quarter = length // 2, length // 4

    def basis(points, pairs):
        n = np.arange(points)
        columns = []
        for turn, numbers in pairs:
            for m in numbers:
                scale = np.sqrt((1.0 if m in (0, half) else 2.0) / length)
                columns.append(scale * turn(2.0 * np.pi / length * ((m * n) % length)))
        return np.stack(columns, axis=1)

    fours = basis(quarter, ((np.cos, range(0, half + 1, 4)), (np.sin, range(4, half, 4))))
    twos = basis(quarter, ((np.cos, range(2, half, 4)), (np.sin, range(2, half, 4))))
    odds = basis(half, ((np.cos, range(1, half, 2)), (np.sin, range(1, half, 2))))
    out = np.stack([
        np.concatenate([np.concatenate([e, t], axis=1), o], axis=0)
        for e, t, o in ((fours, twos, odds), (fours.T, twos.T, odds.T))
    ]).astype(np.float32)
    high = out.astype(jnp.bfloat16)
    return np.stack([high, (out - high.astype(np.float32)).astype(jnp.bfloat16)], axis=1)


def split_parts(value):
    high = value.astype(jnp.bfloat16)
    return high, (value - high.astype(jnp.float32)).astype(jnp.bfloat16)


def kernel(
    nsub, nlat, nlon, x_hbm, back_hbm, w_hbm, waves_hbm, out_hbm,
    waves_ref, w_ref, wpad, scales, frows, own, top, bot, corners,
    corner_packs, packed, got_packed, following, extra, slab, y_own, state, mid1, mid2,
    waves_sem, w_sem, own_sem, extra_sem, rows_send, rows_recv, corner_send, corner_recv,
    pack_send, pack_recv, next_send, next_recv, part_send, part_recv, relay_send, relay_recv, in_send, in_recv, out_send, out_recv,
):
    k = lax.axis_index("sub")
    a = lax.axis_index("lat")
    z = lax.axis_index("lon")
    fields, _, span, width = x_hbm.shape
    length = width * nlon
    half = length // 2
    quarter = length // 4
    groups = width // LANES
    ring = groups + 1
    chunks = span // CHUNK
    per = SUBLANES // nlon
    stages = 3 * STEPS
    k_up = lax.rem(k + 1, nsub)
    k_down = lax.rem(k + nsub - 1, nsub)
    a_up = lax.rem(a + 1, nlat)
    a_down = lax.rem(a + nlat - 1, nlat)
    z_up = lax.rem(z + 1, nlon)
    z_down = lax.rem(z + nlon - 1, nlon)
    last = nsub - 1
    giver, taker = (last - 2, last - 1) if nsub > 2 else (-1, -1)
    kept = chunks - EXTRA
    is_giver, is_taker = (k == giver).astype(jnp.int32), (k == taker).astype(jnp.int32)
    is_first, is_last = (k == 0).astype(jnp.int32), (k == last).astype(jnp.int32)
    n_own = chunks - EXTRA * (is_giver + is_last)
    n_extra = EXTRA * (is_taker + is_first)

    barrier = pltpu.get_barrier_semaphore()
    for d in range(1, nlon):
        pl.semaphore_signal(
            barrier, inc=1, device_id=(k, a, lax.rem(z + d, nlon)), device_id_type=MESH
        )
    for there in ((k_up, a, z), (k_down, a, z)) + tuple(
        (k, lat, lon) for lat in (a_up, a_down) for lon in (z_down, z, z_up)
    ):
        pl.semaphore_signal(barrier, inc=1, device_id=there, device_id_type=MESH)

    mine = pl.ds(pl.multiple_of(z * width, width), width)

    def local(src, dst, sem):
        return pltpu.make_async_copy(src, dst, sem)

    def remote(src, dst, send, recv, there):
        return pltpu.make_async_remote_copy(
            src_ref=src, dst_ref=dst, send_sem=send, recv_sem=recv,
            device_id=there, device_id_type=MESH,
        )

    def landed(block, sem):
        local(block, block, sem).wait()

    low_rows, high_rows = pl.ds(0, PAD), pl.ds(span - PAD, PAD)
    first_lanes, last_lanes = pl.ds(0, LANES), pl.ds(width - LANES, LANES)

    def row_copies():
        return [
            remote(x_hbm.at[:, SUBLANES - 1, high_rows, :], top, rows_send.at[0], rows_recv.at[0], (k, a_up, z)),
            remote(x_hbm.at[:, 0, low_rows, :], bot, rows_send.at[1], rows_recv.at[1], (k, a_down, z)),
        ]

    def corner_copies():
        return [
            remote(
                corner_packs.at[2 * i + j], corners.at[2 * i + j],
                corner_send.at[2 * i + j], corner_recv.at[2 * i + j], (k, lat, lon),
            )
            for i, lat in enumerate((a_up, a_down)) for j, lon in enumerate((z_down, z_up))
        ]

    blocks_of_span = span // SUBLANES
    turn = PAD // SUBLANES
    slots = LANES // EDGE
    first_blocks = list(range(turn + 1)) + list(range(blocks_of_span - turn, blocks_of_span))
    other_blocks = [i for i in range(blocks_of_span) if i not in first_blocks]
    early, late = [[(i, g) for i in numbers for g in range(SUBLANES)] for numbers in (first_blocks, other_blocks)]
    n_early, n_late = pl.cdiv(len(early), slots), pl.cdiv(len(late), slots)
    packs = ((early, 0), (late, n_early))

    def pack_copies(part):
        at = pl.ds(0, n_early) if part == 0 else pl.ds(n_early, n_late)
        return [
            remote(
                packed.at[i, :, at], got_packed.at[i, :, at],
                pack_send.at[part, i], pack_recv.at[part, i], (k, a, lon),
            )
            for i, lon in enumerate((z_down, z_up))
        ]

    def rows_of(c):
        return pl.ds(pl.multiple_of(c * CHUNK, CHUNK), CHUNK)

    def next_copy(c):
        return remote(
            x_hbm.at[:, :, rows_of(c), :], following.at[:, :, rows_of(c), :],
            next_send.at[c], next_recv.at[c], (k_down, a, z),
        )

    def part_copy(c, d):
        block = (slice(None), pl.ds(lax.rem(z + d, nlon) * per, per), rows_of(c), slice(None))
        return remote(
            x_hbm.at[block], following.at[block], part_send.at[c, d], part_recv.at[c, d], (k_down, a, z)
        )

    def inward(c, d, extras=False):
        zt = lax.rem(z + d, nlon)
        block = extra.at[:, :, rows_of(c - chunks), :] if extras else following.at[:, :, rows_of(c), :]
        src = block.at[:, pl.ds(zt * per, per)]
        dst = slab.at[:, :, rows_of(c), mine]
        if d == 0:
            return local(src, dst, in_recv.at[c, z])
        return remote(src, dst, in_send.at[c, d], in_recv.at[c, z], (k, a, zt))

    def relay(e):
        return remote(
            following.at[:, :, rows_of(kept + e), :], extra.at[:, :, rows_of(e), :],
            relay_send.at[e], relay_recv.at[e], (k_up, a, z),
        )

    def homeward(c, d, extras=False):
        zt = lax.rem(z + d, nlon)
        home = c - EXTRA if extras else c
        src = y_own.at[:, :, rows_of(c), pl.ds(pl.multiple_of(zt * width, width), width)]
        dst = out_hbm.at[:, pl.ds(z * per, per), rows_of(home), :]
        if extras and d == 0:
            return local(src, dst, out_recv.at[home, z])
        return remote(
            src, dst, out_send.at[c, d], out_recv.at[home, z], (k if extras else k_up, a, zt)
        )

    order = list(range(1, nlon)) + [0]

    def own_copies(src):
        return [local(src.at[c], own.at[c], own_sem.at[c]) for c in range(fields)]

    @pl.when(k < last)
    def _():
        for copy in own_copies(x_hbm):
            copy.start()

    @pl.when(k == last)
    def _():
        for copy in own_copies(back_hbm):
            copy.start()

    extra_copy = local(back_hbm.at[:, :, pl.ds(kept * CHUNK, EXTRA * CHUNK), :], extra, extra_sem)

    @pl.when(k == 0)
    def _():
        extra_copy.start()

    waves_copy = local(waves_hbm, waves_ref, waves_sem)

    lane = lax.broadcasted_iota(jnp.int32, (SUBLANES, LANES), 1)

    def strided(r, g):
        return pl.ds(SUBLANES * r + g, SUBLANES, stride=SUBLANES)

    def spread(put, low, main, high):
        for g in range(SUBLANES):
            for b in range((span + 2 * PAD) // SUBLANES):
                r = b * SUBLANES - PAD
                if r < 0:
                    value = low(r + PAD) if g == 0 else main(g - 1, span + r)
                elif r >= span:
                    value = high(r - span) if g == SUBLANES - 1 else main(g + 1, r - span)
                else:
                    value = main(g, r)
                put(strided(b * SUBLANES, g), value)

    def coriolis_rows():
        total = nlat * SUBLANES * span
        group = lax.broadcasted_iota(jnp.int32, (SUBLANES, LANES), 0)
        for first in range(0, span + 2 * PAD, LANES):
            row = a * (SUBLANES * span) + group * span + lane + (first - PAD)
            row = lax.rem(row + total, total).astype(jnp.float32)
            line = (2.0 * coriolis_peak) * jnp.sin((2.0 * np.pi / total) * (row + 0.5))
            for r in range(first, min(first + LANES, span + 2 * PAD)):
                frows[SUBLANES * r : SUBLANES * (r + 1), :] = jnp.broadcast_to(
                    line[:, r - first : r - first + 1], (SUBLANES, LANES)
                )

    def merge(parts, side):
        step = EDGE
        while len(parts) > 1:
            merged = []
            for i in range(0, len(parts) - 1, 2):
                if side == 0:
                    far = pltpu.roll(parts[i + 1], step, 1)
                    merged.append(jnp.where(lanes_of(far) < step, parts[i], far))
                else:
                    far = pltpu.roll(parts[i + 1], LANES - step, 1)
                    merged.append(jnp.where(lanes_of(far) >= LANES - step, parts[i], far))
            if len(parts) % 2:
                merged.append(parts[-1])
            parts, step = merged, 2 * step
        return parts[0]

    def lanes_of(value):
        return lax.broadcasted_iota(jnp.int32, value.shape, len(value.shape) - 1)

    def join(right, left, slot):
        shift = EDGE * slot
        near = pltpu.roll(right, LANES - shift, 1) if slot else right
        far = pltpu.roll(left, shift, 1) if slot else left
        return jnp.where(lane < EDGE, near, jnp.where(lane >= LANES - EDGE, far, 0.0))

    ends = ((SUBLANES - 1, span - PAD), (0, 0))

    @pl.when(k < last)
    def _():
        for copy in own_copies(x_hbm):
            copy.wait()

        @pl.loop(0, fields)
        def _(c):
            for side in range(2):
                cols = pl.ds(0 if side == 0 else width - LANES, LANES)
                for blocks, base in packs:
                    for v in range(0, len(blocks), slots):
                        packed[side, c, base + v // slots] = merge(
                            [own[c, g, pl.ds(SUBLANES * i, SUBLANES), cols] for i, g in blocks[v : v + slots]],
                            side,
                        )

        for i, (g, first) in enumerate(ends):
            for side in range(2):
                cols = pl.ds(0 if side == 0 else width - LANES, LANES)
                corner_packs[2 * i + side] = merge(
                    [
                        own[c, g, pl.ds(first + SUBLANES * b, SUBLANES), cols]
                        for c in range(fields) for b in range(turn)
                    ],
                    side,
                )

    @pl.when(k == 0)
    def _():
        extra_copy.wait()

        @pl.loop(0, fields)
        def _(c):
            extra[c] = own[c, :, pl.ds(kept * CHUNK, EXTRA * CHUNK), :] - extra[c]

    pl.semaphore_wait(barrier, nlon - 1 + 8)

    @pl.when(k < last)
    def _():
        for copy in pack_copies(0) + row_copies() + corner_copies():
            copy.start()

    @pl.when(k == 0)
    def _():
        for c in range(kept):
            for d in order:
                part_copy(c, d).start()

    @pl.when(k > 0)
    def _():
        for c in range(chunks):
            next_copy(c).start()

    @pl.when(k == 0)
    def _():
        @pl.loop(0, EXTRA)
        def _(e):
            for d in order:
                inward(chunks + e, d, True).start()

    @pl.when(k < last)
    def _():
        for copy in pack_copies(1):
            copy.start()

    waves_copy.start()
    w_copy = local(w_hbm, w_ref, w_sem)
    w_copy.start()

    def edge_blocks(blocks, base, corner):
        @pl.loop(0, fields)
        def _(c):
            def put(r, g, value):
                state[c, groups, strided(r + PAD, g), :] = value

            for n, (i, g) in enumerate(blocks):
                v = base + n // slots
                value = join(got_packed[0, c, v], got_packed[1, c, v], n % slots)
                r = SUBLANES * i
                put(r, g, value)
                if r >= span - PAD and g < SUBLANES - 1:
                    put(r - span, g + 1, value)
                if r < PAD and g > 0:
                    put(r + span, g - 1, value)

        for c in range(fields):
            for b in range(turn):
                value = join(corners[2 * corner], corners[2 * corner + 1], c * turn + b)
                g, r = ((0, -PAD), (SUBLANES - 1, span))[corner]
                state[c, groups, strided(r + SUBLANES * b + PAD, g), :] = value

    def late_edges():
        for i in range(2):
            landed(got_packed.at[i, :, pl.ds(n_early, n_late)], pack_recv.at[1, i])
            landed(corners.at[2 + i], corner_recv.at[2 + i])
        edge_blocks(late, n_early, 1)

    @pl.when(k < last)
    def _():
        landed(top, rows_recv.at[0])
        landed(bot, rows_recv.at[1])
        coriolis_rows()

        @pl.loop(0, fields)
        def _(c):
            for j in range(groups):
                cols = pl.ds(j * LANES, LANES)

                def put(at, value):
                    state[c, j, at, :] = value

                spread(
                    put,
                    lambda r: top[c, pl.ds(r, SUBLANES), cols],
                    lambda g, r: own[c, g, pl.ds(r, SUBLANES), cols],
                    lambda r: bot[c, pl.ds(r, SUBLANES), cols],
                )

        for i in range(2):
            landed(got_packed.at[i, :, pl.ds(0, n_early)], pack_recv.at[0, i])
            landed(corners.at[i], corner_recv.at[i])
        edge_blocks(early, 0, 0)

    @pl.when(k == last)
    def _():
        for copy in own_copies(back_hbm):
            copy.wait()

    def spread_scales():
        wpad[...] = jnp.zeros_like(wpad)
        w_copy.wait()
        wpad[0:fields, 0 : half + 1] = w_ref[...]
        depth = wpad.shape[1]
        parts, rest = [], wpad[...]
        for _ in range(3):
            part = rest.astype(jnp.bfloat16).astype(jnp.float32)
            parts.append(part)
            rest = rest - part
        parts = jnp.concatenate(parts + [jnp.zeros_like(rest)], axis=0).astype(jnp.bfloat16)
        at = lax.broadcasted_iota(jnp.int32, (LANES, length), 1)
        row = lax.broadcasted_iota(jnp.int32, (LANES, length), 0)
        eighth = quarter // 2
        fours = 4 * jnp.where(at <= eighth, at, at - eighth)
        twos = 4 * lax.rem(at, eighth) + 2
        odds = 2 * lax.rem(at, quarter) + 1
        number = jnp.where(at < quarter, fours, jnp.where(at < half, twos, odds))
        total = jnp.zeros((parts.shape[0], length), jnp.float32)
        for b in range(depth // LANES):
            chosen = jnp.where(number == row + b * LANES, 1.0, 0.0).astype(jnp.bfloat16)
            total += jnp.dot(
                parts[:, b * LANES : (b + 1) * LANES], chosen, preferred_element_type=jnp.float32
            )
        line = total[0:8] + (total[8:16] + total[16:24])
        rows = per * CHUNK
        for c in range(fields):
            scales[c * rows : (c + 1) * rows, :] = jnp.broadcast_to(line[c : c + 1, :], (rows, length))

    at_first = lax.broadcasted_iota(jnp.int32, (BLOCK, SUBLANES, LANES), 2) == 0
    at_last = lax.broadcasted_iota(jnp.int32, (BLOCK, SUBLANES, LANES), 2) == LANES - 1

    def beside(parts):
        ahead = [pltpu.roll(q, LANES - 1, 2) for q in parts]
        behind = [pltpu.roll(q, 1, 2) for q in parts]
        return [
            (
                jnp.where(at_last, ahead[(j + 1) % ring], ahead[j]),
                jnp.where(at_first, behind[(j - 1) % ring], behind[j]),
            )
            for j in range(ring)
        ]

    def stage(arg, base, out, keep, mix, gain, start, blocks):
        @pl.loop(0, blocks)
        def _(i):
            r0 = start + i * BLOCK
            wide = pl.ds(pl.multiple_of(SUBLANES * (r0 - 1), SUBLANES), SUBLANES * (BLOCK + 2))
            at = pl.ds(pl.multiple_of(SUBLANES * r0, SUBLANES), SUBLANES * BLOCK)
            h, u, v = [
                [arg[c, j, wide, :].reshape(BLOCK + 2, SUBLANES, LANES) for j in range(ring)]
                for c in range(3)
            ]
            f2 = frows[at, :].reshape(BLOCK, SUBLANES, LANES)
            hm, um, vm = [[q[1:-1] for q in field] for field in (h, u, v)]

            def along(q):
                return q[2:] - q[:-2]

            h_by, u_by, v_by = beside(hm), beside(um), beside(vm)
            for j in range(ring):
                (h1, h0), (u1, u0), (v1, v0) = h_by[j], u_by[j], v_by[j]
                dv = v[j] + h[j] * v[j]
                rate_h = (u1 + h1 * u1) - (u0 + h0 * u0) + along(dv)
                rate_u = um[j] * (u1 - u0) + vm[j] * along(u[j]) + (h1 - h0) - f2 * vm[j]
                rate_v = um[j] * (v1 - v0) + vm[j] * along(v[j]) + along(h[j]) + f2 * um[j]
                for c, (m, rate) in enumerate(((hm[j], rate_h), (um[j], rate_u), (vm[j], rate_v))):
                    if base is None:
                        value = m - gain * rate
                    else:
                        old = base[c, j, at, :].reshape(BLOCK, SUBLANES, LANES)
                        value = keep * old + mix * m - gain * rate
                    out[c, j, at, :] = value.reshape(SUBLANES * BLOCK, LANES)

    def forecast(c):
        def bounds(t):
            ahead = stages - t
            fill = 2 * ahead + BLOCK - 1
            first = c * CHUNK + ahead
            extra = jnp.where(c == 0, fill - lax.rem(fill, BLOCK), 0)
            return PAD + first - extra, (CHUNK + extra) // BLOCK

        half_step = 0.5 * time_step

        @pl.loop(0, STEPS)
        def _(step):
            stage(state, None, mid1, 0.0, 1.0, half_step, *bounds(3 * step + 1))
            stage(mid1, state, mid2, 0.75, 0.25, 0.25 * half_step, *bounds(3 * step + 2))
            stage(mid2, state, state, 1.0 / 3.0, 2.0 / 3.0, 2.0 / 3.0 * half_step, *bounds(3 * step + 3))

    def filtered(c):
        for s in range(nlon):
            landed(slab.at[:, :, rows_of(c), pl.ds(s * width, width)], in_recv.at[c, s])
        rows = fields * per * CHUNK

        def product(value, way, place):
            high, low = split_parts(value)
            both = jnp.concatenate([high, low], axis=0)
            twice = jnp.dot(both, waves_ref[(way, 0) + place], preferred_element_type=jnp.float32)
            rest = jnp.dot(high, waves_ref[(way, 1) + place], preferred_element_type=jnp.float32)
            return twice[:rows] + (twice[rows:] + rest)

        value = slab[:, :, rows_of(c), :].reshape(rows, length)
        left, right = value[:, :half], value[:, half:]
        even, odd = left + right, left - right
        places = (
            (slice(0, quarter), slice(0, quarter)),
            (slice(0, quarter), slice(quarter, half)),
            (slice(quarter, quarter + half), slice(0, half)),
        )
        inputs = (even[:, :quarter] + even[:, quarter:], even[:, :quarter] - even[:, quarter:], odd)
        at, outputs = 0, []
        for place, mix in zip(places, inputs):
            count = mix.shape[1]
            coefficients = product(mix, 0, place) * scales[:, at : at + count]
            outputs.append(product(coefficients, 1, place))
            at += count
        fours, twos, odds = outputs
        for first, even in ((0, fours + twos), (quarter, fours - twos)):
            part = odds[:, first : first + quarter]
            for start, result in ((first, even + part), (first + half, even - part)):
                y_own[:, :, rows_of(c), start : start + quarter] = result.reshape(
                    fields, per, CHUNK, quarter
                )

        @pl.when(c < chunks)
        def _():
            for d in order:
                homeward(c, d).start()

        @pl.when(c >= chunks)
        def _():
            for d in order:
                homeward(c, d, True).start()

    def send_defects(c):
        for d in order:
            inward(c, d).start()

    def pass_on(e):
        landed(extra.at[:, :, rows_of(e), :], relay_recv.at[e])
        for d in order:
            inward(chunks + e, d, True).start()

    @pl.when(k == last)
    def _():
        @pl.loop(0, kept)
        def _(c):
            for d in order:
                at = pl.ds(lax.rem(z + d, nlon) * per, per)
                landed(following.at[:, at, rows_of(c), :], part_recv.at[c, d])
                following[:, at, rows_of(c), :] = (
                    following[:, at, rows_of(c), :] - own[:, at, rows_of(c), :]
                )
                inward(c, d).start()

        spread_scales()
        waves_copy.wait()

    @pl.when(k < last)
    def _():
        @pl.loop(0, chunks)
        def _(c):
            forecast(c)
            landed(following.at[:, :, rows_of(c), :], next_recv.at[c])

            @pl.loop(0, fields)
            def _(field):
                for g in range(SUBLANES):
                    at = pl.ds(SUBLANES * (c * CHUNK + PAD) + g, CHUNK, stride=SUBLANES)
                    for j in range(groups):
                        cols = pl.ds(j * LANES, LANES)
                        following[field, g, rows_of(c), cols] = (
                            following[field, g, rows_of(c), cols] - state[field, j, at, :]
                        )

            passes = (k == giver) & (c >= kept)

            @pl.when(passes)
            def _():
                relay(c - kept).start()

            @pl.when(jnp.logical_not(passes))
            def _():
                send_defects(c)

            @pl.when((k == taker) & (c > kept))
            def _():
                pass_on(c - kept - 1)

            @pl.when(c == 0)
            def _():
                late_edges()
                spread_scales()
                waves_copy.wait()

            @pl.loop(0, 2)
            def _(turn):
                slot = jnp.where(turn == 0, chunks + c, c - LAG)
                begun = ((k == 0) & (c < EXTRA)).astype(jnp.int32)
                ready = ((c >= LAG) & (c - LAG < n_own)).astype(jnp.int32)

                @pl.when(jnp.where(turn == 0, begun, ready) == 1)
                def _():
                    filtered(slot)

        @pl.when(k == taker)
        def _():
            pass_on(EXTRA - 1)

    first_slot = jnp.where(k == last, 0, jnp.minimum(n_own, chunks - LAG))

    @pl.loop(first_slot, n_own + EXTRA * is_taker)
    def _(c):
        filtered(c)

    @pl.when(k == 0)
    def _():
        for c in range(kept):
            for d in range(nlon):
                part_copy(c, d).wait_send()

    @pl.when(k > 0)
    def _():
        for c in range(chunks):
            next_copy(c).wait_send()

    @pl.loop(0, n_own)
    def _(c):
        for d in range(nlon):
            if d:
                inward(c, d).wait_send()
            homeward(c, d).wait_send()

    @pl.loop(chunks, chunks + n_extra)
    def _(c):
        for d in range(1, nlon):
            inward(c, d, True).wait_send()
            homeward(c, d, True).wait_send()

    @pl.when(k == giver)
    def _():
        for e in range(EXTRA):
            relay(e).wait_send()

    @pl.when(k < last)
    def _():
        for copy in row_copies() + corner_copies() + pack_copies(0) + pack_copies(1):
            copy.wait_send()

    @pl.loop(0, chunks)
    def _(c):
        for s in range(nlon):
            landed(out_hbm.at[:, pl.ds(s * per, per), rows_of(c), :], out_recv.at[c, s])


def solution(mesh):
    nsub, nlat, nlon = mesh.shape["sub"], mesh.shape["lat"], mesh.shape["lon"]

    def shards(launch, backdrop, inverse_variances):
        fields, lat_rows, width = backdrop.shape
        length = width * nlon
        half = length // 2
        span = lat_rows // SUBLANES
        chunks = span // CHUNK
        per = SUBLANES // nlon
        ring = width // LANES + 1
        natural = (fields, SUBLANES, span, width)
        f32, bf16 = jnp.float32, jnp.bfloat16
        dma = pltpu.SemaphoreType.DMA
        any_space = pl.BlockSpec(memory_space=pl.ANY)
        spread_rows = SUBLANES * (span + 2 * PAD)
        corner_like = pltpu.VMEM((4, SUBLANES, LANES), f32)
        slots = LANES // EDGE
        near = SUBLANES * (2 * (PAD // SUBLANES) + 1)
        n_packs = pl.cdiv(near, slots) + pl.cdiv(span - near, slots)
        pack_like = pltpu.VMEM((2, fields, n_packs, SUBLANES, LANES), f32)
        rows_like = pltpu.VMEM((fields, ring, spread_rows, LANES), f32)
        slab_like = pltpu.VMEM((fields, per, span + EXTRA * CHUNK, length), f32)
        out = pl.pallas_call(
            lambda *refs: kernel(nsub, nlat, nlon, *refs),
            name="weighted_defects",
            out_shape=jax.ShapeDtypeStruct(natural, f32),
            in_specs=[any_space, any_space, any_space, any_space],
            out_specs=any_space,
            scratch_shapes=[
                pltpu.VMEM((2, 2, half + half // 2, half), bf16),
                pltpu.VMEM((fields, half + 1), f32),
                pltpu.VMEM((8, half + LANES), f32),
                pltpu.VMEM((fields * per * CHUNK, length), f32),
                pltpu.VMEM((spread_rows, LANES), f32),
                pltpu.VMEM(natural, f32),
                pltpu.VMEM((fields, PAD, width), f32),
                pltpu.VMEM((fields, PAD, width), f32),
                corner_like, corner_like, pack_like, pack_like,
                pltpu.VMEM(natural, f32),
                pltpu.VMEM((fields, SUBLANES, EXTRA * CHUNK, width), f32),
                slab_like, slab_like,
                rows_like, rows_like, rows_like,
                dma, dma, dma((fields,)), dma,
                dma((2,)), dma((2,)), dma((4,)), dma((4,)), dma((2, 2)), dma((2, 2)),
                dma((chunks,)), dma((chunks,)),
                dma((chunks - EXTRA, nlon)), dma((chunks - EXTRA, nlon)), dma((EXTRA,)), dma((EXTRA,)),
                dma((chunks + EXTRA, nlon)), dma((chunks + EXTRA, nlon)),
                dma((chunks + EXTRA, nlon)), dma((chunks, nlon)),
            ],
            compiler_params=pltpu.CompilerParams(collective_id=0, has_side_effects=True, vmem_limit_bytes=VMEM_LIMIT),
        )(
            launch.reshape(natural), backdrop.reshape(natural), pltpu.with_memory_space_constraint(inverse_variances, pltpu.HBM),
            jnp.asarray(waves(length)),
        )
        return out.reshape(launch.shape)

    return jax.shard_map(
        shards,
        mesh=mesh,
        in_specs=(P("sub", None, "lat", "lon"), P(None, "lat", "lon"), P()),
        out_specs=P("sub", None, "lat", "lon"),
        check_vma=False,
    )
```

```python
import numpy as np
import jax
import jax.numpy as jnp
from jax import lax
from jax.experimental import pallas as pl
from jax.experimental.pallas import tpu as pltpu
from jax.sharding import PartitionSpec as P

STEPS = 3
PAD = 16
EDGE = 3 * STEPS
SUBLANES = 8
LANES = 128
CHUNK = 8
BLOCK = 4
LAG = 3
EXTRA = 4
VMEM_LIMIT = 52 * 2**20
MESH = pl.DeviceIdType.MESH

time_step = 0.5
coriolis_peak = 0.4


def waves(length):
    half, quarter = length // 2, length // 4

    def basis(points, pairs):
        n = np.arange(points)
        columns = []
        for turn, numbers in pairs:
            for m in numbers:
                scale = np.sqrt((1.0 if m in (0, half) else 2.0) / length)
                columns.append(scale * turn(2.0 * np.pi / length * ((m * n) % length)))
        return np.stack(columns, axis=1)

    fours = basis(quarter, ((np.cos, range(0, half + 1, 4)), (np.sin, range(4, half, 4))))
    twos = basis(quarter, ((np.cos, range(2, half, 4)), (np.sin, range(2, half, 4))))
    odds = basis(half, ((np.cos, range(1, half, 2)), (np.sin, range(1, half, 2))))
    out = np.stack([
        np.concatenate([np.concatenate([e, t], axis=1), o], axis=0)
        for e, t, o in ((fours, twos, odds), (fours.T, twos.T, odds.T))
    ]).astype(np.float32)
    high = out.astype(jnp.bfloat16)
    return np.stack([high, (out - high.astype(np.float32)).astype(jnp.bfloat16)], axis=1)


def split_parts(value):
    high = value.astype(jnp.bfloat16)
    return high, (value - high.astype(jnp.float32)).astype(jnp.bfloat16)


def kernel(
    nsub, nlat, nlon, x_hbm, back_hbm, w_hbm, waves_hbm, out_hbm,
    waves_ref, w_ref, wpad, scales, frows, own, top, bot, corners,
    corner_packs, packed, got_packed, following, extra, slab, y_own, state, mid1, mid2,
    waves_sem, w_sem, own_sem, extra_sem, rows_send, rows_recv, corner_send, corner_recv,
    pack_send, pack_recv, next_send, next_recv, part_send, part_recv, relay_send, relay_recv, in_send, in_recv, out_send, out_recv,
):
    k = lax.axis_index("sub")
    a = lax.axis_index("lat")
    z = lax.axis_index("lon")
    fields, _, span, width = x_hbm.shape
    length = width * nlon
    half = length // 2
    quarter = length // 4
    groups = width // LANES
    ring = groups + 1
    chunks = span // CHUNK
    per = SUBLANES // nlon
    stages = 3 * STEPS
    k_up = lax.rem(k + 1, nsub)
    k_down = lax.rem(k + nsub - 1, nsub)
    a_up = lax.rem(a + 1, nlat)
    a_down = lax.rem(a + nlat - 1, nlat)
    z_up = lax.rem(z + 1, nlon)
    z_down = lax.rem(z + nlon - 1, nlon)
    last = nsub - 1
    giver, taker = (last - 2, last - 1) if nsub > 2 else (-1, -1)
    kept = chunks - EXTRA
    is_giver, is_taker = (k == giver).astype(jnp.int32), (k == taker).astype(jnp.int32)
    is_first, is_last = (k == 0).astype(jnp.int32), (k == last).astype(jnp.int32)
    n_own = chunks - EXTRA * (is_giver + is_last)
    n_extra = EXTRA * (is_taker + is_first)

    barrier = pltpu.get_barrier_semaphore()
    for d in range(1, nlon):
        pl.semaphore_signal(
            barrier, inc=1, device_id=(k, a, lax.rem(z + d, nlon)), device_id_type=MESH
        )
    for there in ((k_up, a, z), (k_down, a, z)) + tuple(
        (k, lat, lon) for lat in (a_up, a_down) for lon in (z_down, z, z_up)
    ):
        pl.semaphore_signal(barrier, inc=1, device_id=there, device_id_type=MESH)

    mine = pl.ds(pl.multiple_of(z * width, width), width)

    def local(src, dst, sem):
        return pltpu.make_async_copy(src, dst, sem)

    def remote(src, dst, send, recv, there):
        return pltpu.make_async_remote_copy(
            src_ref=src, dst_ref=dst, send_sem=send, recv_sem=recv,
            device_id=there, device_id_type=MESH,
        )

    def landed(block, sem):
        local(block, block, sem).wait()

    low_rows, high_rows = pl.ds(0, PAD), pl.ds(span - PAD, PAD)
    first_lanes, last_lanes = pl.ds(0, LANES), pl.ds(width - LANES, LANES)

    def row_copies():
        return [
            remote(x_hbm.at[:, SUBLANES - 1, high_rows, :], top, rows_send.at[0], rows_recv.at[0], (k, a_up, z)),
            remote(x_hbm.at[:, 0, low_rows, :], bot, rows_send.at[1], rows_recv.at[1], (k, a_down, z)),
        ]

    def corner_copies():
        return [
            remote(
                corner_packs.at[2 * i + j], corners.at[2 * i + j],
                corner_send.at[2 * i + j], corner_recv.at[2 * i + j], (k, lat, lon),
            )
            for i, lat in enumerate((a_up, a_down)) for j, lon in enumerate((z_down, z_up))
        ]

    blocks_of_span = span // SUBLANES
    turn = PAD // SUBLANES
    slots = LANES // EDGE
    first_blocks = list(range(turn + 1)) + list(range(blocks_of_span - turn, blocks_of_span))
    other_blocks = [i for i in range(blocks_of_span) if i not in first_blocks]
    early, late = [[(i, g) for i in numbers for g in range(SUBLANES)] for numbers in (first_blocks, other_blocks)]
    n_early, n_late = pl.cdiv(len(early), slots), pl.cdiv(len(late), slots)
    packs = ((early, 0), (late, n_early))

    def pack_copies(part):
        at = pl.ds(0, n_early) if part == 0 else pl.ds(n_early, n_late)
        return [
            remote(
                packed.at[i, :, at], got_packed.at[i, :, at],
                pack_send.at[part, i], pack_recv.at[part, i], (k, a, lon),
            )
            for i, lon in enumerate((z_down, z_up))
        ]

    def rows_of(c):
        return pl.ds(pl.multiple_of(c * CHUNK, CHUNK), CHUNK)

    def next_copy(c):
        return remote(
            x_hbm.at[:, :, rows_of(c), :], following.at[:, :, rows_of(c), :],
            next_send.at[c], next_recv.at[c], (k_down, a, z),
        )

    def part_copy(c, d):
        block = (slice(None), pl.ds(lax.rem(z + d, nlon) * per, per), rows_of(c), slice(None))
        return remote(
            x_hbm.at[block], following.at[block], part_send.at[c, d], part_recv.at[c, d], (k_down, a, z)
        )

    def inward(c, d, extras=False):
        zt = lax.rem(z + d, nlon)
        block = extra.at[:, :, rows_of(c - chunks), :] if extras else following.at[:, :, rows_of(c), :]
        src = block.at[:, pl.ds(zt * per, per)]
        dst = slab.at[:, :, rows_of(c), mine]
        if d == 0:
            return local(src, dst, in_recv.at[c, z])
        return remote(src, dst, in_send.at[c, d], in_recv.at[c, z], (k, a, zt))

    def relay(e):
        return remote(
            following.at[:, :, rows_of(kept + e), :], extra.at[:, :, rows_of(e), :],
            relay_send.at[e], relay_recv.at[e], (k_up, a, z),
        )

    def homeward(c, d, extras=False):
        zt = lax.rem(z + d, nlon)
        home = c - EXTRA if extras else c
        src = y_own.at[:, :, rows_of(c), pl.ds(pl.multiple_of(zt * width, width), width)]
        dst = out_hbm.at[:, pl.ds(z * per, per), rows_of(home), :]
        if extras and d == 0:
            return local(src, dst, out_recv.at[home, z])
        return remote(
            src, dst, out_send.at[c, d], out_recv.at[home, z], (k if extras else k_up, a, zt)
        )

    order = sorted(range(1, nlon), key=lambda d: -min(d, nlon - d)) + [0]

    def own_copies(src):
        return [local(src.at[c], own.at[c], own_sem.at[c]) for c in range(fields)]

    @pl.when(k < last)
    def _():
        for copy in own_copies(x_hbm):
            copy.start()

    @pl.when(k == last)
    def _():
        for copy in own_copies(back_hbm):
            copy.start()

    extra_copy = local(back_hbm.at[:, :, pl.ds(kept * CHUNK, EXTRA * CHUNK), :], extra, extra_sem)

    @pl.when(k == 0)
    def _():
        extra_copy.start()

    waves_copy = local(waves_hbm, waves_ref, waves_sem)

    lane = lax.broadcasted_iota(jnp.int32, (SUBLANES, LANES), 1)

    def strided(r, g):
        return pl.ds(SUBLANES * r + g, SUBLANES, stride=SUBLANES)

    def spread(put, low, main, high):
        for g in range(SUBLANES):
            for b in range((span + 2 * PAD) // SUBLANES):
                r = b * SUBLANES - PAD
                if r < 0:
                    value = low(r + PAD) if g == 0 else main(g - 1, span + r)
                elif r >= span:
                    value = high(r - span) if g == SUBLANES - 1 else main(g + 1, r - span)
                else:
                    value = main(g, r)
                put(strided(b * SUBLANES, g), value)

    def coriolis_rows():
        total = nlat * SUBLANES * span
        group = lax.broadcasted_iota(jnp.int32, (SUBLANES, LANES), 0)
        for first in range(0, span + 2 * PAD, LANES):
            row = a * (SUBLANES * span) + group * span + lane + (first - PAD)
            row = lax.rem(row + total, total).astype(jnp.float32)
            line = (2.0 * coriolis_peak) * jnp.sin((2.0 * np.pi / total) * (row + 0.5))
            for r in range(first, min(first + LANES, span + 2 * PAD)):
                frows[SUBLANES * r : SUBLANES * (r + 1), :] = jnp.broadcast_to(
                    line[:, r - first : r - first + 1], (SUBLANES, LANES)
                )

    def merge(parts, side):
        step = EDGE
        while len(parts) > 1:
            merged = []
            for i in range(0, len(parts) - 1, 2):
                if side == 0:
                    far = pltpu.roll(parts[i + 1], step, 1)
                    merged.append(jnp.where(lanes_of(far) < step, parts[i], far))
                else:
                    far = pltpu.roll(parts[i + 1], LANES - step, 1)
                    merged.append(jnp.where(lanes_of(far) >= LANES - step, parts[i], far))
            if len(parts) % 2:
                merged.append(parts[-1])
            parts, step = merged, 2 * step
        return parts[0]

    def lanes_of(value):
        return lax.broadcasted_iota(jnp.int32, value.shape, len(value.shape) - 1)

    def join(right, left, slot):
        shift = EDGE * slot
        near = pltpu.roll(right, LANES - shift, 1) if slot else right
        far = pltpu.roll(left, shift, 1) if slot else left
        return jnp.where(lane < EDGE, near, jnp.where(lane >= LANES - EDGE, far, 0.0))

    ends = ((SUBLANES - 1, span - PAD), (0, 0))

    @pl.when(k < last)
    def _():
        for copy in own_copies(x_hbm):
            copy.wait()

        @pl.loop(0, fields)
        def _(c):
            for side in range(2):
                cols = pl.ds(0 if side == 0 else width - LANES, LANES)
                for blocks, base in packs:
                    for v in range(0, len(blocks), slots):
                        packed[side, c, base + v // slots] = merge(
                            [own[c, g, pl.ds(SUBLANES * i, SUBLANES), cols] for i, g in blocks[v : v + slots]],
                            side,
                        )

        for i, (g, first) in enumerate(ends):
            for side in range(2):
                cols = pl.ds(0 if side == 0 else width - LANES, LANES)
                corner_packs[2 * i + side] = merge(
                    [
                        own[c, g, pl.ds(first + SUBLANES * b, SUBLANES), cols]
                        for c in range(fields) for b in range(turn)
                    ],
                    side,
                )

    @pl.when(k == 0)
    def _():
        extra_copy.wait()

        @pl.loop(0, fields)
        def _(c):
            extra[c] = own[c, :, pl.ds(kept * CHUNK, EXTRA * CHUNK), :] - extra[c]

    pl.semaphore_wait(barrier, nlon - 1 + 8)

    @pl.when(k < last)
    def _():
        for copy in pack_copies(0) + row_copies() + corner_copies():
            copy.start()

    @pl.when(k == 0)
    def _():
        for c in range(kept):
            for d in order:
                part_copy(c, d).start()

    @pl.when(k > 0)
    def _():
        for c in range(chunks):
            next_copy(c).start()

    @pl.when(k == 0)
    def _():
        @pl.loop(0, EXTRA)
        def _(e):
            for d in order:
                inward(chunks + e, d, True).start()

    @pl.when(k < last)
    def _():
        for copy in pack_copies(1):
            copy.start()

    waves_copy.start()
    w_copy = local(w_hbm, w_ref, w_sem)
    w_copy.start()

    def edge_blocks(blocks, base, corner):
        @pl.loop(0, fields)
        def _(c):
            def put(r, g, value):
                state[c, groups, strided(r + PAD, g), :] = value

            for n, (i, g) in enumerate(blocks):
                v = base + n // slots
                value = join(got_packed[0, c, v], got_packed[1, c, v], n % slots)
                r = SUBLANES * i
                put(r, g, value)
                if r >= span - PAD and g < SUBLANES - 1:
                    put(r - span, g + 1, value)
                if r < PAD and g > 0:
                    put(r + span, g - 1, value)

        for c in range(fields):
            for b in range(turn):
                value = join(corners[2 * corner], corners[2 * corner + 1], c * turn + b)
                g, r = ((0, -PAD), (SUBLANES - 1, span))[corner]
                state[c, groups, strided(r + SUBLANES * b + PAD, g), :] = value

    def late_edges():
        for i in range(2):
            landed(got_packed.at[i, :, pl.ds(n_early, n_late)], pack_recv.at[1, i])
            landed(corners.at[2 + i], corner_recv.at[2 + i])
        edge_blocks(late, n_early, 1)

    @pl.when(k < last)
    def _():
        landed(top, rows_recv.at[0])
        landed(bot, rows_recv.at[1])
        coriolis_rows()

        @pl.loop(0, fields)
        def _(c):
            for j in range(groups):
                cols = pl.ds(j * LANES, LANES)

                def put(at, value):
                    state[c, j, at, :] = value

                spread(
                    put,
                    lambda r: top[c, pl.ds(r, SUBLANES), cols],
                    lambda g, r: own[c, g, pl.ds(r, SUBLANES), cols],
                    lambda r: bot[c, pl.ds(r, SUBLANES), cols],
                )

        for i in range(2):
            landed(got_packed.at[i, :, pl.ds(0, n_early)], pack_recv.at[0, i])
            landed(corners.at[i], corner_recv.at[i])
        edge_blocks(early, 0, 0)

    @pl.when(k == last)
    def _():
        for copy in own_copies(back_hbm):
            copy.wait()

    def spread_scales():
        wpad[...] = jnp.zeros_like(wpad)
        w_copy.wait()
        wpad[0:fields, 0 : half + 1] = w_ref[...]
        depth = wpad.shape[1]
        parts, rest = [], wpad[...]
        for _ in range(3):
            part = rest.astype(jnp.bfloat16).astype(jnp.float32)
            parts.append(part)
            rest = rest - part
        parts = jnp.concatenate(parts + [jnp.zeros_like(rest)], axis=0).astype(jnp.bfloat16)
        at = lax.broadcasted_iota(jnp.int32, (LANES, length), 1)
        row = lax.broadcasted_iota(jnp.int32, (LANES, length), 0)
        eighth = quarter // 2
        fours = 4 * jnp.where(at <= eighth, at, at - eighth)
        twos = 4 * lax.rem(at, eighth) + 2
        odds = 2 * lax.rem(at, quarter) + 1
        number = jnp.where(at < quarter, fours, jnp.where(at < half, twos, odds))
        total = jnp.zeros((parts.shape[0], length), jnp.float32)
        for b in range(depth // LANES):
            chosen = jnp.where(number == row + b * LANES, 1.0, 0.0).astype(jnp.bfloat16)
            total += jnp.dot(
                parts[:, b * LANES : (b + 1) * LANES], chosen, preferred_element_type=jnp.float32
            )
        line = total[0:8] + (total[8:16] + total[16:24])
        rows = per * CHUNK
        for c in range(fields):
            scales[c * rows : (c + 1) * rows, :] = jnp.broadcast_to(line[c : c + 1, :], (rows, length))

    at_first = lax.broadcasted_iota(jnp.int32, (BLOCK, SUBLANES, LANES), 2) == 0
    at_last = lax.broadcasted_iota(jnp.int32, (BLOCK, SUBLANES, LANES), 2) == LANES - 1

    def beside(parts):
        ahead = [pltpu.roll(q, LANES - 1, 2) for q in parts]
        behind = [pltpu.roll(q, 1, 2) for q in parts]
        return [
            (
                jnp.where(at_last, ahead[(j + 1) % ring], ahead[j]),
                jnp.where(at_first, behind[(j - 1) % ring], behind[j]),
            )
            for j in range(ring)
        ]

    def stage(arg, base, out, keep, mix, gain, start, blocks):
        @pl.loop(0, blocks)
        def _(i):
            r0 = start + i * BLOCK
            wide = pl.ds(pl.multiple_of(SUBLANES * (r0 - 1), SUBLANES), SUBLANES * (BLOCK + 2))
            at = pl.ds(pl.multiple_of(SUBLANES * r0, SUBLANES), SUBLANES * BLOCK)
            h, u, v = [
                [arg[c, j, wide, :].reshape(BLOCK + 2, SUBLANES, LANES) for j in range(ring)]
                for c in range(3)
            ]
            f2 = frows[at, :].reshape(BLOCK, SUBLANES, LANES)
            hm, um, vm = [[q[1:-1] for q in field] for field in (h, u, v)]

            def along(q):
                return q[2:] - q[:-2]

            h_by, u_by, v_by = beside(hm), beside(um), beside(vm)
            for j in range(ring):
                (h1, h0), (u1, u0), (v1, v0) = h_by[j], u_by[j], v_by[j]
                dv = v[j] + h[j] * v[j]
                rate_h = (u1 + h1 * u1) - (u0 + h0 * u0) + along(dv)
                rate_u = um[j] * (u1 - u0) + vm[j] * along(u[j]) + (h1 - h0) - f2 * vm[j]
                rate_v = um[j] * (v1 - v0) + vm[j] * along(v[j]) + along(h[j]) + f2 * um[j]
                for c, (m, rate) in enumerate(((hm[j], rate_h), (um[j], rate_u), (vm[j], rate_v))):
                    if base is None:
                        value = m - gain * rate
                    else:
                        old = base[c, j, at, :].reshape(BLOCK, SUBLANES, LANES)
                        value = keep * old + mix * m - gain * rate
                    out[c, j, at, :] = value.reshape(SUBLANES * BLOCK, LANES)

    def forecast(c):
        def bounds(t):
            ahead = stages - t
            fill = 2 * ahead + BLOCK - 1
            first = c * CHUNK + ahead
            extra = jnp.where(c == 0, fill - lax.rem(fill, BLOCK), 0)
            return PAD + first - extra, (CHUNK + extra) // BLOCK

        half_step = 0.5 * time_step

        @pl.loop(0, STEPS)
        def _(step):
            stage(state, None, mid1, 0.0, 1.0, half_step, *bounds(3 * step + 1))
            stage(mid1, state, mid2, 0.75, 0.25, 0.25 * half_step, *bounds(3 * step + 2))
            stage(mid2, state, state, 1.0 / 3.0, 2.0 / 3.0, 2.0 / 3.0 * half_step, *bounds(3 * step + 3))

    def filtered(c):
        for s in range(nlon):
            landed(slab.at[:, :, rows_of(c), pl.ds(s * width, width)], in_recv.at[c, s])
        rows = fields * per * CHUNK

        def product(value, way, place):
            high, low = split_parts(value)
            both = jnp.concatenate([high, low], axis=0)
            twice = jnp.dot(both, waves_ref[(way, 0) + place], preferred_element_type=jnp.float32)
            rest = jnp.dot(high, waves_ref[(way, 1) + place], preferred_element_type=jnp.float32)
            return twice[:rows] + (twice[rows:] + rest)

        value = slab[:, :, rows_of(c), :].reshape(rows, length)
        left, right = value[:, :half], value[:, half:]
        even, odd = left + right, left - right
        places = (
            (slice(0, quarter), slice(0, quarter)),
            (slice(0, quarter), slice(quarter, half)),
            (slice(quarter, quarter + half), slice(0, half)),
        )
        inputs = (even[:, :quarter] + even[:, quarter:], even[:, :quarter] - even[:, quarter:], odd)
        at, outputs = 0, []
        for place, mix in zip(places, inputs):
            count = mix.shape[1]
            coefficients = product(mix, 0, place) * scales[:, at : at + count]
            outputs.append(product(coefficients, 1, place))
            at += count
        fours, twos, odds = outputs
        for first, even in ((0, fours + twos), (quarter, fours - twos)):
            part = odds[:, first : first + quarter]
            for start, result in ((first, even + part), (first + half, even - part)):
                y_own[:, :, rows_of(c), start : start + quarter] = result.reshape(
                    fields, per, CHUNK, quarter
                )

        @pl.when(c < chunks)
        def _():
            for d in order:
                homeward(c, d).start()

        @pl.when(c >= chunks)
        def _():
            for d in order:
                homeward(c, d, True).start()

    def send_defects(c):
        for d in order:
            inward(c, d).start()

    def pass_on(e):
        landed(extra.at[:, :, rows_of(e), :], relay_recv.at[e])
        for d in order:
            inward(chunks + e, d, True).start()

    @pl.when(k == last)
    def _():
        @pl.loop(0, kept)
        def _(c):
            for d in order:
                at = pl.ds(lax.rem(z + d, nlon) * per, per)
                landed(following.at[:, at, rows_of(c), :], part_recv.at[c, d])
                following[:, at, rows_of(c), :] = (
                    following[:, at, rows_of(c), :] - own[:, at, rows_of(c), :]
                )
                inward(c, d).start()

        spread_scales()
        waves_copy.wait()

    @pl.when(k < last)
    def _():
        @pl.loop(0, chunks)
        def _(c):
            forecast(c)
            landed(following.at[:, :, rows_of(c), :], next_recv.at[c])

            @pl.loop(0, fields)
            def _(field):
                for g in range(SUBLANES):
                    at = pl.ds(SUBLANES * (c * CHUNK + PAD) + g, CHUNK, stride=SUBLANES)
                    for j in range(groups):
                        cols = pl.ds(j * LANES, LANES)
                        following[field, g, rows_of(c), cols] = (
                            following[field, g, rows_of(c), cols] - state[field, j, at, :]
                        )

            passes = (k == giver) & (c >= kept)

            @pl.when(passes)
            def _():
                relay(c - kept).start()

            @pl.when(jnp.logical_not(passes))
            def _():
                send_defects(c)

            @pl.when((k == taker) & (c > kept))
            def _():
                pass_on(c - kept - 1)

            @pl.when(c == 0)
            def _():
                late_edges()
                spread_scales()
                waves_copy.wait()

            @pl.loop(0, 2)
            def _(turn):
                slot = jnp.where(turn == 0, chunks + c, c - LAG)
                begun = ((k == 0) & (c < EXTRA)).astype(jnp.int32)
                ready = ((c >= LAG) & (c - LAG < n_own)).astype(jnp.int32)

                @pl.when(jnp.where(turn == 0, begun, ready) == 1)
                def _():
                    filtered(slot)

        @pl.when(k == taker)
        def _():
            pass_on(EXTRA - 1)

    first_slot = jnp.where(k == last, 0, jnp.minimum(n_own, chunks - LAG))

    @pl.loop(first_slot, n_own + EXTRA * is_taker)
    def _(c):
        filtered(c)

    @pl.when(k == 0)
    def _():
        for c in range(kept):
            for d in range(nlon):
                part_copy(c, d).wait_send()

    @pl.when(k > 0)
    def _():
        for c in range(chunks):
            next_copy(c).wait_send()

    @pl.loop(0, n_own)
    def _(c):
        for d in range(nlon):
            if d:
                inward(c, d).wait_send()
            homeward(c, d).wait_send()

    @pl.loop(chunks, chunks + n_extra)
    def _(c):
        for d in range(1, nlon):
            inward(c, d, True).wait_send()
            homeward(c, d, True).wait_send()

    @pl.when(k == giver)
    def _():
        for e in range(EXTRA):
            relay(e).wait_send()

    @pl.when(k < last)
    def _():
        for copy in row_copies() + corner_copies() + pack_copies(0) + pack_copies(1):
            copy.wait_send()

    @pl.loop(0, chunks)
    def _(c):
        for s in range(nlon):
            landed(out_hbm.at[:, pl.ds(s * per, per), rows_of(c), :], out_recv.at[c, s])


def solution(mesh):
    nsub, nlat, nlon = mesh.shape["sub"], mesh.shape["lat"], mesh.shape["lon"]

    def shards(launch, backdrop, inverse_variances):
        fields, lat_rows, width = backdrop.shape
        length = width * nlon
        half = length // 2
        span = lat_rows // SUBLANES
        chunks = span // CHUNK
        per = SUBLANES // nlon
        ring = width // LANES + 1
        natural = (fields, SUBLANES, span, width)
        f32, bf16 = jnp.float32, jnp.bfloat16
        dma = pltpu.SemaphoreType.DMA
        any_space = pl.BlockSpec(memory_space=pl.ANY)
        spread_rows = SUBLANES * (span + 2 * PAD)
        corner_like = pltpu.VMEM((4, SUBLANES, LANES), f32)
        slots = LANES // EDGE
        near = SUBLANES * (2 * (PAD // SUBLANES) + 1)
        n_packs = pl.cdiv(near, slots) + pl.cdiv(span - near, slots)
        pack_like = pltpu.VMEM((2, fields, n_packs, SUBLANES, LANES), f32)
        rows_like = pltpu.VMEM((fields, ring, spread_rows, LANES), f32)
        slab_like = pltpu.VMEM((fields, per, span + EXTRA * CHUNK, length), f32)
        out = pl.pallas_call(
            lambda *refs: kernel(nsub, nlat, nlon, *refs),
            name="weighted_defects",
            out_shape=jax.ShapeDtypeStruct(natural, f32),
            in_specs=[any_space, any_space, any_space, any_space],
            out_specs=any_space,
            scratch_shapes=[
                pltpu.VMEM((2, 2, half + half // 2, half), bf16),
                pltpu.VMEM((fields, half + 1), f32),
                pltpu.VMEM((8, half + LANES), f32),
                pltpu.VMEM((fields * per * CHUNK, length), f32),
                pltpu.VMEM((spread_rows, LANES), f32),
                pltpu.VMEM(natural, f32),
                pltpu.VMEM((fields, PAD, width), f32),
                pltpu.VMEM((fields, PAD, width), f32),
                corner_like, corner_like, pack_like, pack_like,
                pltpu.VMEM(natural, f32),
                pltpu.VMEM((fields, SUBLANES, EXTRA * CHUNK, width), f32),
                slab_like, slab_like,
                rows_like, rows_like, rows_like,
                dma, dma, dma((fields,)), dma,
                dma((2,)), dma((2,)), dma((4,)), dma((4,)), dma((2, 2)), dma((2, 2)),
                dma((chunks,)), dma((chunks,)),
                dma((chunks - EXTRA, nlon)), dma((chunks - EXTRA, nlon)), dma((EXTRA,)), dma((EXTRA,)),
                dma((chunks + EXTRA, nlon)), dma((chunks + EXTRA, nlon)),
                dma((chunks + EXTRA, nlon)), dma((chunks, nlon)),
            ],
            compiler_params=pltpu.CompilerParams(collective_id=0, has_side_effects=True, vmem_limit_bytes=VMEM_LIMIT),
        )(
            launch.reshape(natural), backdrop.reshape(natural), pltpu.with_memory_space_constraint(inverse_variances, pltpu.HBM),
            jnp.asarray(waves(length)),
        )
        return out.reshape(launch.shape)

    return jax.shard_map(
        shards,
        mesh=mesh,
        in_specs=(P("sub", None, "lat", "lon"), P(None, "lat", "lon"), P()),
        out_specs=P("sub", None, "lat", "lon"),
        check_vma=False,
    )
```
